128 devices in a mesh: batch: 32 (over y, z, core), mp: 4 (over x).
Axes of the slice: x: 4, y: 4, z: 4, core: 2. Of those that a mesh axis runs over, the one named last changes fastest.
Arguments:
- init_state: float32 [16384, 256], P(('batch', 'mp')), may hold values from -6 to 6
- brownian: bfloat16 [32, 16384, 256], P(None, ('batch', 'mp')), may hold values from -6 to 6
- step_size: float32 [16384], P(('batch', 'mp')), may hold values from 0.02 to 0.1
- lengths: int32 [16384], P(('batch', 'mp')), may hold values from 1 to 32, as said below
- obs_steps: int32 [16384, 8], P(('batch', 'mp')), may hold values from 1 to 32, as said below
- observed: bfloat16 [16384, 8, 128], P(('batch', 'mp')), may hold values from -6 to 6
- w_in: bfloat16 [256, 1024], P(None, 'mp'), may hold values from -0.375 to 0.375
- b_in: bfloat16 [1024], P('mp'), may hold values from -3 to 3
- w_out: bfloat16 [1024, 256], P('mp'), may hold values from -0.1875 to 0.1875
- b_out: float32 [256], replicated, may hold values from -4 to 4
- decoder: bfloat16 [256, 128], replicated, may hold values from -0.375 to 0.375
- prior_rate: float32 [256], replicated, may hold values from 0.1 to 2
- diffusion: float32 [256], replicated, may hold values from 0.7 to 1.4
Outputs:
- elbo_series: float32 [16384], P(('batch', 'mp'))
- scores: float32 [2], replicated
- grad_w_in: float32 [256, 1024], P(None, 'mp')
- grad_b_in: float32 [1024], P('mp')
- grad_w_out: float32 [1024, 256], P('mp')
- grad_b_out: float32 [256], replicated
- grad_decoder: float32 [256, 128], replicated
- grad_init: float32 [16384, 256], P(('batch', 'mp'))
The draws below stay inside these ranges and needn't reach their ends.
Inputs may be any that keep to these rules, and one draw needn't show every extreme that they name: `lengths`: some series has 32 live steps in every draw. obs_steps[i, j] is at most lengths[i].
All inputs are finite; a program needn't handle non-finite values.
Results may differ from the reference program's by a relative error of at most 0.0019.
Values may be sent and summed in bfloat16 or wider, within the bound.
A program may use at most 64 MiB of HBM per device.

```python
import math
import jax
import jax.numpy as jnp
from jax import lax

L = 256
H = 1024
P_SIZE = 128
OBS = 8
S_STEPS = 32
ROWS_DEV = 128
SERIES = 16384


def length_table(key):
    block_count = SERIES // ROWS_DEV
    key_ceiling, key_choose, key_length, key_place = jax.random.split(jax.random.fold_in(key, 11), 4)
    ceilings = jax.random.randint(key_ceiling, (block_count,), S_STEPS // 4, S_STEPS + 1)
    chosen = jax.random.randint(key_choose, (), 0, block_count)
    ceilings = jnp.where(jnp.arange(block_count) == chosen, S_STEPS, ceilings)
    per_row = jnp.repeat(ceilings, ROWS_DEV, total_repeat_length=SERIES)
    drawn = jax.random.randint(key_length, (SERIES,), 1, per_row + 1)
    places = jax.random.randint(key_place, (block_count,), 0, ROWS_DEV)
    topmost = jnp.arange(SERIES) % ROWS_DEV == jnp.repeat(places, ROWS_DEV, total_repeat_length=SERIES)
    return jnp.where(topmost, per_row, drawn).astype(jnp.int32)


def draw_lengths(key, part):
    return length_table(key)


def draw_obs_steps(key, part):
    table = length_table(key)
    picks = jax.random.randint(jax.random.fold_in(key, 23), (SERIES, OBS), 1, table[:, None] + 1)
    return picks.astype(jnp.int32)


def levels(rng, shape, cuts, smallest, top_value):
    level, own = 1.0, jax.random.fold_in(rng, 6)
    for axis_at, blocks in cuts:
        steps = jnp.exp(jax.random.uniform(jax.random.fold_in(own, axis_at), (blocks,), jnp.float32, smallest / len(cuts), top_value / len(cuts)))
        level = level * jnp.repeat(steps, shape[axis_at] // blocks).reshape([-1 if axis == axis_at else 1 for axis in range(len(shape))])
    return level


def gaussian(own_key, extent, spread, bound, cuts=(), kind=jnp.bfloat16):
    gain = levels(own_key, extent, cuts, -0.22, 0.18) if cuts else 1.0
    values = jax.random.normal(own_key, extent, jnp.float32) * spread * gain
    return jnp.minimum(jnp.maximum(values, -bound), bound).astype(kind)


def setup_inputs(seed: int = 0) -> dict:
    key_list = jax.random.split(jax.random.key(seed), 14)
    init_state = gaussian(key_list[0], (SERIES, L), 1.0, 6.0, ((0, 128),), jnp.float32)
    brownian = gaussian(key_list[1], (S_STEPS, SERIES, L), 1.0, 6.0, ((1, 128),))
    step_size = jnp.clip(jnp.exp(math.log(0.1) - 1.609438 * jax.random.uniform(key_list[2], (SERIES,), jnp.float32) ** levels(key_list[2], (SERIES,), ((0, 128),), -0.2, 0.2)), 0.02, 0.1)
    lengths = draw_lengths(jax.random.fold_in(key_list[13], 71), 0)
    obs_steps = draw_obs_steps(jax.random.fold_in(key_list[13], 71), 0)
    observed = gaussian(key_list[5], (SERIES, OBS, P_SIZE), 1.0, 6.0, ((0, 128),))
    w_in = gaussian(key_list[6], (L, H), L ** -0.5, 0.375, ((1, 4),))
    b_in = gaussian(key_list[7], (H,), 0.5, 3.0, ((0, 4),))
    w_out = gaussian(key_list[8], (H, L), H ** -0.5, 0.1875, ((0, 4),))
    b_out = gaussian(key_list[9], (L,), 1.0, 4.0, (), jnp.float32)
    decoder = gaussian(key_list[10], (L, P_SIZE), L ** -0.5, 0.375)
    prior_rate = jnp.clip(jnp.exp(jax.random.uniform(key_list[11], (L,), jnp.float32, math.log(0.1), math.log(2.0))), 0.1, 2.0)
    diffusion = jnp.clip(jax.random.uniform(key_list[12], (L,), jnp.float32, 0.7, 1.4), 0.7, 1.4)
    return dict(init_state=init_state, brownian=brownian, step_size=step_size, lengths=lengths, obs_steps=obs_steps, observed=observed, w_in=w_in, b_in=b_in, w_out=w_out, b_out=b_out, decoder=decoder, prior_rate=prior_rate, diffusion=diffusion)


def block_terms(block_init, block_noise, block_step, block_lengths, block_obs, block_observed, w_in, b_in, w_out, b_out, decoder, prior_rate, diffusion):
    row_count = block_init.shape[0]
    num_steps = block_noise.shape[0]
    live_mask = (jnp.arange(num_steps, dtype=jnp.int32)[:, None] < block_lengths[None, :]).astype(jnp.float32)
    step_col = block_step[:, None]
    root_col = jnp.sqrt(block_step)[:, None]
    bias_in = b_in.astype(jnp.float32)

    def forward(loop_state, inputs):
        current, kl_sum = loop_state
        increment, live_now = inputs
        activity = jnp.tanh(jnp.dot(current.astype(jnp.bfloat16), w_in, preferred_element_type=jnp.float32) + bias_in).astype(jnp.bfloat16)
        drift_now = jnp.dot(activity, w_out, preferred_element_type=jnp.float32) + b_out
        residual = (drift_now + prior_rate * current) / diffusion
        kl_sum = kl_sum + live_now * 0.5 * block_step * lax.optimization_barrier(jnp.sum(residual * residual, axis=1))
        following = current + live_now[:, None] * (step_col * drift_now + diffusion * root_col * increment.astype(jnp.float32))
        return ((following, kl_sum), (current, activity, residual))
    (last_state, kl_total), (visited, activities, residuals) = lax.scan(forward, (block_init, jnp.zeros((row_count,), jnp.float32)), (block_noise, live_mask))
    trajectory = jnp.concatenate([visited, last_state[None]], axis=0)
    picked = trajectory[block_obs, jnp.arange(row_count, dtype=jnp.int32)[:, None]]
    picked_round = picked.astype(jnp.bfloat16).reshape(-1, picked.shape[2])
    flat_obs = block_observed.reshape(-1, block_observed.shape[2]).astype(jnp.float32)
    misfit = jnp.dot(picked_round, decoder, preferred_element_type=jnp.float32) - flat_obs
    loglik = -0.5 * lax.optimization_barrier(jnp.sum((misfit * misfit).reshape(row_count, -1), axis=1))
    misfit_round = misfit.astype(jnp.bfloat16)
    decoder_grad = jnp.dot(picked_round.T, misfit_round, preferred_element_type=jnp.float32)
    misfit_back = jnp.dot(misfit_round, decoder.T, preferred_element_type=jnp.float32).reshape(row_count, block_obs.shape[1], -1)
    onehot = (block_obs[:, :, None] == jnp.arange(num_steps + 1, dtype=jnp.int32)[None, None, :]).astype(jnp.float32)
    obs_back = jnp.einsum('bjs,bjl->sbl', onehot, misfit_back, precision=lax.Precision.HIGHEST)

    def backward(loop_state, inputs):
        cotangent, sum_w_in, sum_b_in, sum_w_out, sum_b_out = loop_state
        current, activity, residual, live_now, obs_here = inputs
        factor = (live_now * block_step)[:, None]
        scaled = residual / diffusion
        update = factor * (cotangent + scaled)
        update_round = update.astype(jnp.bfloat16)
        activity_value = activity.astype(jnp.float32)
        pre_grad = jnp.dot(update_round, w_out.T, preferred_element_type=jnp.float32) * (1.0 - activity_value * activity_value)
        pre_round = pre_grad.astype(jnp.bfloat16)
        cotangent = cotangent + factor * prior_rate * scaled + jnp.dot(pre_round, w_in.T, preferred_element_type=jnp.float32) + obs_here
        sum_w_in = sum_w_in + jnp.dot(current.astype(jnp.bfloat16).T, pre_round, preferred_element_type=jnp.float32)
        sum_b_in = sum_b_in + lax.optimization_barrier(jnp.sum(pre_grad, axis=0))
        sum_w_out = sum_w_out + jnp.dot(activity.T, update_round, preferred_element_type=jnp.float32)
        sum_b_out = sum_b_out + lax.optimization_barrier(jnp.sum(update, axis=0))
        return ((cotangent, sum_w_in, sum_b_in, sum_w_out, sum_b_out), None)
    start_back = (obs_back[num_steps], jnp.zeros(w_in.shape, jnp.float32), jnp.zeros((w_in.shape[1],), jnp.float32), jnp.zeros(w_out.shape, jnp.float32), jnp.zeros((w_out.shape[1],), jnp.float32))
    (cotangent, sum_w_in, sum_b_in, sum_w_out, sum_b_out), _ = lax.scan(backward, start_back, (visited, activities, residuals, live_mask, obs_back[:num_steps]), reverse=True)
    divisor = (L * block_lengths + P_SIZE * OBS).astype(jnp.float32)
    elbo_rows = (loglik - kl_total) / divisor
    return (elbo_rows, cotangent, jnp.sum(loglik), jnp.sum(kl_total), sum_w_in, sum_b_in, sum_w_out, sum_b_out, decoder_grad)

def reference(init_state, brownian, step_size, lengths, obs_steps, observed, w_in, b_in, w_out, b_out, decoder, prior_rate, diffusion):
    block_count = SERIES // ROWS_DEV
    blocked = (init_state.reshape(block_count, ROWS_DEV, L), jnp.transpose(brownian.reshape(S_STEPS, block_count, ROWS_DEV, L), (1, 0, 2, 3)), step_size.reshape(block_count, ROWS_DEV), lengths.reshape(block_count, ROWS_DEV), obs_steps.reshape(block_count, ROWS_DEV, OBS), observed.reshape(block_count, ROWS_DEV, OBS, P_SIZE))
    zero_totals = (jnp.zeros((L, H), jnp.float32), jnp.zeros((H,), jnp.float32), jnp.zeros((H, L), jnp.float32), jnp.zeros((L,), jnp.float32), jnp.zeros((L, P_SIZE), jnp.float32), jnp.zeros((), jnp.float32), jnp.zeros((), jnp.float32))

    def visit(totals, pieces):
        outcome = block_terms(pieces[0], pieces[1], pieces[2], pieces[3], pieces[4], pieces[5], w_in, b_in, w_out, b_out, decoder, prior_rate, diffusion)
        elbo_rows, init_grad, loglik_sum, kl_sum, sum_w_in, sum_b_in, sum_w_out, sum_b_out, decoder_grad = outcome
        fresh = (sum_w_in, sum_b_in, sum_w_out, sum_b_out, decoder_grad, loglik_sum, kl_sum)
        totals = tuple((first + second for first, second in zip(totals, fresh)))
        return (totals, (elbo_rows, init_grad))
    totals, (elbo_rows, init_grads) = lax.scan(visit, zero_totals, blocked)
    elbo_series = elbo_rows.reshape(SERIES)
    grad_init = init_grads.reshape(SERIES, L)
    scores = jnp.stack([totals[5] / SERIES, totals[6] / SERIES])
    return (elbo_series, scores, totals[0] / SERIES, totals[1] / SERIES, totals[2] / SERIES, totals[3] / SERIES, totals[4] / SERIES, grad_init)
```

```python
import functools

import jax
import jax.numpy as jnp
from jax import lax
from jax.experimental import pallas as pl
from jax.experimental.pallas import tpu as pltpu
from jax.sharding import Mesh
from jax.sharding import PartitionSpec as P

BATCH_MP = ("batch_0", "batch_1", "batch_2", "mp")
F32, BF16 = jnp.float32, jnp.bfloat16
UNROLL = 2


def mm(a, b):
    return jnp.dot(a, b, preferred_element_type=F32)


def twice(a):
    return jnp.concatenate([a, a], axis=1)


def solve_kernel(
    scale,
    init, brown, step, length, obs, observed, w_in, b_in, w_out, b_out, dec, prior, diff,
    elbo, big, small, ginit,
    state, stepb, lenb, dr, obsb, obsf, acc, klacc, traj_t, acts, scaled, pre, back, upd_t,
    w_in_t, w_out_t, dec_t, cot, sum_in, sum_out,
):
    steps, rows, width = brown.shape
    hidden = w_in.shape[1]
    n_obs = obs.shape[1]

    stepb[...] = jnp.broadcast_to(step[...], (rows, rows)).T
    lenb[...] = jnp.broadcast_to(length[...], (rows, rows)).T
    dr[...] = diff[...] * twice(jnp.sqrt(stepb[...]))
    obs_all = obs[...]
    for j in range(n_obs):
        obsb[j] = jnp.broadcast_to(obs_all[:, j : j + 1], (rows, rows))
    obsf[...] = observed[...].astype(F32).reshape(rows * n_obs, dec.shape[1])
    w_in_t[...] = w_in[...].T
    w_out_t[...] = w_out[...].T
    dec_flip = dec[...].T
    dec_t[...] = jnp.concatenate([dec_flip, dec_flip], axis=0)
    klacc[...] = jnp.zeros_like(klacc)
    acc[...] = jnp.zeros_like(acc)
    sum_in[...] = jnp.zeros_like(sum_in)
    sum_out[...] = jnp.zeros_like(sum_out)
    state[...] = init[...]
    bias = b_in[...].astype(F32)
    inv = 1.0 / diff[...]

    def see(k, rounded):
        seen = mm(rounded, dec[...])
        for j in range(n_obs):
            acc[j] = jnp.where(obsb[j] == k, seen, acc[j])

    def at(k):
        return pl.ds(pl.multiple_of(k * rows, rows), rows)

    def forward(k, carry):
        s = state[...]
        rounded = s.astype(BF16)
        activity = jnp.tanh(mm(rounded, w_in[...]) + bias).astype(BF16)
        drift = mm(activity, w_out[...]) + b_out[...]
        live = lenb[...] > k
        factor = jnp.where(live, stepb[...], 0.0)
        residual = (drift + prior[...] * s) * inv
        noise = dr[...] * brown[k].astype(F32)
        state[...] = s + twice(factor) * drift + jnp.where(twice(live), noise, 0.0)
        acts[at(k), :] = activity
        scaled[k] = residual * inv
        square = residual * residual
        klacc[...] += (0.5 * factor) * (square[:, :rows] + square[:, rows:])
        traj_t[:, at(k)] = rounded.T
        see(k, rounded)
        return carry

    lax.fori_loop(0, steps, forward, 0, unroll=UNROLL)
    last = state[...].astype(BF16)
    traj_t[:, at(steps)] = last.T
    see(steps, last)

    total = jnp.zeros((rows, rows), F32)
    for j in range(n_obs):
        misfit = acc[j] - obsf[pl.ds(j, rows, stride=n_obs), :]
        total = total + misfit * misfit
        acc[j] = misfit.astype(BF16).astype(F32)
    loglik = -0.5 * total
    divisor = (width * lenb[...] + rows * n_obs).astype(F32)
    per_series = jnp.sum(loglik - klacc[...], axis=1, keepdims=True) / divisor
    elbo[...] = per_series.T[0:1, :]

    def gathered(k):
        m = jnp.zeros((rows, rows), F32)
        for j in range(n_obs):
            m = m + jnp.where(obsb[j] == k, acc[j], 0.0)
        high = m.astype(BF16)
        low = (m - high.astype(F32)).astype(BF16)
        return jnp.concatenate([high, low], axis=1)

    final = gathered(steps)
    back[at(steps), :] = final
    cot[...] = mm(final, dec_t[...])

    def backward(i, carry):
        k = steps - 1 - i
        c = cot[...]
        factor = twice(jnp.where(lenb[...] > k, stepb[...], 0.0))
        part = scaled[k]
        update = factor * (c + part)
        rounded = update.astype(BF16)
        value = acts[at(k), :].astype(F32)
        pre_grad = mm(rounded, w_out_t[...]) * (1.0 - value * value)
        pre_round = pre_grad.astype(BF16)
        seen = gathered(k)
        cot[...] = (
            c + factor * prior[...] * part + (mm(pre_round, w_in_t[...]) + mm(seen, dec_t[...]))
        )
        pre[at(k), :] = pre_round
        back[at(k), :] = seen
        upd_t[:, at(k)] = rounded.T
        sum_in[...] += jnp.sum(pre_grad.reshape(rows // 8, 8, hidden), axis=0)
        sum_out[...] += jnp.sum(update.reshape(rows // 8, 8, width), axis=0)
        return carry

    lax.fori_loop(0, steps, backward, 0, unroll=UNROLL)
    ginit[...] = cot[...]

    def weights(n, carry):
        cols = pl.ds(pl.multiple_of(n * width, width), width)
        grad_in = mm(traj_t[:, : steps * rows], pre[:, cols]) * scale
        grad_out = mm(upd_t[...], acts[:, cols]) * scale
        for h in range(2):
            big[h, :, n] = grad_in[:, h * rows : (h + 1) * rows].reshape(2, 4, 4, 8, rows)
            big[2 + h, :, n] = grad_out[:, h * rows : (h + 1) * rows].reshape(2, 4, 4, 8, rows)
        return carry

    lax.fori_loop(0, hidden // width, weights, 0)
    grad_dec = mm(traj_t[...], back[...]) * scale
    small[...] = jnp.zeros_like(small)
    small[:, :, :, 0] = (grad_dec[:, :rows] + grad_dec[:, rows:]).reshape(2, 4, 4, 8, rows)
    row_in = jnp.sum(sum_in[...], axis=0, keepdims=True) * scale
    row_out = jnp.sum(sum_out[...], axis=0, keepdims=True) * scale
    for r in range(hidden // rows):
        small[0, 0, 0, 1, r : r + 1, :] = row_in[:, r * rows : (r + 1) * rows]
    for r in range(width // rows):
        small[0, 0, 1, 1, r : r + 1, :] = row_out[:, r * rows : (r + 1) * rows]
    for r, part in ((2, loglik), (3, klacc[...])):
        whole = jnp.sum(jnp.sum(part, axis=0, keepdims=True), axis=1, keepdims=True) * scale
        small[0, 0, 1, 1, r : r + 1, :] = jnp.broadcast_to(whole, (1, rows))


def solve(total, init, brown, step, length, obs, observed, w_in, b_in, w_out, b_out, dec, prior, diff):
    steps, rows, width = brown.shape
    hidden, n_obs = w_in.shape[1], obs.shape[1]
    vmem = pltpu.VMEM
    return pl.pallas_call(
        functools.partial(solve_kernel, 1.0 / total),
        out_shape=(
            jax.ShapeDtypeStruct((1, rows), F32),
            jax.ShapeDtypeStruct((4, 2, 4, 4, 4, 8, rows), F32),
            jax.ShapeDtypeStruct((2, 4, 4, 2, 8, rows), F32),
            jax.ShapeDtypeStruct((rows, width), F32),
        ),
        in_specs=[pl.BlockSpec(memory_space=vmem)] * 13,
        out_specs=[pl.BlockSpec(memory_space=vmem)] * 4,
        scratch_shapes=[
            vmem((rows, width), F32),
            vmem((rows, rows), F32),
            vmem((rows, rows), jnp.int32),
            vmem((rows, width), F32),
            vmem((n_obs, rows, rows), jnp.int32),
            vmem((rows * n_obs, rows), F32),
            vmem((n_obs, rows, rows), F32),
            vmem((rows, rows), F32),
            vmem((width, (steps + 1) * rows), BF16),
            vmem((steps * rows, hidden), BF16),
            vmem((steps, rows, width), F32),
            vmem((steps * rows, hidden), BF16),
            vmem(((steps + 1) * rows, width), BF16),
            vmem((width, steps * rows), BF16),
            vmem((hidden, width), BF16),
            vmem((width, hidden), BF16),
            vmem((width, width), BF16),
            vmem((rows, width), F32),
            vmem((8, hidden), F32),
            vmem((8, width), F32),
        ],
        compiler_params=pltpu.CompilerParams(vmem_limit_bytes=58 * 1024 * 1024),
        name="solve",
    )(
        init, brown, step.reshape(1, -1), length.reshape(1, -1), obs, observed, w_in,
        b_in.reshape(1, -1), w_out, b_out.reshape(1, -1), dec, prior.reshape(1, -1), diff.reshape(1, -1),
    )


def on_device(
    init_state, brownian, step_size, lengths, obs_steps, observed,
    w_in, b_in, w_out, b_out, decoder, prior_rate, diffusion,
):
    total = init_state.shape[0] * lax.axis_size(BATCH_MP)
    share = w_in.shape[1]
    w_in_all = lax.all_gather(w_in, "mp", axis=1, tiled=True)
    w_out_all = lax.all_gather(w_out, "mp", axis=0, tiled=True)
    b_in_all = lax.all_gather(b_in, "mp", axis=0, tiled=True)
    elbo, big, small, grad_init = solve(
        total, init_state, brownian, step_size, lengths, obs_steps, observed,
        w_in_all, b_in_all, w_out_all, b_out, decoder, prior_rate, diffusion,
    )
    big, small = lax.psum((big, small), BATCH_MP)
    me = lax.axis_index("mp")
    own = lax.dynamic_index_in_dim(big, me, 2, keepdims=False)
    own = own.reshape(2, 2, 256, 128)
    own_in = jnp.concatenate([own[0, 0], own[0, 1]], axis=1)
    own_out = jnp.concatenate([own[1, 0], own[1, 1]], axis=1).T
    grad_dec = small[:, :, :, 0].reshape(256, 128)
    own_b = lax.dynamic_slice_in_dim(small[0, 0, 0, 1].reshape(-1), me * share, share, 0)
    tail = small[0, 0, 1, 1]
    return (
        elbo.reshape(-1), tail[2:4, 0], own_in, own_b, own_out, tail[0:2].reshape(-1), grad_dec, grad_init,
    )


def solution(mesh):
    torus = Mesh(
        mesh.devices.reshape(4, 4, 2, mesh.shape["mp"]), ("batch_0", "batch_1", "batch_2", "mp")
    )
    placed = (
        P(BATCH_MP, None), P(None, BATCH_MP, None), P(BATCH_MP), P(BATCH_MP), P(BATCH_MP, None),
        P(BATCH_MP, None, None), P(None, "mp"), P("mp"), P("mp", None), P(), P(), P(), P(),
    )
    return jax.shard_map(
        on_device,
        mesh=torus,
        in_specs=placed,
        out_specs=(
            P(BATCH_MP), P(), P(None, "mp"), P("mp"), P("mp", None), P(), P(), P(BATCH_MP, None),
        ),
        check_vma=False,
    )
```

```python
import functools

import jax
import jax.numpy as jnp
from jax import lax
from jax.experimental import pallas as pl
from jax.experimental.pallas import tpu as pltpu
from jax.sharding import Mesh
from jax.sharding import PartitionSpec as P

BATCH_MP = ("batch_0", "batch_1", "batch_2", "mp")
F32, BF16 = jnp.float32, jnp.bfloat16
UNROLL = 2


def mm(a, b):
    return jnp.dot(a, b, preferred_element_type=F32)


def twice(a):
    return jnp.concatenate([a, a], axis=1)


def solve_kernel(
    scale,
    init, brown, step, length, obs, observed, w_in, b_in, w_out, b_out, dec, prior, diff,
    elbo, big, small, ginit,
    state, stepb, lenb, dr, obsb, obsf, acc, klacc, traj_t, acts, scaled, pre, back, upd_t,
    w_in_t, w_out_t, dec_t, cot, sum_in, sum_out,
):
    steps, rows, width = brown.shape
    hidden = w_in.shape[1]
    n_obs = obs.shape[0]

    stepb[...] = jnp.broadcast_to(step[...], (rows, rows)).T
    lenb[...] = jnp.broadcast_to(length[...], (rows, rows)).T
    dr[...] = diff[...] * twice(jnp.sqrt(stepb[...]))
    for j in range(n_obs):
        obsb[j] = jnp.broadcast_to(obs[j : j + 1, :], (rows, rows)).T
    obsf[...] = observed[...].astype(F32).reshape(rows * n_obs, dec.shape[1])
    w_in_t[...] = w_in[...].T
    w_out_t[...] = w_out[...].T
    dec_flip = dec[...].T
    dec_t[...] = jnp.concatenate([dec_flip, dec_flip], axis=0)
    klacc[...] = jnp.zeros_like(klacc)
    acc[...] = jnp.zeros_like(acc)
    sum_in[...] = jnp.zeros_like(sum_in)
    sum_out[...] = jnp.zeros_like(sum_out)
    state[...] = init[...]
    bias = jnp.concatenate([b_in[m] for m in range(4)], axis=1).astype(F32)
    inv = 1.0 / diff[...]

    def see(k, rounded):
        seen = mm(rounded, dec[...])
        for j in range(n_obs):
            acc[j] = jnp.where(obsb[j] == k, seen, acc[j])

    def at(k):
        return pl.ds(pl.multiple_of(k * rows, rows), rows)

    def forward(k, carry):
        s = state[...]
        rounded = s.astype(BF16)
        activity = jnp.tanh(mm(rounded, w_in[...]) + bias).astype(BF16)
        drift = mm(activity, w_out[...]) + b_out[...]
        live = lenb[...] > k
        factor = jnp.where(live, stepb[...], 0.0)
        residual = (drift + prior[...] * s) * inv
        noise = dr[...] * brown[k].astype(F32)
        state[...] = s + twice(factor) * drift + jnp.where(twice(live), noise, 0.0)
        acts[at(k), :] = activity
        scaled[k] = residual * inv
        square = residual * residual
        klacc[...] += (0.5 * factor) * (square[:, :rows] + square[:, rows:])
        traj_t[:, at(k)] = rounded.T
        see(k, rounded)
        return carry

    lax.fori_loop(0, steps, forward, 0, unroll=UNROLL)
    last = state[...].astype(BF16)
    traj_t[:, at(steps)] = last.T
    see(steps, last)

    total = jnp.zeros((rows, rows), F32)
    for j in range(n_obs):
        misfit = acc[j] - obsf[pl.ds(j, rows, stride=n_obs), :]
        total = total + misfit * misfit
        acc[j] = misfit.astype(BF16).astype(F32)
    loglik = -0.5 * total
    divisor = (width * lenb[...] + rows * n_obs).astype(F32)
    per_series = jnp.sum(loglik - klacc[...], axis=1, keepdims=True) / divisor
    elbo[...] = per_series.T[0:1, :]

    def gathered(k):
        m = jnp.zeros((rows, rows), F32)
        for j in range(n_obs):
            m = m + jnp.where(obsb[j] == k, acc[j], 0.0)
        high = m.astype(BF16)
        low = (m - high.astype(F32)).astype(BF16)
        return jnp.concatenate([high, low], axis=1)

    final = gathered(steps)
    back[at(steps), :] = final
    cot[...] = mm(final, dec_t[...])

    def backward(i, carry):
        k = steps - 1 - i
        c = cot[...]
        factor = twice(jnp.where(lenb[...] > k, stepb[...], 0.0))
        part = scaled[k]
        update = factor * (c + part)
        rounded = update.astype(BF16)
        value = acts[at(k), :].astype(F32)
        pre_grad = mm(rounded, w_out_t[...]) * (1.0 - value * value)
        pre_round = pre_grad.astype(BF16)
        seen = gathered(k)
        cot[...] = (
            c + factor * prior[...] * part + (mm(pre_round, w_in_t[...]) + mm(seen, dec_t[...]))
        )
        pre[at(k), :] = pre_round
        back[at(k), :] = seen
        upd_t[:, at(k)] = rounded.T
        sum_in[...] += jnp.sum(pre_grad.reshape(rows // 8, 8, hidden), axis=0)
        sum_out[...] += jnp.sum(update.reshape(rows // 8, 8, width), axis=0)
        return carry

    lax.fori_loop(0, steps, backward, 0, unroll=UNROLL)
    ginit[...] = cot[...]

    def weights(n, carry):
        cols = pl.ds(pl.multiple_of(n * width, width), width)
        grad_in = mm(traj_t[:, : steps * rows], pre[:, cols]) * scale
        grad_out = mm(upd_t[...], acts[:, cols]) * scale
        for h in range(2):
            big[h, :, n] = grad_in[:, h * rows : (h + 1) * rows].reshape(2, 4, 4, 8, rows)
            big[2 + h, :, n] = grad_out[:, h * rows : (h + 1) * rows].reshape(2, 4, 4, 8, rows)
        return carry

    lax.fori_loop(0, hidden // width, weights, 0)
    grad_dec = mm(traj_t[...], back[...]) * scale
    small[...] = jnp.zeros_like(small)
    small[:, :, :, 0] = (grad_dec[:, :rows] + grad_dec[:, rows:]).reshape(2, 4, 4, 8, rows)
    row_in = jnp.sum(sum_in[...], axis=0, keepdims=True) * scale
    row_out = jnp.sum(sum_out[...], axis=0, keepdims=True) * scale
    for r in range(hidden // rows):
        small[0, 0, 0, 1, r : r + 1, :] = row_in[:, r * rows : (r + 1) * rows]
    for r in range(width // rows):
        small[0, 0, 1, 1, r : r + 1, :] = row_out[:, r * rows : (r + 1) * rows]
    for r, part in ((2, loglik), (3, klacc[...])):
        whole = jnp.sum(jnp.sum(part, axis=0, keepdims=True), axis=1, keepdims=True) * scale
        small[0, 0, 1, 1, r : r + 1, :] = jnp.broadcast_to(whole, (1, rows))


def solve(total, init, brown, step, length, obs, observed, w_in, b_in, w_out, b_out, dec, prior, diff):
    steps, rows, width = brown.shape
    hidden, n_obs = w_in.shape[1], obs.shape[1]
    vmem = pltpu.VMEM
    return pl.pallas_call(
        functools.partial(solve_kernel, 1.0 / total),
        out_shape=(
            jax.ShapeDtypeStruct((1, rows), F32),
            jax.ShapeDtypeStruct((4, 2, 4, 4, 4, 8, rows), F32),
            jax.ShapeDtypeStruct((2, 4, 4, 2, 8, rows), F32),
            jax.ShapeDtypeStruct((rows, width), F32),
        ),
        in_specs=[pl.BlockSpec(memory_space=vmem)] * 13,
        out_specs=[pl.BlockSpec(memory_space=vmem)] * 4,
        scratch_shapes=[
            vmem((rows, width), F32),
            vmem((rows, rows), F32),
            vmem((rows, rows), jnp.int32),
            vmem((rows, width), F32),
            vmem((n_obs, rows, rows), jnp.int32),
            vmem((rows * n_obs, rows), F32),
            vmem((n_obs, rows, rows), F32),
            vmem((rows, rows), F32),
            vmem((width, (steps + 1) * rows), BF16),
            vmem((steps * rows, hidden), BF16),
            vmem((steps, rows, width), F32),
            vmem((steps * rows, hidden), BF16),
            vmem(((steps + 1) * rows, width), BF16),
            vmem((width, steps * rows), BF16),
            vmem((hidden, width), BF16),
            vmem((width, hidden), BF16),
            vmem((width, width), BF16),
            vmem((rows, width), F32),
            vmem((8, hidden), F32),
            vmem((8, width), F32),
        ],
        compiler_params=pltpu.CompilerParams(vmem_limit_bytes=58 * 1024 * 1024),
        name="solve",
    )(
        init, brown, step.reshape(1, -1), length.reshape(1, -1), obs.T, observed, w_in,
        b_in, w_out, b_out.reshape(1, -1), dec, prior.reshape(1, -1), diff.reshape(1, -1),
    )


AXES = {"x": "mp", "y": "batch_0", "z": "batch_1", "c": "batch_2"}
LOGICAL = pl.DeviceIdType.MESH
ORDERS = ("xyz", "xyz", "yzx", "zxy")


def far(axis, where):
    return {AXES[axis]: where}


def remote(src, dst, send, recv, to):
    copy = pltpu.make_async_remote_copy(
        src_ref=src, dst_ref=dst, send_sem=send, recv_sem=recv, device_id=to, device_id_type=LOGICAL
    )
    copy.start()
    return copy


def meet(peers):
    barrier = pltpu.get_barrier_semaphore()
    for peer in peers:
        pl.semaphore_signal(barrier, inc=1, device_id=peer, device_id_type=LOGICAL)
    pl.semaphore_wait(barrier, len(peers))


def gather_kernel(w_in, w_out, b_in, wi, wo, bi, send, recv, bsend, brecv, psend, precv, local):
    me, core = lax.axis_index("mp"), lax.axis_index("batch_2")
    right, left, other = lax.rem(me + 1, 4), lax.rem(me + 3, 4), lax.rem(me + 2, 4)
    depth, share = w_in.shape
    half = depth // 2
    upper = pl.ds(pl.multiple_of(core * half, half), half)
    to_right, to_left, mate = far("x", right), far("x", left), far("c", 1 - core)
    meet((to_right, to_left, far("x", other), mate))

    def at_in(block):
        return wi.at[upper, pl.ds(pl.multiple_of(block * share, share), share)]

    def at_out(block):
        return wo.at[pl.ds(pl.multiple_of(block * share + core * half, half), half), :]

    own_in, own_out = w_in.at[upper, :], w_out.at[upper, :]
    in_r = remote(own_in, at_in(me), send.at[0], recv.at[0], to_right)
    out_l = remote(own_out, at_out(me), send.at[1], recv.at[1], to_left)
    out_r = remote(own_out, at_out(me), send.at[2], recv.at[2], to_right)
    in_l = remote(own_in, at_in(me), send.at[3], recv.at[3], to_left)
    biases = [
        remote(b_in, bi.at[me], bsend.at[d], brecv.at[d], far("x", lax.rem(me + d, 4)))
        for d in (1, 2, 3)
    ]
    kept = [
        pltpu.make_async_copy(w_in, wi.at[:, pl.ds(pl.multiple_of(me * share, share), share)], local.at[0]),
        pltpu.make_async_copy(w_out, wo.at[pl.ds(pl.multiple_of(me * share, share), share), :], local.at[1]),
        pltpu.make_async_copy(b_in, bi.at[me], local.at[2]),
    ]
    for copy in kept:
        copy.start()
    sent = []

    def share_with_mate(n, ref):
        sent.append(remote(ref, ref, psend.at[n], precv.at[n], mate))

    in_r.wait_recv()
    in_rr = remote(at_in(left), at_in(left), send.at[4], recv.at[4], to_right)
    share_with_mate(0, at_in(left))
    out_l.wait_recv()
    out_ll = remote(at_out(right), at_out(right), send.at[5], recv.at[5], to_left)
    share_with_mate(1, at_out(right))
    out_r.wait_recv()
    share_with_mate(2, at_out(left))
    in_l.wait_recv()
    share_with_mate(3, at_in(right))
    in_rr.wait_recv()
    share_with_mate(4, at_in(other))
    out_ll.wait_recv()
    share_with_mate(5, at_out(other))
    for copy in kept:
        copy.wait()
    for copy in biases + sent:
        copy.wait()
    for copy in (in_r, out_l, out_r, in_l, in_rr, out_ll):
        copy.wait_send()


def gather(w_in, w_out, b_in):
    depth, share = w_in.shape
    vmem, dma = pltpu.VMEM, pltpu.SemaphoreType.DMA
    return pl.pallas_call(
        gather_kernel,
        out_shape=(
            jax.ShapeDtypeStruct((depth, 4 * share), BF16),
            jax.ShapeDtypeStruct((4 * share, depth), BF16),
            jax.ShapeDtypeStruct((4, 1, share), BF16),
        ),
        in_specs=[pl.BlockSpec(memory_space=vmem)] * 3,
        out_specs=[pl.BlockSpec(memory_space=vmem)] * 3,
        scratch_shapes=[dma((6,)), dma((6,)), dma((4,)), dma((4,)), dma((6,)), dma((6,)), dma((3,))],
        compiler_params=pltpu.CompilerParams(collective_id=0, has_side_effects=True),
        name="gather",
    )(w_in, w_out, b_in.reshape(1, -1))


def reduce_kernel(
    big, small, out,
    got, cur, small_got, small_cur, r1, r2, r3, s1, s2, sx, fin,
    dsend, drecv, send, recv, gsend, grecv, hsend, hrecv,
):
    place = {a: lax.axis_index(AXES[a]) for a in "xyzc"}
    core = place["c"]
    mate = far("c", 1 - core)

    def other(axis, d):
        return lax.rem(place[axis] + d, 4)

    plane = [(dy, dz) for dy in range(4) for dz in range(4) if (dy, dz) != (0, 0)]

    def in_plane(dy, dz):
        return {AXES["y"]: other("y", dy), AXES["z"]: other("z", dz)}

    peers = [mate] + [far("x", other("x", d)) for d in (1, 2, 3)] + [in_plane(*p) for p in plane]
    meet(peers)

    pending = []
    first = [remote(big.at[u, 1 - core], got.at[u], dsend.at[u], drecv.at[u], mate) for u in range(4)]
    first.append(remote(small.at[1 - core], small_got, dsend.at[4], drecv.at[4], mate))
    pending += first

    boxes = (r1, r2, r3)

    def pick(ref, dims, axis, index):
        return ref.at[tuple(index if a == axis else slice(None) for a in dims)]

    def start(flow, stage, ref, dims, axis, box):
        copies = []
        for d in (1, 2, 3):
            n = (flow * 3 + stage) * 3 + d - 1
            copies.append(
                remote(
                    pick(ref, dims, axis, other(axis, d)), box.at[d - 1], send.at[n], recv.at[n],
                    far(axis, other(axis, d)),
                )
            )
        pending.extend(copies)
        return copies

    def finish(copies, ref, dims, axis, box):
        for copy in copies:
            copy.wait_recv()
        mine = pick(ref, dims, axis, place[axis])[...]
        return mine + box[0] + box[1] + box[2]

    flying = {}
    for u in (2, 3, 0, 1):
        first[u].wait_recv()
        cur[u] = big[u, core] + got[u]
        flying[u] = start(u, 0, cur.at[u], "xyz", ORDERS[u][0], r1.at[u])
    first[4].wait_recv()
    small_cur[...] = small[core] + small_got[...]
    flying[4] = start(4, 0, small_cur, "yz", "y", s1)

    s = finish(flying[4], small_cur, "yz", "y", s1)
    small_got[0] = s
    flying[4] = start(4, 1, small_got.at[0], "z", "z", s2)
    for u in (2, 3, 0, 1):
        axis = ORDERS[u][0]
        got[u, 0] = finish(flying[u], cur.at[u], "xyz", axis, r1.at[u])
        dims = "xyz".replace(axis, "")
        flying[u] = start(u, 1, got.at[u, 0], dims, ORDERS[u][1], r2.at[u])
    s = finish(flying[4], small_got.at[0], "z", "z", s2)
    small_got[1, 0] = s
    xs = []
    for d in (1, 2, 3):
        n = (4 * 3 + 2) * 3 + d - 1
        xs.append(remote(small_got.at[1, 0], sx.at[place["x"]], send.at[n], recv.at[n], far("x", other("x", d))))
    pending.extend(xs)
    sx[place["x"]] = s
    for u in (2, 3, 0, 1):
        axis = ORDERS[u][1]
        dims = "xyz".replace(ORDERS[u][0], "")
        got[u, 1, 0] = finish(flying[u], got.at[u, 0], dims, axis, r2.at[u])
        flying[u] = start(u, 2, got.at[u, 1, 0], ORDERS[u][2], ORDERS[u][2], r3.at[u])
    for copy in xs:
        copy.wait_recv()
    fin[4:6] = sx[0] + sx[1] + sx[2] + sx[3]
    for u in (2, 3, 0, 1):
        fin[u] = finish(flying[u], got.at[u, 1, 0], ORDERS[u][2], ORDERS[u][2], r3.at[u])

    home = out.at[core, place["y"], place["z"]]
    spread = []
    for n, (dy, dz) in enumerate(plane):
        spread.append(remote(fin, home, gsend.at[n], grecv.at[n], in_plane(dy, dz)))
    pair = [remote(fin, home, hsend.at[15], hrecv.at[15], mate)]
    out[core, place["y"], place["z"]] = fin[...]
    for n, (dy, dz) in enumerate(plane):
        spread[n].wait_recv()
        came = out.at[core, lax.rem(place["y"] + 4 - dy, 4), lax.rem(place["z"] + 4 - dz, 4)]
        pair.append(remote(came, came, hsend.at[n], hrecv.at[n], mate))
    for copy in pair:
        copy.wait()
    for copy in pending + spread:
        copy.wait_send()


def reduce(big, small):
    vmem, dma = pltpu.VMEM, pltpu.SemaphoreType.DMA
    tile = (8, 128)
    return pl.pallas_call(
        reduce_kernel,
        out_shape=jax.ShapeDtypeStruct((2, 4, 4, 6) + tile, F32),
        in_specs=[pl.BlockSpec(memory_space=vmem)] * 2,
        out_specs=pl.BlockSpec(memory_space=vmem),
        scratch_shapes=[
            vmem((4, 4, 4, 4) + tile, F32),
            vmem((4, 4, 4, 4) + tile, F32),
            vmem((4, 4, 2) + tile, F32),
            vmem((4, 4, 2) + tile, F32),
            vmem((4, 3, 4, 4) + tile, F32),
            vmem((4, 3, 4) + tile, F32),
            vmem((4, 3) + tile, F32),
            vmem((3, 4, 2) + tile, F32),
            vmem((3, 2) + tile, F32),
            vmem((4, 2) + tile, F32),
            vmem((6,) + tile, F32),
            dma((5,)), dma((5,)), dma((45,)), dma((45,)), dma((15,)), dma((15,)), dma((16,)), dma((16,)),
        ],
        compiler_params=pltpu.CompilerParams(
            collective_id=1, has_side_effects=True, vmem_limit_bytes=24 * 1024 * 1024
        ),
        name="reduce",
    )(big, small)


def finish_kernel(out, w_in, w_out, dec, b_in, b_out, scores):
    me = lax.axis_index("mp")

    def whole(u):
        return out[:, :, :, u].reshape(256, 128)

    w_in[:, :128] = whole(0)
    w_in[:, 128:] = whole(1)
    w_out[:128, :] = whole(2).T
    w_out[128:, :] = whole(3).T
    dec[...] = whole(4)
    for r in range(2):
        b_in[:, r * 128 : (r + 1) * 128] = out[0, 0, 0, 5, pl.ds(2 * me + r, 1), :]
        b_out[:, r * 128 : (r + 1) * 128] = out[0, 0, 1, 5, r : r + 1, :]
    scores[...] = out[0, 0, 1, 5, 2:4, :]


def unpack(out):
    vmem = pltpu.VMEM
    return pl.pallas_call(
        finish_kernel,
        out_shape=tuple(
            jax.ShapeDtypeStruct(s, F32)
            for s in ((256, 256), (256, 256), (256, 128), (1, 256), (1, 256), (2, 128))
        ),
        in_specs=[pl.BlockSpec(memory_space=vmem)],
        out_specs=[pl.BlockSpec(memory_space=vmem)] * 6,
        name="unpack",
    )(out)


def on_device(
    init_state, brownian, step_size, lengths, obs_steps, observed,
    w_in, b_in, w_out, b_out, decoder, prior_rate, diffusion,
):
    total = init_state.shape[0] * lax.axis_size(BATCH_MP)
    w_in_all, w_out_all, b_in_all = gather(w_in, w_out, b_in)
    elbo, big, small, grad_init = solve(
        total, init_state, brownian, step_size, lengths, obs_steps, observed,
        w_in_all, b_in_all, w_out_all, b_out, decoder, prior_rate, diffusion,
    )
    own_in, own_out, grad_dec, own_b, grad_b_out, scores = unpack(reduce(big, small))
    return (
        elbo.reshape(-1), scores[:, 0], own_in, own_b.reshape(-1), own_out, grad_b_out.reshape(-1),
        grad_dec, grad_init,
    )


def solution(mesh):
    torus = Mesh(
        mesh.devices.reshape(4, 4, 2, mesh.shape["mp"]), ("batch_0", "batch_1", "batch_2", "mp")
    )
    placed = (
        P(BATCH_MP, None), P(None, BATCH_MP, None), P(BATCH_MP), P(BATCH_MP), P(BATCH_MP, None),
        P(BATCH_MP, None, None), P(None, "mp"), P("mp"), P("mp", None), P(), P(), P(), P(),
    )
    return jax.shard_map(
        on_device,
        mesh=torus,
        in_specs=placed,
        out_specs=(
            P(BATCH_MP), P(), P(None, "mp"), P("mp"), P("mp", None), P(), P(), P(BATCH_MP, None),
        ),
        check_vma=False,
    )
```

```python
import functools

import jax
import jax.numpy as jnp
from jax import lax
from jax.experimental import pallas as pl
from jax.experimental.pallas import tpu as pltpu
from jax.sharding import Mesh
from jax.sharding import PartitionSpec as P

BATCH_MP = ("batch_0", "batch_1", "batch_2", "mp")
F32, BF16 = jnp.float32, jnp.bfloat16
UNROLL = 2


def mm(a, b):
    return jnp.dot(a, b, preferred_element_type=F32)


def twice(a):
    return jnp.concatenate([a, a], axis=1)


AXES = {"x": "mp", "y": "batch_0", "z": "batch_1", "c": "batch_2"}
LOGICAL = pl.DeviceIdType.MESH
ORDERS = ("xyz", "xyz", "yzx", "zxy")


def far(axis, where):
    return {AXES[axis]: where}


def remote(src, dst, send, recv, to):
    copy = pltpu.make_async_remote_copy(
        src_ref=src, dst_ref=dst, send_sem=send, recv_sem=recv, device_id=to, device_id_type=LOGICAL
    )
    copy.start()
    return copy


def meet(peers):
    barrier = pltpu.get_barrier_semaphore()
    for peer in peers:
        pl.semaphore_signal(barrier, inc=1, device_id=peer, device_id_type=LOGICAL)
    pl.semaphore_wait(barrier, len(peers))


def whole_kernel(
    scale,
    init, brown_hbm, step, length, obs, observed_hbm, w_in, b_in, w_out, b_out, dec, prior, diff,
    elbo, out, ginit,
    wi, wo, bi, brown, observed,
    state, stepb, lenb, dr, obsb, obsf, acc, klacc, traj_t, acts, scaled, pre, back, upd_t,
    w_in_t, w_out_t, dec_t, cot, sum_in, sum_out,
    big, small, got, cur, small_got, small_cur, r1, r2, r3, s1, s2, sx, fin,
    wsend, wrecv, bsend, brecv, psend, precv, local,
    dsend, drecv, send, recv, gsend, grecv, hsend, hrecv,
):
    steps, rows, width = brown.shape
    hidden = wi.shape[1]
    n_obs = obs.shape[0]
    loads = [
        pltpu.make_async_copy(observed_hbm, observed, local.at[3]),
        pltpu.make_async_copy(brown_hbm, brown, local.at[4]),
    ]
    for copy in loads:
        copy.start()

    place = {a: lax.axis_index(AXES[a]) for a in "xyzc"}
    me, core = place["x"], place["c"]
    mate = far("c", 1 - core)

    def other(axis, d):
        return lax.rem(place[axis] + d, 4)

    plane = [(dy, dz) for dy in range(4) for dz in range(4) if (dy, dz) != (0, 0)]

    def in_plane(dy, dz):
        return {AXES["y"]: other("y", dy), AXES["z"]: other("z", dz)}

    meet([mate] + [far("x", other("x", d)) for d in (1, 2, 3)] + [in_plane(*p) for p in plane])

    right, left, across = other("x", 1), other("x", 3), other("x", 2)
    depth, share = w_in.shape
    half = depth // 2
    upper = pl.ds(pl.multiple_of(core * half, half), half)
    to_right, to_left = far("x", right), far("x", left)

    def at_in(block):
        return wi.at[upper, pl.ds(pl.multiple_of(block * share, share), share)]

    def at_out(block):
        return wo.at[pl.ds(pl.multiple_of(block * share + core * half, half), half), :]

    own_in, own_out = w_in.at[upper, :], w_out.at[upper, :]
    in_r = remote(own_in, at_in(me), wsend.at[0], wrecv.at[0], to_right)
    out_l = remote(own_out, at_out(me), wsend.at[1], wrecv.at[1], to_left)
    out_r = remote(own_out, at_out(me), wsend.at[2], wrecv.at[2], to_right)
    in_l = remote(own_in, at_in(me), wsend.at[3], wrecv.at[3], to_left)
    biases = [
        remote(b_in, bi.at[me], bsend.at[d], brecv.at[d], far("x", other("x", d))) for d in (1, 2, 3)
    ]
    kept = [
        pltpu.make_async_copy(w_in, wi.at[:, pl.ds(pl.multiple_of(me * share, share), share)], local.at[0]),
        pltpu.make_async_copy(w_out, wo.at[pl.ds(pl.multiple_of(me * share, share), share), :], local.at[1]),
        pltpu.make_async_copy(b_in, bi.at[me], local.at[2]),
    ]
    for copy in kept:
        copy.start()

    stepb[...] = jnp.broadcast_to(step[...], (rows, rows)).T
    lenb[...] = jnp.broadcast_to(length[...], (rows, rows)).T
    dr[...] = diff[...] * twice(jnp.sqrt(stepb[...]))
    for j in range(n_obs):
        obsb[j] = jnp.broadcast_to(obs[j : j + 1, :], (rows, rows)).T
    dec_flip = dec[...].T
    dec_t[...] = jnp.concatenate([dec_flip, dec_flip], axis=0)
    klacc[...] = jnp.zeros_like(klacc)
    acc[...] = jnp.zeros_like(acc)
    sum_in[...] = jnp.zeros_like(sum_in)
    sum_out[...] = jnp.zeros_like(sum_out)
    small[...] = jnp.zeros_like(small)
    state[...] = init[...]
    inv = 1.0 / diff[...]
    loads[0].wait()
    obsf[...] = observed[...].astype(F32).reshape(rows * n_obs, dec.shape[1])

    sent = []

    def share_with_mate(n, ref):
        sent.append(remote(ref, ref, psend.at[n], precv.at[n], mate))

    in_r.wait_recv()
    in_rr = remote(at_in(left), at_in(left), wsend.at[4], wrecv.at[4], to_right)
    share_with_mate(0, at_in(left))
    out_l.wait_recv()
    out_ll = remote(at_out(right), at_out(right), wsend.at[5], wrecv.at[5], to_left)
    share_with_mate(1, at_out(right))
    out_r.wait_recv()
    share_with_mate(2, at_out(left))
    in_l.wait_recv()
    share_with_mate(3, at_in(right))
    in_rr.wait_recv()
    share_with_mate(4, at_in(across))
    out_ll.wait_recv()
    share_with_mate(5, at_out(across))
    for copy in kept:
        copy.wait()
    for copy in biases + sent:
        copy.wait()
    for copy in (in_r, out_l, out_r, in_l, in_rr, out_ll):
        copy.wait_send()

    w_in_t[...] = wi[...].T
    w_out_t[...] = wo[...].T
    bias = jnp.concatenate([bi[m] for m in range(4)], axis=1).astype(F32)
    loads[1].wait()

    def see(k, rounded):
        seen = mm(rounded, dec[...])
        for j in range(n_obs):
            acc[j] = jnp.where(obsb[j] == k, seen, acc[j])

    def at(k):
        return pl.ds(pl.multiple_of(k * rows, rows), rows)

    def forward(k, carry):
        s = state[...]
        rounded = s.astype(BF16)
        drift = b_out[...]
        for n in range(0, hidden, width):
            cs = slice(n, n + width)
            activity = jnp.tanh(mm(rounded, wi[:, cs]) + bias[:, cs]).astype(BF16)
            acts[at(k), cs] = activity
            drift = drift + mm(activity, wo[cs, :])
        live = lenb[...] > k
        factor = jnp.where(live, stepb[...], 0.0)
        residual = (drift + prior[...] * s) * inv
        noise = dr[...] * brown[k].astype(F32)
        state[...] = s + twice(factor) * drift + jnp.where(twice(live), noise, 0.0)
        scaled[k] = residual * inv
        square = residual * residual
        klacc[...] += (0.5 * factor) * (square[:, :rows] + square[:, rows:])
        traj_t[:, at(k)] = rounded.T
        see(k, rounded)
        return carry

    lax.fori_loop(0, steps, forward, 0, unroll=UNROLL)
    last = state[...].astype(BF16)
    traj_t[:, at(steps)] = last.T
    see(steps, last)

    total = jnp.zeros((rows, rows), F32)
    for j in range(n_obs):
        misfit = acc[j] - obsf[pl.ds(j, rows, stride=n_obs), :]
        total = total + misfit * misfit
        acc[j] = misfit.astype(BF16).astype(F32)
    loglik = -0.5 * total
    divisor = (width * lenb[...] + rows * n_obs).astype(F32)
    per_series = jnp.sum(loglik - klacc[...], axis=1, keepdims=True) / divisor
    elbo[...] = per_series.T[0:1, :]

    def gathered(k):
        m = jnp.zeros((rows, rows), F32)
        for j in range(n_obs):
            m = m + jnp.where(obsb[j] == k, acc[j], 0.0)
        high = m.astype(BF16)
        low = (m - high.astype(F32)).astype(BF16)
        return jnp.concatenate([high, low], axis=1)

    final = gathered(steps)
    back[at(steps), :] = final
    cot[...] = mm(final, dec_t[...])

    def backward(i, carry):
        k = steps - 1 - i
        c = cot[...]
        factor = twice(jnp.where(lenb[...] > k, stepb[...], 0.0))
        part = scaled[k]
        update = factor * (c + part)
        rounded = update.astype(BF16)
        value = acts[at(k), :].astype(F32)
        pre_grad = mm(rounded, w_out_t[...]) * (1.0 - value * value)
        pre_round = pre_grad.astype(BF16)
        seen = gathered(k)
        cot[...] = (
            c + factor * prior[...] * part + (mm(pre_round, w_in_t[...]) + mm(seen, dec_t[...]))
        )
        pre[at(k), :] = pre_round
        back[at(k), :] = seen
        upd_t[:, at(k)] = rounded.T
        sum_in[...] += jnp.sum(pre_grad.reshape(rows // 8, 8, hidden), axis=0)
        sum_out[...] += jnp.sum(update.reshape(rows // 8, 8, width), axis=0)
        return carry

    lax.fori_loop(0, steps, backward, 0, unroll=UNROLL)
    ginit[...] = cot[...]

    pending = []
    first = {}
    flying = {}

    def pick(ref, dims, axis, index):
        return ref.at[tuple(index if a == axis else slice(None) for a in dims)]

    def hop(flow, stage, d, src, box, axis):
        n = (flow * 3 + stage) * 3 + d - 1
        copy = remote(src, box.at[d - 1], send.at[n], recv.at[n], far(axis, other(axis, d)))
        pending.append(copy)
        flying.setdefault((flow, stage), []).append(copy)

    def start(flow, stage, ref, dims, axis, box):
        for d in (2, 1, 3):
            hop(flow, stage, d, pick(ref, dims, axis, other(axis, d)), box, axis)

    def finish(flow, stage, ref, dims, axis, box):
        for copy in flying[flow, stage]:
            copy.wait_recv()
        mine = pick(ref, dims, axis, place[axis])[...]
        return mine + box[0] + box[1] + box[2]

    def to_mate(n, src, dst):
        copy = remote(src, dst, dsend.at[n], drecv.at[n], mate)
        pending.append(copy)
        return copy

    def grads(d, base, left_ref, right_ref):
        n = other("x", d)
        cols = pl.ds(pl.multiple_of(n * width, width), width)
        grad = mm(left_ref[:, : steps * rows], right_ref[:, cols]) * scale
        for h in range(2):
            u = base + h
            big[u, :, n] = grad[:, h * rows : (h + 1) * rows].reshape(2, 4, 4, 8, rows)
        for h in range(2):
            u = base + h
            first[u, d] = to_mate(u * 4 + d, big.at[u, 1 - core, n], got.at[u, n])

    for d in (2, 1, 3, 0):
        grads(d, 0, traj_t, pre)

    grad_dec = mm(traj_t[...], back[...]) * scale
    small[:, :, :, 0] = (grad_dec[:, :rows] + grad_dec[:, rows:]).reshape(2, 4, 4, 8, rows)
    row_in = jnp.sum(sum_in[...], axis=0, keepdims=True) * scale
    row_out = jnp.sum(sum_out[...], axis=0, keepdims=True) * scale
    for r in range(hidden // rows):
        small[0, 0, 0, 1, r : r + 1, :] = row_in[:, r * rows : (r + 1) * rows]
    for r in range(width // rows):
        small[0, 0, 1, 1, r : r + 1, :] = row_out[:, r * rows : (r + 1) * rows]
    for r, part in ((2, loglik), (3, klacc[...])):
        total = jnp.sum(jnp.sum(part, axis=0, keepdims=True), axis=1, keepdims=True) * scale
        small[0, 0, 1, 1, r : r + 1, :] = jnp.broadcast_to(total, (1, rows))
    first[4] = to_mate(16, small.at[1 - core], small_got)

    for d in (2, 1, 3, 0):
        grads(d, 2, upd_t, acts)
        n = other("x", d)
        for u in (0, 1):
            first[u, d].wait_recv()
            cur[u, n] = big[u, core, n] + got[u, n]
            if d:
                hop(u, 0, d, cur.at[u, n], r1.at[u], "x")
    first[4].wait_recv()
    small_cur[...] = small[core] + small_got[...]
    start(4, 0, small_cur, "yz", "y", s1)
    for u in (2, 3):
        for d in (2, 1, 3, 0):
            first[u, d].wait_recv()
        cur[u] = big[u, core] + got[u]
        start(u, 0, cur.at[u], "xyz", ORDERS[u][0], r1.at[u])

    small_got[0] = finish(4, 0, small_cur, "yz", "y", s1)
    start(4, 1, small_got.at[0], "z", "z", s2)
    for u in (0, 1, 2, 3):
        axis = ORDERS[u][0]
        got[u, 0] = finish(u, 0, cur.at[u], "xyz", axis, r1.at[u])
        dims = "xyz".replace(axis, "")
        start(u, 1, got.at[u, 0], dims, ORDERS[u][1], r2.at[u])
    s = finish(4, 1, small_got.at[0], "z", "z", s2)
    small_got[1, 0] = s
    for d in (1, 2, 3):
        n = (4 * 3 + 2) * 3 + d - 1
        copy = remote(small_got.at[1, 0], sx.at[me], send.at[n], recv.at[n], far("x", other("x", d)))
        pending.append(copy)
        flying.setdefault((4, 2), []).append(copy)
    sx[me] = s
    for u in (0, 1, 2, 3):
        axis = ORDERS[u][1]
        dims = "xyz".replace(ORDERS[u][0], "")
        got[u, 1, 0] = finish(u, 1, got.at[u, 0], dims, axis, r2.at[u])
        start(u, 2, got.at[u, 1, 0], ORDERS[u][2], ORDERS[u][2], r3.at[u])
    for copy in flying[4, 2]:
        copy.wait_recv()
    fin[4:6] = sx[0] + sx[1] + sx[2] + sx[3]
    for u in (0, 1, 2, 3):
        fin[u] = finish(u, 2, got.at[u, 1, 0], ORDERS[u][2], ORDERS[u][2], r3.at[u])

    home = out.at[core, place["y"], place["z"]]
    spread = []
    for n, (dy, dz) in enumerate(plane):
        spread.append(remote(fin, home, gsend.at[n], grecv.at[n], in_plane(dy, dz)))
    pair = [remote(fin, home, hsend.at[15], hrecv.at[15], mate)]
    out[core, place["y"], place["z"]] = fin[...]
    for n, (dy, dz) in enumerate(plane):
        spread[n].wait_recv()
        came = out.at[core, lax.rem(place["y"] + 4 - dy, 4), lax.rem(place["z"] + 4 - dz, 4)]
        pair.append(remote(came, came, hsend.at[n], hrecv.at[n], mate))
    for copy in pair:
        copy.wait()
    for copy in pending + spread:
        copy.wait_send()


def whole(total, init, brown, step, length, obs, observed, w_in, b_in, w_out, b_out, dec, prior, diff):
    steps, rows, width = brown.shape
    hidden, n_obs = 4 * w_in.shape[1], obs.shape[1]
    vmem, dma = pltpu.VMEM, pltpu.SemaphoreType.DMA
    near, rest = pl.BlockSpec(memory_space=vmem), pl.BlockSpec(memory_space=pl.ANY)
    tile = (8, 128)
    return pl.pallas_call(
        functools.partial(whole_kernel, 1.0 / total),
        out_shape=(
            jax.ShapeDtypeStruct((1, rows), F32),
            jax.ShapeDtypeStruct((2, 4, 4, 6) + tile, F32),
            jax.ShapeDtypeStruct((rows, width), F32),
        ),
        in_specs=[near, rest, near, near, near, rest] + [near] * 7,
        out_specs=[near] * 3,
        scratch_shapes=[
            vmem((width, hidden), BF16),
            vmem((hidden, width), BF16),
            vmem((4, 1, width), BF16),
            vmem(brown.shape, BF16),
            vmem(observed.shape, BF16),
            vmem((rows, width), F32),
            vmem((rows, rows), F32),
            vmem((rows, rows), jnp.int32),
            vmem((rows, width), F32),
            vmem((n_obs, rows, rows), jnp.int32),
            vmem((rows * n_obs, rows), F32),
            vmem((n_obs, rows, rows), F32),
            vmem((rows, rows), F32),
            vmem((width, (steps + 1) * rows), BF16),
            vmem((steps * rows, hidden), BF16),
            vmem((steps, rows, width), F32),
            vmem((steps * rows, hidden), BF16),
            vmem(((steps + 1) * rows, width), BF16),
            vmem((width, steps * rows), BF16),
            vmem((hidden, width), BF16),
            vmem((width, hidden), BF16),
            vmem((width, width), BF16),
            vmem((rows, width), F32),
            vmem((8, hidden), F32),
            vmem((8, width), F32),
            vmem((4, 2, 4, 4, 4) + tile, F32),
            vmem((2, 4, 4, 2) + tile, F32),
            vmem((4, 4, 4, 4) + tile, F32),
            vmem((4, 4, 4, 4) + tile, F32),
            vmem((4, 4, 2) + tile, F32),
            vmem((4, 4, 2) + tile, F32),
            vmem((4, 3, 4, 4) + tile, F32),
            vmem((4, 3, 4) + tile, F32),
            vmem((4, 3) + tile, F32),
            vmem((3, 4, 2) + tile, F32),
            vmem((3, 2) + tile, F32),
            vmem((4, 2) + tile, F32),
            vmem((6,) + tile, F32),
            dma((6,)), dma((6,)), dma((4,)), dma((4,)), dma((6,)), dma((6,)), dma((5,)),
            dma((17,)), dma((17,)), dma((45,)), dma((45,)), dma((15,)), dma((15,)), dma((16,)), dma((16,)),
        ],
        compiler_params=pltpu.CompilerParams(
            collective_id=0, has_side_effects=True, vmem_limit_bytes=58 * 1024 * 1024
        ),
        name="whole",
    )(
        init, brown, step.reshape(1, -1), length.reshape(1, -1), obs.T, observed, w_in,
        b_in.reshape(1, -1), w_out, b_out.reshape(1, -1), dec, prior.reshape(1, -1), diff.reshape(1, -1),
    )


def finish_kernel(elbo_in, out, ginit_in, elbo, w_in, w_out, dec, b_in, b_out, scores, ginit):
    me = lax.axis_index("mp")

    def gathered(u):
        return out[:, :, :, u].reshape(256, 128)

    elbo[...] = elbo_in[...]
    ginit[...] = ginit_in[...]
    w_in[:, :128] = gathered(0)
    w_in[:, 128:] = gathered(1)
    w_out[:128, :] = gathered(2).T
    w_out[128:, :] = gathered(3).T
    dec[...] = gathered(4)
    for r in range(2):
        b_in[:, r * 128 : (r + 1) * 128] = out[0, 0, 0, 5, pl.ds(2 * me + r, 1), :]
        b_out[:, r * 128 : (r + 1) * 128] = out[0, 0, 1, 5, r : r + 1, :]
    first = lax.broadcasted_iota(jnp.int32, (1, 128), 1) == 0
    both = jnp.where(first, out[0, 0, 1, 5, 2:3, :], out[0, 0, 1, 5, 3:4, :])
    scores[...] = both[:, :2]


def unpack(elbo, out, ginit):
    vmem = pltpu.VMEM
    return pl.pallas_call(
        finish_kernel,
        out_shape=tuple(
            jax.ShapeDtypeStruct(s, F32)
            for s in ((1, 128), (256, 256), (256, 256), (256, 128), (1, 256), (1, 256), (1, 2), (128, 256))
        ),
        in_specs=[pl.BlockSpec(memory_space=vmem)] * 3,
        out_specs=[pl.BlockSpec(memory_space=vmem)] * 8,
        name="unpack",
    )(elbo, out, ginit)


def on_device(
    init_state, brownian, step_size, lengths, obs_steps, observed,
    w_in, b_in, w_out, b_out, decoder, prior_rate, diffusion,
):
    total = init_state.shape[0] * lax.axis_size(BATCH_MP)
    elbo, parts, grad_init = whole(
        total, init_state, brownian, step_size, lengths, obs_steps, observed,
        w_in, b_in, w_out, b_out, decoder, prior_rate, diffusion,
    )
    elbo, own_in, own_out, grad_dec, own_b, grad_b_out, scores, grad_init = unpack(elbo, parts, grad_init)
    return (
        elbo.reshape(-1), scores.reshape(-1), own_in, own_b.reshape(-1), own_out, grad_b_out.reshape(-1),
        grad_dec, grad_init,
    )


def solution(mesh):
    torus = Mesh(
        mesh.devices.reshape(4, 4, 2, mesh.shape["mp"]), ("batch_0", "batch_1", "batch_2", "mp")
    )
    placed = (
        P(BATCH_MP, None), P(None, BATCH_MP, None), P(BATCH_MP), P(BATCH_MP), P(BATCH_MP, None),
        P(BATCH_MP, None, None), P(None, "mp"), P("mp"), P("mp", None), P(), P(), P(), P(),
    )
    return jax.shard_map(
        on_device,
        mesh=torus,
        in_specs=placed,
        out_specs=(
            P(BATCH_MP), P(), P(None, "mp"), P("mp"), P("mp", None), P(), P(), P(BATCH_MP, None),
        ),
        check_vma=False,
    )
```

```python
import functools
import itertools

import jax
import jax.numpy as jnp
from jax import lax
from jax.experimental import pallas as pl
from jax.experimental.pallas import tpu as pltpu
from jax.sharding import Mesh
from jax.sharding import PartitionSpec as P

BATCH_MP = ("batch_0", "batch_1", "batch_2", "mp")
F32, BF16 = jnp.float32, jnp.bfloat16
UNROLL = 4


def mm(a, b):
    return jnp.dot(a, b, preferred_element_type=F32)


def twice(a):
    return jnp.concatenate([a, a], axis=1)


AXES = {"x": "mp", "y": "batch_0", "z": "batch_1", "c": "batch_2"}
LOGICAL = pl.DeviceIdType.MESH
FIRST = "xxyz"
COPIES = 144


def pack(tiles):
    rows, marks = [], []
    for tile in tiles:
        top = jnp.max(jnp.max(jnp.abs(tile), axis=0, keepdims=True), axis=1, keepdims=True)
        power = jnp.ceil(jnp.log2(jnp.maximum(top, 1e-30) * (1.0 / 32000.0)))
        rows.append(jnp.floor(tile * jnp.exp2(-power) + 0.5))
        marks.append(jnp.broadcast_to(power, (1, 128)))
    marks.append(jnp.zeros((3, 128), F32))
    return jnp.concatenate(rows + marks, axis=0).astype(jnp.int32).astype(jnp.int16)


def far(axis, where):
    return {AXES[axis]: where}


def remote(src, dst, send, recv, to):
    copy = pltpu.make_async_remote_copy(
        src_ref=src, dst_ref=dst, send_sem=send, recv_sem=recv, device_id=to, device_id_type=LOGICAL
    )
    copy.start()
    return copy


def meet(peers):
    barrier = pltpu.get_barrier_semaphore()
    for peer in peers:
        pl.semaphore_signal(barrier, inc=1, device_id=peer, device_id_type=LOGICAL)
    pl.semaphore_wait(barrier, len(peers))


def whole_kernel(
    scale,
    init, brown_hbm, step, length, obs, observed_hbm, w_in, b_in, w_out, b_out, dec, prior, diff,
    elbo, out, tiny_out, ginit,
    wi, wo, bi, brown, observed,
    state, stepb, lenb, dr, obsb, obsf, acc, klacc, traj_t, acts, scaled, pre, back, upd_t,
    w_in_t, w_out_t, dec_t, cot, ob, sum_in, sum_out,
    big, small, tiny, got, cur, mid, r1, r2, small_got, small_cur, s1, s2, tiny_got, tiny_cur, t1, t2, packed,
    wsend, wrecv, bsend, brecv, psend, precv, local, send, recv,
):
    steps, rows, width = brown.shape
    hidden = wi.shape[1]
    n_obs = obs.shape[0]
    loads = [
        pltpu.make_async_copy(observed_hbm, observed, local.at[3]),
        pltpu.make_async_copy(brown_hbm, brown, local.at[4]),
    ]
    for copy in loads:
        copy.start()

    place = {a: lax.axis_index(AXES[a]) for a in "xyzc"}
    me, core = place["x"], place["c"]
    mate = far("c", 1 - core)

    def other(axis, d):
        return lax.rem(place[axis] + d, 4)

    plane = [(dy, dz) for dy in range(4) for dz in range(4) if (dy, dz) != (0, 0)]

    def in_plane(axes, da, db):
        return {AXES[axes[0]]: other(axes[0], da), AXES[axes[1]]: other(axes[1], db)}

    peers = [far(a, other(a, d)) for a in "xyz" for d in (1, 2, 3)]
    peers += [in_plane(axes, *p) for axes in ("yz", "xz", "xy") for p in plane if 0 not in p]
    meet([mate] + peers)

    right, left, across = other("x", 1), other("x", 3), other("x", 2)
    depth, share = w_in.shape
    half = depth // 2
    upper = pl.ds(pl.multiple_of(core * half, half), half)
    to_right, to_left = far("x", right), far("x", left)

    def at_in(block):
        return wi.at[upper, pl.ds(pl.multiple_of(block * share, share), share)]

    def at_out(block):
        return wo.at[pl.ds(pl.multiple_of(block * share + core * half, half), half), :]

    own_in, own_out = w_in.at[upper, :], w_out.at[upper, :]
    in_r = remote(own_in, at_in(me), wsend.at[0], wrecv.at[0], to_right)
    out_l = remote(own_out, at_out(me), wsend.at[1], wrecv.at[1], to_left)
    out_r = remote(own_out, at_out(me), wsend.at[2], wrecv.at[2], to_right)
    in_l = remote(own_in, at_in(me), wsend.at[3], wrecv.at[3], to_left)
    own_bias = bi.at[pl.ds(pl.multiple_of(me * share, share), share)]
    biases = [
        remote(b_in, own_bias, bsend.at[d], brecv.at[d], far("x", other("x", d))) for d in (1, 2, 3)
    ]
    kept = [
        pltpu.make_async_copy(w_in, wi.at[:, pl.ds(pl.multiple_of(me * share, share), share)], local.at[0]),
        pltpu.make_async_copy(w_out, wo.at[pl.ds(pl.multiple_of(me * share, share), share), :], local.at[1]),
        pltpu.make_async_copy(b_in, own_bias, local.at[2]),
    ]
    for copy in kept:
        copy.start()

    stepb[...] = jnp.broadcast_to(step[...], (rows, rows)).T
    lenb[...] = jnp.broadcast_to(length[...], (rows, rows)).T
    dr[...] = diff[...] * twice(jnp.sqrt(stepb[...]))
    for j in range(n_obs):
        obsb[j] = jnp.broadcast_to(obs[j : j + 1, :], (rows, rows)).T
    dec_flip = dec[...].T
    dec_t[...] = jnp.concatenate([dec_flip, dec_flip], axis=0)
    klacc[...] = jnp.zeros_like(klacc)
    acc[...] = jnp.zeros_like(acc)
    sum_in[...] = jnp.zeros_like(sum_in)
    sum_out[...] = jnp.zeros_like(sum_out)
    tiny[...] = jnp.zeros_like(tiny)
    state[...] = init[...]
    inv = 1.0 / diff[...]
    loads[0].wait()
    obsf[...] = observed[...].astype(F32).reshape(rows * n_obs, dec.shape[1])

    sent = []

    def share_with_mate(n, ref):
        sent.append(remote(ref, ref, psend.at[n], precv.at[n], mate))

    in_r.wait_recv()
    in_rr = remote(at_in(left), at_in(left), wsend.at[4], wrecv.at[4], to_right)
    share_with_mate(0, at_in(left))
    out_l.wait_recv()
    out_ll = remote(at_out(right), at_out(right), wsend.at[5], wrecv.at[5], to_left)
    share_with_mate(1, at_out(right))
    out_r.wait_recv()
    share_with_mate(2, at_out(left))
    in_l.wait_recv()
    share_with_mate(3, at_in(right))
    in_rr.wait_recv()
    share_with_mate(4, at_in(across))
    out_ll.wait_recv()
    share_with_mate(5, at_out(across))
    for copy in kept:
        copy.wait()
    for copy in biases + sent:
        copy.wait()
    for copy in (in_r, out_l, out_r, in_l, in_rr, out_ll):
        copy.wait_send()

    w_in_t[...] = wi[...].T
    w_out_t[...] = wo[...].T
    bias = bi[...].astype(F32).reshape(1, hidden)
    loads[1].wait()

    def see(k, rounded):
        seen = mm(rounded, dec[...])
        for j in range(n_obs):
            acc[j] = jnp.where(obsb[j] == k, seen, acc[j])

    def at(k):
        return pl.ds(pl.multiple_of(k * rows, rows), rows)

    def forward(k, carry):
        s = state[...]
        rounded = s.astype(BF16)
        drift = b_out[...]
        for n in range(0, hidden, width):
            cs = slice(n, n + width)
            activity = jnp.tanh(mm(rounded, wi[:, cs]) + bias[:, cs]).astype(BF16)
            acts[at(k), cs] = activity
            drift = drift + mm(activity, wo[cs, :])
        live = lenb[...] > k
        factor = jnp.where(live, stepb[...], 0.0)
        residual = (drift + prior[...] * s) * inv
        noise = dr[...] * brown[k].astype(F32)
        state[...] = s + twice(factor) * drift + jnp.where(twice(live), noise, 0.0)
        scaled[k] = residual * inv
        square = residual * residual
        klacc[...] += (0.5 * factor) * (square[:, :rows] + square[:, rows:])
        traj_t[:, at(k)] = rounded.T
        see(k, rounded)
        return carry

    lax.fori_loop(0, steps, forward, 0, unroll=UNROLL)
    last = state[...].astype(BF16)
    traj_t[:, at(steps)] = last.T
    see(steps, last)

    total = jnp.zeros((rows, rows), F32)
    for j in range(n_obs):
        misfit = acc[j] - obsf[pl.ds(j, rows, stride=n_obs), :]
        total = total + misfit * misfit
        acc[j] = misfit.astype(BF16).astype(F32)
    loglik = -0.5 * total
    divisor = (width * lenb[...] + rows * n_obs).astype(F32)
    per_series = jnp.sum(loglik - klacc[...], axis=1, keepdims=True) / divisor
    elbo[...] = per_series.T[0:1, :]

    def gathered(k):
        m = jnp.zeros((rows, rows), F32)
        for j in range(n_obs):
            m = m + jnp.where(obsb[j] == k, acc[j], 0.0)
        high = m.astype(BF16)
        low = (m - high.astype(F32)).astype(BF16)
        return jnp.concatenate([high, low], axis=1)

    final = gathered(steps)
    back[at(steps), :] = final
    cot[...] = mm(final, dec_t[...])
    final = gathered(steps - 1)
    back[at(steps - 1), :] = final
    ob[...] = mm(final, dec_t[...])

    def backward(i, carry):
        k = steps - 1 - i
        c = cot[...]
        factor = twice(jnp.where(lenb[...] > k, stepb[...], 0.0))
        part = scaled[k]
        update = factor * (c + part)
        rounded = update.astype(BF16)
        value = acts[at(k), :].astype(F32)
        pre_grad = mm(rounded, w_out_t[...]) * (1.0 - value * value)
        pre_round = pre_grad.astype(BF16)
        ahead = ob[...]
        before = jnp.maximum(k - 1, 0)
        seen = gathered(before)
        ob[...] = mm(seen, dec_t[...])
        cot[...] = (c + factor * prior[...] * part + ahead) + mm(pre_round, w_in_t[...])
        pre[at(k), :] = pre_round
        back[at(before), :] = seen
        upd_t[:, at(k)] = rounded.T
        sum_in[...] += jnp.sum(pre_grad.reshape(rows // 8, 8, hidden), axis=0)
        sum_out[...] += jnp.sum(update.reshape(rows // 8, 8, width), axis=0)
        return carry

    lax.fori_loop(0, steps, backward, 0, unroll=UNROLL)
    ginit[...] = cot[...]

    pending = []
    first = {}
    flying = {}
    used = itertools.count()

    def go(src, dst, to, *key):
        n = next(used)
        copy = remote(src, dst, send.at[n], recv.at[n], to)
        pending.append(copy)
        flying.setdefault(key, []).append(copy)

    def landed(*key):
        for copy in flying[key]:
            copy.wait_recv()

    def along(dims, axis, index):
        return tuple(index if a == axis else slice(None) for a in dims)

    def grads(d, base, left_ref, right_ref):
        n = other("x", d)
        cols = pl.ds(pl.multiple_of(n * width, width), width)
        grad = mm(left_ref[:, : steps * rows], right_ref[:, cols]) * scale
        for u in (base, base + 1):
            h = u - base
            big[u, :, n] = grad[:, h * rows : (h + 1) * rows].reshape(2, 4, 4, 8, rows)
        for u in (base, base + 1):
            go(big.at[u, 1 - core, n], got.at[u, n], mate, "half", u, d)

    for d in (2, 1, 3, 0):
        grads(d, 0, traj_t, pre)

    grad_dec = mm(traj_t[...], back[...]) * scale
    small[...] = (grad_dec[:, :rows] + grad_dec[:, rows:]).reshape(2, 4, 4, 8, rows)
    row_in = jnp.sum(sum_in[...], axis=0, keepdims=True) * scale
    row_out = jnp.sum(sum_out[...], axis=0, keepdims=True) * scale
    for r in range(hidden // rows):
        tiny[0, r : r + 1, :] = row_in[:, r * rows : (r + 1) * rows]
    for r in range(width // rows):
        tiny[1, r : r + 1, :] = row_out[:, r * rows : (r + 1) * rows]
    for r, part in ((2, loglik), (3, klacc[...])):
        total = jnp.sum(jnp.sum(part, axis=0, keepdims=True), axis=1, keepdims=True) * scale
        tiny[1, r : r + 1, :] = jnp.broadcast_to(total, (1, rows))
    go(small.at[1 - core], small_got, mate, "half", "small")
    go(tiny.at[1 - core], tiny_got, mate, "half", "tiny")

    for d in (2, 1, 3, 0):
        grads(d, 2, upd_t, acts)
        n = other("x", d)
        for u in (0, 1):
            landed("half", u, d)
            cur[u, n] = big[u, core, n] + got[u, n]
            if d:
                go(cur.at[u, n], r1.at[u, d - 1], far("x", n), "one", u)

    landed("half", "small")
    small_cur[...] = small[core] + small_got[...]
    landed("half", "tiny")
    tiny_cur[0] = tiny[core] + tiny_got[...]
    for d in (2, 1, 3):
        to = far("y", other("y", d))
        go(small_cur.at[other("y", d)], s1.at[d - 1], to, "one", "small")
        go(tiny_cur.at[0], t1.at[place["y"]], to, "one", "tiny")
    for u in (2, 3):
        axis = FIRST[u]
        for d in (2, 1, 3, 0):
            landed("half", u, d)
        cur[u] = big[u, core] + got[u]
        for d in (2, 1, 3):
            p = other(axis, d)
            go(cur.at[u].at[along("xyz", axis, p)], r1.at[u, d - 1], far(axis, p), "one", u)

    landed("one", "tiny")
    t1[place["y"]] = tiny_cur[0]
    tiny_cur[1] = t1[0] + t1[1] + t1[2] + t1[3]
    landed("one", "small")
    small_got[0] = small_cur[place["y"]] + s1[0] + s1[1] + s1[2]
    for dx, dz in plane:
        to = in_plane("xz", dx, dz)
        go(small_got.at[0, other("z", dz)], s2.at[me, place["z"]], to, "two", "small")
        go(tiny_cur.at[1], t2.at[me, place["z"]], to, "two", "tiny")
    for flow, members in (("x", (0, 1)), ("y", (2,)), ("z", (3,))):
        for u in members:
            landed("one", u)
            own = cur[(u,) + along("xyz", flow, place[flow])]
            mid[u] = own + r1[u, 0] + r1[u, 1] + r1[u, 2]
        axes = "xyz".replace(flow, "")
        us = pl.ds(members[0], len(members))
        for n, (da, db) in enumerate(plane):
            src = mid.at[us, other(axes[0], da), other(axes[1], db)]
            go(src, r2.at[n, us], in_plane(axes, da, db), "two", flow)

    def summed(parts):
        total = parts[0]
        for part in parts[1:]:
            total = total + part
        return total

    landed("two", "small")
    s2[me, place["z"]] = small_got[0, place["z"]]
    landed("two", "tiny")
    t2[me, place["z"]] = tiny_cur[1]
    tiny_out[core] = summed([t2[x, z] for x in range(4) for z in range(4)])
    go(tiny_out.at[core], tiny_out.at[core], mate, "last", "tiny")
    tiles = {4: summed([s2[x, z] for x in range(4) for z in range(4)])}
    for flow, members in (("y", (2,)), ("z", (3,)), ("x", (0, 1))):
        landed("two", flow)
        axes = "xyz".replace(flow, "")
        for u in members:
            own = mid[u, place[axes[0]], place[axes[1]]]
            tiles[u] = summed([own] + [r2[n, u] for n in range(15)])
    packed[...] = pack([tiles[t] for t in range(5)])

    home = out.at[core, place["y"], place["z"]]
    for n, (dy, dz) in enumerate(plane):
        go(packed, home, in_plane("yz", dy, dz), "all", n)
    go(packed, home, mate, "last", "own")
    out[core, place["y"], place["z"]] = packed[...]
    for n, (dy, dz) in enumerate(plane):
        landed("all", n)
        came = out.at[core, lax.rem(place["y"] + 4 - dy, 4), lax.rem(place["z"] + 4 - dz, 4)]
        go(came, came, mate, "last", n)
    landed("last", "tiny")
    landed("last", "own")
    for n in range(len(plane)):
        landed("last", n)
    for copy in pending:
        copy.wait_send()


def whole(total, init, brown, step, length, obs, observed, w_in, b_in, w_out, b_out, dec, prior, diff):
    steps, rows, width = brown.shape
    hidden, n_obs = 4 * w_in.shape[1], obs.shape[1]
    vmem, dma = pltpu.VMEM, pltpu.SemaphoreType.DMA
    near, rest = pl.BlockSpec(memory_space=vmem), pl.BlockSpec(memory_space=pl.ANY)
    tile = (8, 128)
    return pl.pallas_call(
        functools.partial(whole_kernel, 1.0 / total),
        out_shape=(
            jax.ShapeDtypeStruct((1, rows), F32),
            jax.ShapeDtypeStruct((2, 4, 4, 48, 128), jnp.int16),
            jax.ShapeDtypeStruct((2,) + tile, F32),
            jax.ShapeDtypeStruct((rows, width), F32),
        ),
        in_specs=[near, rest, near, near, near, rest] + [near] * 7,
        out_specs=[near] * 4,
        scratch_shapes=[
            vmem((width, hidden), BF16),
            vmem((hidden, width), BF16),
            vmem((hidden,), BF16),
            vmem(brown.shape, BF16),
            vmem(observed.shape, BF16),
            vmem((rows, width), F32),
            vmem((rows, rows), F32),
            vmem((rows, rows), jnp.int32),
            vmem((rows, width), F32),
            vmem((n_obs, rows, rows), jnp.int32),
            vmem((rows * n_obs, rows), F32),
            vmem((n_obs, rows, rows), F32),
            vmem((rows, rows), F32),
            vmem((width, (steps + 1) * rows), BF16),
            vmem((steps * rows, hidden), BF16),
            vmem((steps, rows, width), F32),
            vmem((steps * rows, hidden), BF16),
            vmem(((steps + 1) * rows, width), BF16),
            vmem((width, steps * rows), BF16),
            vmem((hidden, width), BF16),
            vmem((width, hidden), BF16),
            vmem((width, width), BF16),
            vmem((rows, width), F32),
            vmem((rows, width), F32),
            vmem((8, hidden), F32),
            vmem((8, width), F32),
            vmem((4, 2, 4, 4, 4) + tile, F32),
            vmem((2, 4, 4) + tile, F32),
            vmem((2,) + tile, F32),
            vmem((4, 4, 4, 4) + tile, F32),
            vmem((4, 4, 4, 4) + tile, F32),
            vmem((4, 4, 4) + tile, F32),
            vmem((4, 3, 4, 4) + tile, F32),
            vmem((15, 4) + tile, F32),
            vmem((4, 4) + tile, F32),
            vmem((4, 4) + tile, F32),
            vmem((3, 4) + tile, F32),
            vmem((4, 4) + tile, F32),
            vmem(tile, F32),
            vmem((2,) + tile, F32),
            vmem((4,) + tile, F32),
            vmem((4, 4) + tile, F32),
            vmem((48, 128), jnp.int16),
            dma((6,)), dma((6,)), dma((4,)), dma((4,)), dma((6,)), dma((6,)), dma((5,)),
            dma((COPIES,)), dma((COPIES,)),
        ],
        compiler_params=pltpu.CompilerParams(
            collective_id=0, has_side_effects=True, vmem_limit_bytes=58 * 1024 * 1024
        ),
        name="whole",
    )(
        init, brown, step.reshape(1, -1), length.reshape(1, -1), obs.T, observed, w_in,
        b_in, w_out, b_out.reshape(1, -1), dec, prior.reshape(1, -1), diff.reshape(1, -1),
    )


def finish_kernel(elbo_in, out, tiny, ginit_in, elbo, w_in, w_out, dec, b_in, b_out, scores, ginit, turn):
    me = lax.axis_index("mp")
    elbo[...] = elbo_in[...]
    ginit[...] = ginit_in[...]
    for n in range(32):
        block = out[n // 16, (n // 4) % 4, n % 4].astype(jnp.int32).astype(F32)
        rs = slice(n * 8, n * 8 + 8)
        part = [block[t * 8 : t * 8 + 8] * jnp.exp2(block[40 + t : 41 + t]) for t in range(5)]
        w_in[rs, :128] = part[0]
        w_in[rs, 128:] = part[1]
        turn[rs, :128] = part[2]
        turn[rs, 128:] = part[3]
        dec[rs, :] = part[4]
    w_out[...] = turn[...].T
    for r in range(2):
        b_in[:, r * 128 : (r + 1) * 128] = tiny[0, pl.ds(2 * me + r, 1), :]
        b_out[:, r * 128 : (r + 1) * 128] = tiny[1, r : r + 1, :]
    first = lax.broadcasted_iota(jnp.int32, (1, 128), 1) == 0
    both = jnp.where(first, tiny[1, 2:3, :], tiny[1, 3:4, :])
    scores[...] = both[:, :2]


def unpack(elbo, out, tiny, ginit):
    vmem = pltpu.VMEM
    return pl.pallas_call(
        finish_kernel,
        out_shape=tuple(
            jax.ShapeDtypeStruct(s, F32)
            for s in ((1, 128), (256, 256), (256, 256), (256, 128), (1, 256), (1, 256), (1, 2), (128, 256))
        ),
        in_specs=[pl.BlockSpec(memory_space=vmem)] * 4,
        out_specs=[pl.BlockSpec(memory_space=vmem)] * 8,
        scratch_shapes=[vmem((256, 256), F32)],
        name="unpack",
    )(elbo, out, tiny, ginit)


def on_device(
    init_state, brownian, step_size, lengths, obs_steps, observed,
    w_in, b_in, w_out, b_out, decoder, prior_rate, diffusion,
):
    total = init_state.shape[0] * lax.axis_size(BATCH_MP)
    elbo, parts, tiny, grad_init = whole(
        total, init_state, brownian, step_size, lengths, obs_steps, observed,
        w_in, b_in, w_out, b_out, decoder, prior_rate, diffusion,
    )
    elbo, own_in, own_out, grad_dec, own_b, grad_b_out, scores, grad_init = unpack(
        elbo, parts, tiny, grad_init
    )
    return (
        elbo.reshape(-1), scores.reshape(-1), own_in, own_b.reshape(-1), own_out, grad_b_out.reshape(-1),
        grad_dec, grad_init,
    )


def solution(mesh):
    torus = Mesh(
        mesh.devices.reshape(4, 4, 2, mesh.shape["mp"]), ("batch_0", "batch_1", "batch_2", "mp")
    )
    placed = (
        P(BATCH_MP, None), P(None, BATCH_MP, None), P(BATCH_MP), P(BATCH_MP), P(BATCH_MP, None),
        P(BATCH_MP, None, None), P(None, "mp"), P("mp"), P("mp", None), P(), P(), P(), P(),
    )
    return jax.shard_map(
        on_device,
        mesh=torus,
        in_specs=placed,
        out_specs=(
            P(BATCH_MP), P(), P(None, "mp"), P("mp"), P("mp", None), P(), P(), P(BATCH_MP, None),
        ),
        check_vma=False,
    )
```

```python
import functools
import itertools

import jax
import jax.numpy as jnp
from jax import lax
from jax.experimental import pallas as pl
from jax.experimental.pallas import tpu as pltpu
from jax.sharding import Mesh
from jax.sharding import PartitionSpec as P

BATCH_MP = ("batch_0", "batch_1", "batch_2", "mp")
F32, BF16 = jnp.float32, jnp.bfloat16
UNROLL = 4


def mm(a, b):
    return jnp.dot(a, b, preferred_element_type=F32)


def twice(a):
    return jnp.concatenate([a, a], axis=1)


AXES = {"x": "mp", "y": "batch_0", "z": "batch_1", "c": "batch_2"}
LOGICAL = pl.DeviceIdType.MESH
COPIES = 168


def pack(tiles):
    rows, marks = [], []
    for tile in tiles:
        top = jnp.max(jnp.max(jnp.abs(tile), axis=0, keepdims=True), axis=1, keepdims=True)
        power = jnp.ceil(jnp.log2(jnp.maximum(top, 1e-30) * (1.0 / 32000.0)))
        rows.append(jnp.floor(tile * jnp.exp2(-power) + 0.5))
        marks.append(jnp.broadcast_to(power, (1, 128)))
    marks.append(jnp.zeros((3, 128), F32))
    return jnp.concatenate(rows + marks, axis=0).astype(jnp.int32).astype(jnp.int16)


def far(axis, where):
    return {AXES[axis]: where}


def remote(src, dst, send, recv, to):
    copy = pltpu.make_async_remote_copy(
        src_ref=src, dst_ref=dst, send_sem=send, recv_sem=recv, device_id=to, device_id_type=LOGICAL
    )
    copy.start()
    return copy


def meet(peers):
    barrier = pltpu.get_barrier_semaphore()
    for peer in peers:
        pl.semaphore_signal(barrier, inc=1, device_id=peer, device_id_type=LOGICAL)
    pl.semaphore_wait(barrier, len(peers))


def whole_kernel(
    scale,
    init, brown_hbm, step, length, obs, observed_hbm, w_in, b_in, w_out, b_out, dec, prior, diff,
    elbo, out, tiny_out, ginit,
    wi, wo, bi, brown, observed,
    state, stepb, lenb, dr, obsb, obsf, acc, klacc, traj_t, acts, scaled, pre, back, upd_t,
    w_in_t, w_out_t, dec_t, cot, ob, sum_in, sum_out,
    big, small, tiny, got, cur, mid, r1, chain, r2, small_got, small_cur, s1, s2, tiny_got, tiny_cur, t1, t2, packed,
    wsend, wrecv, bsend, brecv, psend, precv, local, send, recv,
):
    steps, rows, width = brown.shape
    hidden = wi.shape[1]
    n_obs = obs.shape[0]
    loads = [
        pltpu.make_async_copy(observed_hbm, observed, local.at[3]),
        pltpu.make_async_copy(brown_hbm, brown, local.at[4]),
    ]
    for copy in loads:
        copy.start()

    place = {a: lax.axis_index(AXES[a]) for a in "xyzc"}
    me, core = place["x"], place["c"]
    mate = far("c", 1 - core)

    def other(axis, d):
        return lax.rem(place[axis] + d, 4)

    plane = [(da, db) for da in range(4) for db in range(4) if (da, db) != (0, 0)]
    plane.sort(key=lambda p: -sum(min(d, 4 - d) for d in p))

    def in_plane(axes, da, db):
        return {AXES[axes[0]]: other(axes[0], da), AXES[axes[1]]: other(axes[1], db)}

    peers = [far(a, other(a, d)) for a in "xyz" for d in (1, 2, 3)]
    peers += [in_plane(axes, *p) for axes in ("yz", "xz", "xy") for p in plane if 0 not in p]
    meet([mate] + peers)

    right, left, across = other("x", 1), other("x", 3), other("x", 2)
    depth, share = w_in.shape
    half = depth // 2
    upper = pl.ds(pl.multiple_of(core * half, half), half)
    to_right, to_left = far("x", right), far("x", left)

    def at_in(block):
        return wi.at[upper, pl.ds(pl.multiple_of(block * share, share), share)]

    def at_out(block):
        return wo.at[pl.ds(pl.multiple_of(block * share + core * half, half), half), :]

    own_in, own_out = w_in.at[upper, :], w_out.at[upper, :]
    in_r = remote(own_in, at_in(me), wsend.at[0], wrecv.at[0], to_right)
    out_l = remote(own_out, at_out(me), wsend.at[1], wrecv.at[1], to_left)
    out_r = remote(own_out, at_out(me), wsend.at[2], wrecv.at[2], to_right)
    in_l = remote(own_in, at_in(me), wsend.at[3], wrecv.at[3], to_left)
    own_bias = bi.at[pl.ds(pl.multiple_of(me * share, share), share)]
    biases = [
        remote(b_in, own_bias, bsend.at[d], brecv.at[d], far("x", other("x", d))) for d in (1, 2, 3)
    ]
    kept = [
        pltpu.make_async_copy(w_in, wi.at[:, pl.ds(pl.multiple_of(me * share, share), share)], local.at[0]),
        pltpu.make_async_copy(w_out, wo.at[pl.ds(pl.multiple_of(me * share, share), share), :], local.at[1]),
        pltpu.make_async_copy(b_in, own_bias, local.at[2]),
    ]
    for copy in kept:
        copy.start()

    stepb[...] = jnp.broadcast_to(step[...], (rows, rows)).T
    lenb[...] = jnp.broadcast_to(length[...], (rows, rows)).T
    dr[...] = diff[...] * twice(jnp.sqrt(stepb[...]))
    for j in range(n_obs):
        obsb[j] = jnp.broadcast_to(obs[j : j + 1, :], (rows, rows)).T
    dec_flip = dec[...].T
    dec_t[...] = jnp.concatenate([dec_flip, dec_flip], axis=0)
    klacc[...] = jnp.zeros_like(klacc)
    acc[...] = jnp.zeros_like(acc)
    sum_in[...] = jnp.zeros_like(sum_in)
    sum_out[...] = jnp.zeros_like(sum_out)
    tiny[...] = jnp.zeros_like(tiny)
    state[...] = init[...]
    inv = 1.0 / diff[...]
    loads[0].wait()
    obsf[...] = observed[...].astype(F32).reshape(rows * n_obs, dec.shape[1])

    sent = []

    def share_with_mate(n, ref):
        sent.append(remote(ref, ref, psend.at[n], precv.at[n], mate))

    in_r.wait_recv()
    in_rr = remote(at_in(left), at_in(left), wsend.at[4], wrecv.at[4], to_right)
    share_with_mate(0, at_in(left))
    out_l.wait_recv()
    out_ll = remote(at_out(right), at_out(right), wsend.at[5], wrecv.at[5], to_left)
    share_with_mate(1, at_out(right))
    out_r.wait_recv()
    share_with_mate(2, at_out(left))
    in_l.wait_recv()
    share_with_mate(3, at_in(right))
    in_rr.wait_recv()
    share_with_mate(4, at_in(across))
    out_ll.wait_recv()
    share_with_mate(5, at_out(across))
    for copy in kept:
        copy.wait()
    for copy in biases + sent:
        copy.wait()
    for copy in (in_r, out_l, out_r, in_l, in_rr, out_ll):
        copy.wait_send()

    w_in_t[...] = wi[...].T
    w_out_t[...] = wo[...].T
    bias = bi[...].astype(F32).reshape(1, hidden)
    loads[1].wait()

    def see(k, rounded):
        seen = mm(rounded, dec[...])
        for j in range(n_obs):
            acc[j] = jnp.where(obsb[j] == k, seen, acc[j])

    def at(k):
        return pl.ds(pl.multiple_of(k * rows, rows), rows)

    def forward(k, carry):
        s = state[...]
        rounded = s.astype(BF16)
        drift = b_out[...]
        for n in range(0, hidden, width):
            cs = slice(n, n + width)
            activity = jnp.tanh(mm(rounded, wi[:, cs]) + bias[:, cs]).astype(BF16)
            acts[at(k), cs] = activity
            drift = drift + mm(activity, wo[cs, :])
        live = lenb[...] > k
        factor = jnp.where(live, stepb[...], 0.0)
        residual = (drift + prior[...] * s) * inv
        noise = dr[...] * brown[k].astype(F32)
        state[...] = s + twice(factor) * drift + jnp.where(twice(live), noise, 0.0)
        scaled[k] = residual * inv
        square = residual * residual
        klacc[...] += (0.5 * factor) * (square[:, :rows] + square[:, rows:])
        traj_t[:, at(k)] = rounded.T
        see(k, rounded)
        return carry

    lax.fori_loop(0, steps, forward, 0, unroll=UNROLL)
    last = state[...].astype(BF16)
    traj_t[:, at(steps)] = last.T
    see(steps, last)

    total = jnp.zeros((rows, rows), F32)
    for j in range(n_obs):
        misfit = acc[j] - obsf[pl.ds(j, rows, stride=n_obs), :]
        total = total + misfit * misfit
        acc[j] = misfit.astype(BF16).astype(F32)
    loglik = -0.5 * total
    divisor = (width * lenb[...] + rows * n_obs).astype(F32)
    per_series = jnp.sum(loglik - klacc[...], axis=1, keepdims=True) / divisor
    elbo[...] = per_series.T[0:1, :]

    def gathered(k):
        m = jnp.zeros((rows, rows), F32)
        for j in range(n_obs):
            m = m + jnp.where(obsb[j] == k, acc[j], 0.0)
        high = m.astype(BF16)
        low = (m - high.astype(F32)).astype(BF16)
        return jnp.concatenate([high, low], axis=1)

    final = gathered(steps)
    back[at(steps), :] = final
    cot[...] = mm(final, dec_t[...])
    final = gathered(steps - 1)
    back[at(steps - 1), :] = final
    ob[...] = mm(final, dec_t[...])

    def backward(i, carry):
        k = steps - 1 - i
        c = cot[...]
        factor = twice(jnp.where(lenb[...] > k, stepb[...], 0.0))
        part = scaled[k]
        update = factor * (c + part)
        rounded = update.astype(BF16)
        value = acts[at(k), :].astype(F32)
        pre_grad = mm(rounded, w_out_t[...]) * (1.0 - value * value)
        pre_round = pre_grad.astype(BF16)
        ahead = ob[...]
        before = jnp.maximum(k - 1, 0)
        seen = gathered(before)
        ob[...] = mm(seen, dec_t[...])
        cot[...] = (c + factor * prior[...] * part + ahead) + mm(pre_round, w_in_t[...])
        pre[at(k), :] = pre_round
        back[at(before), :] = seen
        upd_t[:, at(k)] = rounded.T
        sum_in[...] += jnp.sum(pre_grad.reshape(rows // 8, 8, hidden), axis=0)
        sum_out[...] += jnp.sum(update.reshape(rows // 8, 8, width), axis=0)
        return carry

    lax.fori_loop(0, steps, backward, 0, unroll=UNROLL)
    ginit[...] = cot[...]

    pending = []
    first = {}
    flying = {}
    used = itertools.count()

    def go(src, dst, to, *key):
        n = next(used)
        copy = remote(src, dst, send.at[n], recv.at[n], to)
        pending.append(copy)
        flying.setdefault(key, []).append(copy)

    def landed(*key):
        for copy in flying[key]:
            copy.wait_recv()

    def along(dims, axis, index):
        return tuple(index if a == axis else slice(None) for a in dims)

    def grads(d, base, left_ref, right_ref):
        n = other("x", d)
        cols = pl.ds(pl.multiple_of(n * width, width), width)
        grad = mm(left_ref[:, : steps * rows], right_ref[:, cols]) * scale
        for u in (base, base + 1):
            h = u - base
            big[u, :, n] = grad[:, h * rows : (h + 1) * rows].reshape(2, 4, 4, 8, rows)
        for u in (base, base + 1):
            go(big.at[u, 1 - core, n], got.at[u, n], mate, "half", u, d)

    def halves(d, base):
        n = other("x", d)
        for u in (base, base + 1):
            landed("half", u, d)
            cur[u, n] = big[u, core, n] + got[u, n]
        return n

    def sideways(d):
        n = halves(d, 2)
        for e in (2, 1, 3):
            y, z = other("y", e), other("z", e)
            go(cur.at[2, n, y], r1.at[2, e - 1, n], far("y", y), "one", 2)
            go(cur.at[3, n, :, z], r1.at[3, e - 1, n], far("z", z), "one", 3)

    def relay(u, block, to):
        landed("across", u)
        chain[u, 1] = cur[u, block] + chain[u, 0]
        go(chain.at[u, 1], chain.at[u, 2], to, "one", u)

    grads(2, 0, traj_t, pre)
    grads(2, 2, upd_t, acts)
    grads(1, 2, upd_t, acts)
    halves(2, 0)
    go(cur.at[0, across], chain.at[0, 0], to_right, "across", 0)
    go(cur.at[1, across], chain.at[1, 0], to_left, "across", 1)
    grads(3, 2, upd_t, acts)
    sideways(2)
    grads(0, 2, upd_t, acts)
    sideways(1)
    grads(1, 0, traj_t, pre)
    sideways(3)
    grads(3, 0, traj_t, pre)
    sideways(0)
    grads(0, 0, traj_t, pre)
    halves(1, 0)
    go(cur.at[1, right], chain.at[1, 3], to_right, "one", 1)

    grad_dec = mm(traj_t[...], back[...]) * scale
    small[...] = (grad_dec[:, :rows] + grad_dec[:, rows:]).reshape(2, 4, 4, 8, rows)
    row_in = jnp.sum(sum_in[...], axis=0, keepdims=True) * scale
    row_out = jnp.sum(sum_out[...], axis=0, keepdims=True) * scale
    for r in range(hidden // rows):
        tiny[0, r : r + 1, :] = row_in[:, r * rows : (r + 1) * rows]
    for r in range(width // rows):
        tiny[1, r : r + 1, :] = row_out[:, r * rows : (r + 1) * rows]
    for r, part in ((2, loglik), (3, klacc[...])):
        total = jnp.sum(jnp.sum(part, axis=0, keepdims=True), axis=1, keepdims=True) * scale
        tiny[1, r : r + 1, :] = jnp.broadcast_to(total, (1, rows))
    go(small.at[1 - core], small_got, mate, "half", "small")
    go(tiny.at[1 - core], tiny_got, mate, "half", "tiny")

    halves(3, 0)
    go(cur.at[0, left], chain.at[0, 3], to_left, "one", 0)
    relay(0, right, to_right)
    relay(1, left, to_left)
    halves(0, 0)
    landed("half", "small")
    small_cur[...] = small[core] + small_got[...]
    landed("half", "tiny")
    tiny_cur[0] = tiny[core] + tiny_got[...]
    for d in (2, 1, 3):
        to = far("y", other("y", d))
        go(small_cur.at[other("y", d)], s1.at[d - 1], to, "one", "small")
        go(tiny_cur.at[0], t1.at[place["y"]], to, "one", "tiny")

    for flow, members in (("x", (0, 1)), ("y", (2,)), ("z", (3,))):
        for u in members:
            landed("one", u)
            own = cur[(u,) + along("xyz", flow, place[flow])]
            if flow == "x":
                mid[u] = own + chain[u, 2] + chain[u, 3]
            else:
                mid[u] = own + r1[u, 0] + r1[u, 1] + r1[u, 2]
        axes = "xyz".replace(flow, "")
        us = pl.ds(members[0], len(members))
        for n, (da, db) in enumerate(plane):
            src = mid.at[us, other(axes[0], da), other(axes[1], db)]
            go(src, r2.at[n, us], in_plane(axes, da, db), "two", flow)

    landed("one", "tiny")
    t1[place["y"]] = tiny_cur[0]
    tiny_cur[1] = t1[0] + t1[1] + t1[2] + t1[3]
    landed("one", "small")
    small_got[0] = small_cur[place["y"]] + s1[0] + s1[1] + s1[2]
    for dx, dz in plane:
        to = in_plane("xz", dx, dz)
        go(small_got.at[0, other("z", dz)], s2.at[me, place["z"]], to, "two", "small")
        go(tiny_cur.at[1], t2.at[me, place["z"]], to, "two", "tiny")
    def summed(parts):
        total = parts[0]
        for part in parts[1:]:
            total = total + part
        return total

    tiles = {}
    for flow, members in (("x", (0, 1)), ("y", (2,)), ("z", (3,))):
        landed("two", flow)
        axes = "xyz".replace(flow, "")
        for u in members:
            own = mid[u, place[axes[0]], place[axes[1]]]
            tiles[u] = summed([own] + [r2[n, u] for n in range(15)])
    landed("two", "small")
    s2[me, place["z"]] = small_got[0, place["z"]]
    landed("two", "tiny")
    t2[me, place["z"]] = tiny_cur[1]
    tiny_out[core] = summed([t2[x, z] for x in range(4) for z in range(4)])
    go(tiny_out.at[core], tiny_out.at[core], mate, "last", "tiny")
    tiles[4] = summed([s2[x, z] for x in range(4) for z in range(4)])
    packed[...] = pack([tiles[t] for t in range(5)])

    home = out.at[core, place["y"], place["z"]]
    for n, (dy, dz) in enumerate(plane):
        go(packed, home, in_plane("yz", dy, dz), "all", n)
    go(packed, home, mate, "last", "own")
    out[core, place["y"], place["z"]] = packed[...]
    for n, (dy, dz) in reversed(list(enumerate(plane))):
        landed("all", n)
        came = out.at[core, lax.rem(place["y"] + 4 - dy, 4), lax.rem(place["z"] + 4 - dz, 4)]
        go(came, came, mate, "last", n)
    landed("last", "tiny")
    landed("last", "own")
    for n in range(len(plane)):
        landed("last", n)
    for copy in pending:
        copy.wait_send()


def whole(total, init, brown, step, length, obs, observed, w_in, b_in, w_out, b_out, dec, prior, diff):
    steps, rows, width = brown.shape
    hidden, n_obs = 4 * w_in.shape[1], obs.shape[1]
    vmem, dma = pltpu.VMEM, pltpu.SemaphoreType.DMA
    near, rest = pl.BlockSpec(memory_space=vmem), pl.BlockSpec(memory_space=pl.ANY)
    tile = (8, 128)
    return pl.pallas_call(
        functools.partial(whole_kernel, 1.0 / total),
        out_shape=(
            jax.ShapeDtypeStruct((1, rows), F32),
            jax.ShapeDtypeStruct((2, 4, 4, 48, 128), jnp.int16),
            jax.ShapeDtypeStruct((2,) + tile, F32),
            jax.ShapeDtypeStruct((rows, width), F32),
        ),
        in_specs=[near, rest, near, near, near, rest] + [near] * 7,
        out_specs=[near] * 4,
        scratch_shapes=[
            vmem((width, hidden), BF16),
            vmem((hidden, width), BF16),
            vmem((hidden,), BF16),
            vmem(brown.shape, BF16),
            vmem(observed.shape, BF16),
            vmem((rows, width), F32),
            vmem((rows, rows), F32),
            vmem((rows, rows), jnp.int32),
            vmem((rows, width), F32),
            vmem((n_obs, rows, rows), jnp.int32),
            vmem((rows * n_obs, rows), F32),
            vmem((n_obs, rows, rows), F32),
            vmem((rows, rows), F32),
            vmem((width, (steps + 1) * rows), BF16),
            vmem((steps * rows, hidden), BF16),
            vmem((steps, rows, width), F32),
            vmem((steps * rows, hidden), BF16),
            vmem(((steps + 1) * rows, width), BF16),
            vmem((width, steps * rows), BF16),
            vmem((hidden, width), BF16),
            vmem((width, hidden), BF16),
            vmem((width, width), BF16),
            vmem((rows, width), F32),
            vmem((rows, width), F32),
            vmem((8, hidden), F32),
            vmem((8, width), F32),
            vmem((4, 2, 4, 4, 4) + tile, F32),
            vmem((2, 4, 4) + tile, F32),
            vmem((2,) + tile, F32),
            vmem((4, 4, 4, 4) + tile, F32),
            vmem((4, 4, 4, 4) + tile, F32),
            vmem((4, 4, 4) + tile, F32),
            vmem((4, 3, 4, 4) + tile, F32),
            vmem((2, 4, 4, 4) + tile, F32),
            vmem((15, 4) + tile, F32),
            vmem((4, 4) + tile, F32),
            vmem((4, 4) + tile, F32),
            vmem((3, 4) + tile, F32),
            vmem((4, 4) + tile, F32),
            vmem(tile, F32),
            vmem((2,) + tile, F32),
            vmem((4,) + tile, F32),
            vmem((4, 4) + tile, F32),
            vmem((48, 128), jnp.int16),
            dma((6,)), dma((6,)), dma((4,)), dma((4,)), dma((6,)), dma((6,)), dma((5,)),
            dma((COPIES,)), dma((COPIES,)),
        ],
        compiler_params=pltpu.CompilerParams(
            collective_id=0, has_side_effects=True, vmem_limit_bytes=58 * 1024 * 1024
        ),
        name="whole",
    )(
        init, brown, step.reshape(1, -1), length.reshape(1, -1), obs.T, observed, w_in,
        b_in, w_out, b_out.reshape(1, -1), dec, prior.reshape(1, -1), diff.reshape(1, -1),
    )


def finish_kernel(elbo_in, out, tiny, ginit_in, elbo, w_in, w_out, dec, b_in, b_out, scores, ginit, turn):
    me = lax.axis_index("mp")
    elbo[...] = elbo_in[...]
    ginit[...] = ginit_in[...]
    for n in range(32):
        block = out[n // 16, (n // 4) % 4, n % 4].astype(jnp.int32).astype(F32)
        rs = slice(n * 8, n * 8 + 8)
        part = [block[t * 8 : t * 8 + 8] * jnp.exp2(block[40 + t : 41 + t]) for t in range(5)]
        w_in[rs, :128] = part[0]
        w_in[rs, 128:] = part[1]
        turn[rs, :128] = part[2]
        turn[rs, 128:] = part[3]
        dec[rs, :] = part[4]
    w_out[...] = turn[...].T
    for r in range(2):
        b_in[:, r * 128 : (r + 1) * 128] = tiny[0, pl.ds(2 * me + r, 1), :]
        b_out[:, r * 128 : (r + 1) * 128] = tiny[1, r : r + 1, :]
    first = lax.broadcasted_iota(jnp.int32, (1, 128), 1) == 0
    both = jnp.where(first, tiny[1, 2:3, :], tiny[1, 3:4, :])
    scores[...] = both[:, :2]


def unpack(elbo, out, tiny, ginit):
    vmem = pltpu.VMEM
    return pl.pallas_call(
        finish_kernel,
        out_shape=tuple(
            jax.ShapeDtypeStruct(s, F32)
            for s in ((1, 128), (256, 256), (256, 256), (256, 128), (1, 256), (1, 256), (1, 2), (128, 256))
        ),
        in_specs=[pl.BlockSpec(memory_space=vmem)] * 4,
        out_specs=[pl.BlockSpec(memory_space=vmem)] * 8,
        scratch_shapes=[vmem((256, 256), F32)],
        name="unpack",
    )(elbo, out, tiny, ginit)


def on_device(
    init_state, brownian, step_size, lengths, obs_steps, observed,
    w_in, b_in, w_out, b_out, decoder, prior_rate, diffusion,
):
    total = init_state.shape[0] * lax.axis_size(BATCH_MP)
    elbo, parts, tiny, grad_init = whole(
        total, init_state, brownian, step_size, lengths, obs_steps, observed,
        w_in, b_in, w_out, b_out, decoder, prior_rate, diffusion,
    )
    elbo, own_in, own_out, grad_dec, own_b, grad_b_out, scores, grad_init = unpack(
        elbo, parts, tiny, grad_init
    )
    return (
        elbo.reshape(-1), scores.reshape(-1), own_in, own_b.reshape(-1), own_out, grad_b_out.reshape(-1),
        grad_dec, grad_init,
    )


def solution(mesh):
    torus = Mesh(
        mesh.devices.reshape(4, 4, 2, mesh.shape["mp"]), ("batch_0", "batch_1", "batch_2", "mp")
    )
    placed = (
        P(BATCH_MP, None), P(None, BATCH_MP, None), P(BATCH_MP), P(BATCH_MP), P(BATCH_MP, None),
        P(BATCH_MP, None, None), P(None, "mp"), P("mp"), P("mp", None), P(), P(), P(), P(),
    )
    return jax.shard_map(
        on_device,
        mesh=torus,
        in_specs=placed,
        out_specs=(
            P(BATCH_MP), P(), P(None, "mp"), P("mp"), P("mp", None), P(), P(), P(BATCH_MP, None),
        ),
        check_vma=False,
    )
```

```python
import functools
import itertools

import jax
import jax.numpy as jnp
from jax import lax
from jax.experimental import pallas as pl
from jax.experimental.pallas import tpu as pltpu
from jax.sharding import Mesh
from jax.sharding import PartitionSpec as P

BATCH_MP = ("batch_0", "batch_1", "batch_2", "mp")
F32, BF16 = jnp.float32, jnp.bfloat16
UNROLL = 8


def mm(a, b):
    return jnp.dot(a, b, preferred_element_type=F32)


def twice(a):
    return jnp.concatenate([a, a], axis=1)


AXES = {"x": "mp", "y": "batch_0", "z": "batch_1", "c": "batch_2"}
LOGICAL = pl.DeviceIdType.MESH
COPIES = 168


def pack(tiles):
    rows, marks = [], []
    for tile in tiles:
        top = jnp.max(jnp.max(jnp.abs(tile), axis=0, keepdims=True), axis=1, keepdims=True)
        power = jnp.ceil(jnp.log2(jnp.maximum(top, 1e-30) * (1.0 / 32000.0)))
        rows.append(jnp.floor(tile * jnp.exp2(-power) + 0.5))
        marks.append(jnp.broadcast_to(power, (1, 128)))
    marks.append(jnp.zeros((3, 128), F32))
    return jnp.concatenate(rows + marks, axis=0).astype(jnp.int32).astype(jnp.int16)


def far(axis, where):
    return {AXES[axis]: where}


def remote(src, dst, send, recv, to):
    copy = pltpu.make_async_remote_copy(
        src_ref=src, dst_ref=dst, send_sem=send, recv_sem=recv, device_id=to, device_id_type=LOGICAL
    )
    copy.start()
    return copy


def meet(peers):
    barrier = pltpu.get_barrier_semaphore()
    for peer in peers:
        pl.semaphore_signal(barrier, inc=1, device_id=peer, device_id_type=LOGICAL)
    pl.semaphore_wait(barrier, len(peers))


def whole_kernel(
    scale,
    init_in, brown_in, step_in, length_in, obs_in, observed_in, w_in, b_in, w_out, b_out_in, dec_in, prior_in, diff_in,
    elbo, out, tiny_out, ginit,
    wi, wo, bi, init, brown, step, length, obs, observed, b_out, dec, prior, diff,
    state, stepb, lenb, dr, obsb, obsf, acc, klacc, traj_t, acts, scaled, pre, back, upd_t,
    w_in_t, w_out_t, dec_t, cot, ob, sum_in, sum_out,
    big, small, tiny, got, cur, mid, r1, chain, r2, small_got, small_cur, s1, s2, tiny_got, tiny_cur, t1, t2, packed,
    wsend, wrecv, bsend, brecv, psend, precv, local, send, recv,
):
    steps, rows, width = brown.shape
    hidden = wi.shape[1]
    n_obs = obs.shape[0]
    loads = []

    def fetch(src, dst):
        copy = pltpu.make_async_copy(src, dst, local.at[len(loads)])
        copy.start()
        loads.append(copy)

    me = lax.axis_index("mp")
    depth, share = w_in.shape
    own_cols = pl.ds(pl.multiple_of(me * share, share), share)
    fetch(w_in, wi.at[:, own_cols])
    fetch(w_out, wo.at[own_cols, :])
    fetch(b_in, bi.at[own_cols])
    fetch(step_in, step)
    fetch(length_in, length)
    fetch(obs_in, obs)
    fetch(b_out_in, b_out)
    fetch(prior_in, prior)
    fetch(diff_in, diff)
    fetch(dec_in, dec)
    fetch(init_in, init)
    fetch(observed_in, observed)
    fetch(brown_in, brown)

    place = {a: lax.axis_index(AXES[a]) for a in "xyzc"}
    core = place["c"]
    mate = far("c", 1 - core)

    def other(axis, d):
        return lax.rem(place[axis] + d, 4)

    plane = [(da, db) for da in range(4) for db in range(4) if (da, db) != (0, 0)]
    plane.sort(key=lambda p: -sum(min(d, 4 - d) for d in p))

    def in_plane(axes, da, db):
        return {AXES[axes[0]]: other(axes[0], da), AXES[axes[1]]: other(axes[1], db)}

    peers = [far(a, other(a, d)) for a in "xyz" for d in (1, 2, 3)]
    peers += [in_plane(axes, *p) for axes in ("yz", "xz", "xy") for p in plane if 0 not in p]
    meet([mate] + peers)

    right, left, across = other("x", 1), other("x", 3), other("x", 2)
    half = depth // 2
    upper = pl.ds(pl.multiple_of(core * half, half), half)
    to_right, to_left = far("x", right), far("x", left)

    def at_in(block):
        return wi.at[upper, pl.ds(pl.multiple_of(block * share, share), share)]

    def at_out(block):
        return wo.at[pl.ds(pl.multiple_of(block * share + core * half, half), half), :]

    for copy in loads[:3]:
        copy.wait()
    own_in, own_out = at_in(me), at_out(me)
    in_r = remote(own_in, at_in(me), wsend.at[0], wrecv.at[0], to_right)
    out_l = remote(own_out, at_out(me), wsend.at[1], wrecv.at[1], to_left)
    out_r = remote(own_out, at_out(me), wsend.at[2], wrecv.at[2], to_right)
    in_l = remote(own_in, at_in(me), wsend.at[3], wrecv.at[3], to_left)
    own_bias = bi.at[own_cols]
    biases = [
        remote(own_bias, own_bias, bsend.at[d], brecv.at[d], far("x", other("x", d))) for d in (1, 2, 3)
    ]
    for copy in loads[3:-1]:
        copy.wait()

    stepb[...] = jnp.broadcast_to(step[...], (rows, rows)).T
    lenb[...] = jnp.broadcast_to(length[...], (rows, rows)).T
    dr[...] = diff[...] * twice(jnp.sqrt(stepb[...]))
    for j in range(n_obs):
        obsb[j] = jnp.broadcast_to(obs[j : j + 1, :], (rows, rows)).T
    dec_flip = dec[...].T
    dec_t[...] = jnp.concatenate([dec_flip, dec_flip], axis=0)
    klacc[...] = jnp.zeros_like(klacc)
    acc[...] = jnp.zeros_like(acc)
    sum_in[...] = jnp.zeros_like(sum_in)
    sum_out[...] = jnp.zeros_like(sum_out)
    tiny[...] = jnp.zeros_like(tiny)
    state[...] = init[...]
    inv = 1.0 / diff[...]
    obsf[...] = observed[...].astype(F32).reshape(rows * n_obs, dec.shape[1])

    sent = []

    def share_with_mate(n, ref):
        sent.append(remote(ref, ref, psend.at[n], precv.at[n], mate))

    in_r.wait_recv()
    in_rr = remote(at_in(left), at_in(left), wsend.at[4], wrecv.at[4], to_right)
    share_with_mate(0, at_in(left))
    out_l.wait_recv()
    out_ll = remote(at_out(right), at_out(right), wsend.at[5], wrecv.at[5], to_left)
    share_with_mate(1, at_out(right))
    out_r.wait_recv()
    share_with_mate(2, at_out(left))
    in_l.wait_recv()
    share_with_mate(3, at_in(right))
    in_rr.wait_recv()
    share_with_mate(4, at_in(across))
    out_ll.wait_recv()
    share_with_mate(5, at_out(across))
    for copy in biases + sent:
        copy.wait()
    for copy in (in_r, out_l, out_r, in_l, in_rr, out_ll):
        copy.wait_send()

    w_in_t[...] = wi[...].T
    w_out_t[...] = wo[...].T
    bias = bi[...].astype(F32).reshape(1, hidden)
    loads[-1].wait()

    def see(k, rounded):
        seen = mm(rounded, dec[...])
        for j in range(n_obs):
            acc[j] = jnp.where(obsb[j] == k, seen, acc[j])

    def at(k):
        return pl.ds(pl.multiple_of(k * rows, rows), rows)

    def forward(k, carry):
        s = state[...]
        rounded = s.astype(BF16)
        drift = b_out[...]
        for n in range(0, hidden, width):
            cs = slice(n, n + width)
            activity = jnp.tanh(mm(rounded, wi[:, cs]) + bias[:, cs]).astype(BF16)
            acts[at(k), cs] = activity
            drift = drift + mm(activity, wo[cs, :])
        live = lenb[...] > k
        factor = jnp.where(live, stepb[...], 0.0)
        residual = (drift + prior[...] * s) * inv
        noise = dr[...] * brown[k].astype(F32)
        state[...] = s + twice(factor) * drift + jnp.where(twice(live), noise, 0.0)
        scaled[k] = residual * inv
        square = residual * residual
        klacc[...] += (0.5 * factor) * (square[:, :rows] + square[:, rows:])
        traj_t[:, at(k)] = rounded.T
        see(k, rounded)
        return carry

    lax.fori_loop(0, steps, forward, 0, unroll=UNROLL)
    last = state[...].astype(BF16)
    traj_t[:, at(steps)] = last.T
    see(steps, last)

    total = jnp.zeros((rows, rows), F32)
    for j in range(n_obs):
        misfit = acc[j] - obsf[pl.ds(j, rows, stride=n_obs), :]
        total = total + misfit * misfit
        acc[j] = misfit.astype(BF16).astype(F32)
    loglik = -0.5 * total
    divisor = (width * lenb[...] + rows * n_obs).astype(F32)
    per_series = jnp.sum(loglik - klacc[...], axis=1, keepdims=True) / divisor
    elbo[...] = per_series.T[0:1, :]

    def gathered(k):
        m = jnp.zeros((rows, rows), F32)
        for j in range(n_obs):
            m = m + jnp.where(obsb[j] == k, acc[j], 0.0)
        high = m.astype(BF16)
        low = (m - high.astype(F32)).astype(BF16)
        return jnp.concatenate([high, low], axis=1)

    final = gathered(steps)
    back[at(steps), :] = final
    cot[...] = mm(final, dec_t[...])
    final = gathered(steps - 1)
    back[at(steps - 1), :] = final
    ob[...] = mm(final, dec_t[...])

    def backward(i, carry):
        k = steps - 1 - i
        c = cot[...]
        factor = twice(jnp.where(lenb[...] > k, stepb[...], 0.0))
        part = scaled[k]
        update = factor * (c + part)
        rounded = update.astype(BF16)
        value = acts[at(k), :].astype(F32)
        pre_grad = mm(rounded, w_out_t[...]) * (1.0 - value * value)
        pre_round = pre_grad.astype(BF16)
        ahead = ob[...]
        before = jnp.maximum(k - 1, 0)
        seen = gathered(before)
        ob[...] = mm(seen, dec_t[...])
        cot[...] = (c + factor * prior[...] * part + ahead) + mm(pre_round, w_in_t[...])
        pre[at(k), :] = pre_round
        back[at(before), :] = seen
        upd_t[:, at(k)] = rounded.T
        sum_in[...] += jnp.sum(pre_grad.reshape(rows // 8, 8, hidden), axis=0)
        sum_out[...] += jnp.sum(update.reshape(rows // 8, 8, width), axis=0)
        return carry

    lax.fori_loop(0, steps, backward, 0, unroll=UNROLL)
    ginit[...] = cot[...]

    pending = []
    first = {}
    flying = {}
    used = itertools.count()

    def go(src, dst, to, *key):
        n = next(used)
        copy = remote(src, dst, send.at[n], recv.at[n], to)
        pending.append(copy)
        flying.setdefault(key, []).append(copy)

    def landed(*key):
        for copy in flying[key]:
            copy.wait_recv()

    def along(dims, axis, index):
        return tuple(index if a == axis else slice(None) for a in dims)

    def grads(d, base, left_ref, right_ref):
        n = other("x", d)
        cols = pl.ds(pl.multiple_of(n * width, width), width)
        grad = mm(left_ref[:, : steps * rows], right_ref[:, cols]) * scale
        for u in (base, base + 1):
            h = u - base
            big[u, :, n] = grad[:, h * rows : (h + 1) * rows].reshape(2, 4, 4, 8, rows)
        for u in (base, base + 1):
            go(big.at[u, 1 - core, n], got.at[u, n], mate, "half", u, d)

    def halves(d, base):
        n = other("x", d)
        for u in (base, base + 1):
            landed("half", u, d)
            cur[u, n] = big[u, core, n] + got[u, n]
        return n

    def sideways(d):
        n = halves(d, 2)
        for e in (2, 1, 3):
            y, z = other("y", e), other("z", e)
            go(cur.at[2, n, y], r1.at[2, e - 1, n], far("y", y), "one", 2)
            go(cur.at[3, n, :, z], r1.at[3, e - 1, n], far("z", z), "one", 3)

    def relay(u, block, to):
        landed("across", u)
        chain[u, 1] = cur[u, block] + chain[u, 0]
        go(chain.at[u, 1], chain.at[u, 2], to, "one", u)

    grads(2, 0, traj_t, pre)
    grads(2, 2, upd_t, acts)
    grads(1, 2, upd_t, acts)
    halves(2, 0)
    go(cur.at[0, across], chain.at[0, 0], to_right, "across", 0)
    go(cur.at[1, across], chain.at[1, 0], to_left, "across", 1)
    grads(3, 2, upd_t, acts)
    sideways(2)
    grads(0, 2, upd_t, acts)
    sideways(1)
    grads(1, 0, traj_t, pre)
    sideways(3)
    grads(3, 0, traj_t, pre)
    sideways(0)
    grads(0, 0, traj_t, pre)
    halves(1, 0)
    go(cur.at[1, right], chain.at[1, 3], to_right, "one", 1)

    grad_dec = mm(traj_t[...], back[...]) * scale
    small[...] = (grad_dec[:, :rows] + grad_dec[:, rows:]).reshape(2, 4, 4, 8, rows)
    row_in = jnp.sum(sum_in[...], axis=0, keepdims=True) * scale
    row_out = jnp.sum(sum_out[...], axis=0, keepdims=True) * scale
    for r in range(hidden // rows):
        tiny[0, r : r + 1, :] = row_in[:, r * rows : (r + 1) * rows]
    for r in range(width // rows):
        tiny[1, r : r + 1, :] = row_out[:, r * rows : (r + 1) * rows]
    for r, part in ((2, loglik), (3, klacc[...])):
        total = jnp.sum(jnp.sum(part, axis=0, keepdims=True), axis=1, keepdims=True) * scale
        tiny[1, r : r + 1, :] = jnp.broadcast_to(total, (1, rows))
    go(small.at[1 - core], small_got, mate, "half", "small")
    go(tiny.at[1 - core], tiny_got, mate, "half", "tiny")

    halves(3, 0)
    go(cur.at[0, left], chain.at[0, 3], to_left, "one", 0)
    relay(0, right, to_right)
    relay(1, left, to_left)
    halves(0, 0)
    landed("half", "small")
    small_cur[...] = small[core] + small_got[...]
    landed("half", "tiny")
    tiny_cur[0] = tiny[core] + tiny_got[...]
    for d in (2, 1, 3):
        to = far("y", other("y", d))
        go(small_cur.at[other("y", d)], s1.at[d - 1], to, "one", "small")
        go(tiny_cur.at[0], t1.at[place["y"]], to, "one", "tiny")

    for flow, members in (("x", (0, 1)), ("y", (2,)), ("z", (3,))):
        for u in members:
            landed("one", u)
            own = cur[(u,) + along("xyz", flow, place[flow])]
            if flow == "x":
                mid[u] = own + chain[u, 2] + chain[u, 3]
            else:
                mid[u] = own + r1[u, 0] + r1[u, 1] + r1[u, 2]
        axes = "xyz".replace(flow, "")
        us = pl.ds(members[0], len(members))
        for n, (da, db) in enumerate(plane):
            src = mid.at[us, other(axes[0], da), other(axes[1], db)]
            go(src, r2.at[n, us], in_plane(axes, da, db), "two", flow)

    landed("one", "tiny")
    t1[place["y"]] = tiny_cur[0]
    tiny_cur[1] = t1[0] + t1[1] + t1[2] + t1[3]
    landed("one", "small")
    small_got[0] = small_cur[place["y"]] + s1[0] + s1[1] + s1[2]
    for dx, dz in plane:
        to = in_plane("xz", dx, dz)
        go(small_got.at[0, other("z", dz)], s2.at[me, place["z"]], to, "two", "small")
    for d in (2, 1, 3):
        go(tiny_cur.at[1], t2.at[0, place["z"]], far("z", other("z", d)), "two", "tiny")
    def summed(parts):
        total = parts[0]
        for part in parts[1:]:
            total = total + part
        return total

    tiles = {}
    for flow, members in (("x", (0, 1)), ("y", (2,)), ("z", (3,))):
        landed("two", flow)
        axes = "xyz".replace(flow, "")
        for u in members:
            own = mid[u, place[axes[0]], place[axes[1]]]
            tiles[u] = summed([own] + [r2[n, u] for n in range(15)])
    landed("two", "small")
    s2[me, place["z"]] = small_got[0, place["z"]]
    landed("two", "tiny")
    t2[0, place["z"]] = tiny_cur[1]
    tiny_cur[2] = summed([t2[0, z] for z in range(4)])
    tiles[4] = summed([s2[x, z] for x in range(4) for z in range(4)])
    packed[...] = pack([tiles[t] for t in range(5)])

    home = out.at[core, place["y"], place["z"]]
    for n, (dy, dz) in enumerate(plane):
        go(packed, home, in_plane("yz", dy, dz), "all", n)
    for d in (2, 1, 3):
        go(tiny_cur.at[2], t2.at[1, me], far("x", other("x", d)), "all", "tiny")
    go(packed, home, mate, "last", "own")
    out[core, place["y"], place["z"]] = packed[...]
    for n, (dy, dz) in reversed(list(enumerate(plane))):
        landed("all", n)
        came = out.at[core, lax.rem(place["y"] + 4 - dy, 4), lax.rem(place["z"] + 4 - dz, 4)]
        go(came, came, mate, "last", n)
    landed("all", "tiny")
    t2[1, me] = tiny_cur[2]
    tiny_out[core] = summed([t2[1, x] for x in range(4)])
    go(tiny_out.at[core], tiny_out.at[core], mate, "last", "tiny")
    landed("last", "tiny")
    landed("last", "own")
    for n in range(len(plane)):
        landed("last", n)
    for copy in pending:
        copy.wait_send()


def whole(total, init, brown, step, length, obs, observed, w_in, b_in, w_out, b_out, dec, prior, diff):
    steps, rows, width = brown.shape
    hidden, n_obs = 4 * w_in.shape[1], obs.shape[1]
    vmem, dma = pltpu.VMEM, pltpu.SemaphoreType.DMA
    near, rest = pl.BlockSpec(memory_space=vmem), pl.BlockSpec(memory_space=pl.ANY)
    tile = (8, 128)
    return pl.pallas_call(
        functools.partial(whole_kernel, 1.0 / total),
        out_shape=(
            jax.ShapeDtypeStruct((1, rows), F32),
            jax.ShapeDtypeStruct((2, 4, 4, 48, 128), jnp.int16),
            jax.ShapeDtypeStruct((2,) + tile, F32),
            jax.ShapeDtypeStruct((rows, width), F32),
        ),
        in_specs=[rest] * 13,
        out_specs=[near] * 4,
        scratch_shapes=[
            vmem((width, hidden), BF16),
            vmem((hidden, width), BF16),
            vmem((hidden,), BF16),
            vmem(init.shape, F32),
            vmem(brown.shape, BF16),
            vmem((1, rows), F32),
            vmem((1, rows), jnp.int32),
            vmem((n_obs, rows), jnp.int32),
            vmem(observed.shape, BF16),
            vmem((1, width), F32),
            vmem(dec.shape, BF16),
            vmem((1, width), F32),
            vmem((1, width), F32),
            vmem((rows, width), F32),
            vmem((rows, rows), F32),
            vmem((rows, rows), jnp.int32),
            vmem((rows, width), F32),
            vmem((n_obs, rows, rows), jnp.int32),
            vmem((rows * n_obs, rows), F32),
            vmem((n_obs, rows, rows), F32),
            vmem((rows, rows), F32),
            vmem((width, (steps + 1) * rows), BF16),
            vmem((steps * rows, hidden), BF16),
            vmem((steps, rows, width), F32),
            vmem((steps * rows, hidden), BF16),
            vmem(((steps + 1) * rows, width), BF16),
            vmem((width, steps * rows), BF16),
            vmem((hidden, width), BF16),
            vmem((width, hidden), BF16),
            vmem((width, width), BF16),
            vmem((rows, width), F32),
            vmem((rows, width), F32),
            vmem((8, hidden), F32),
            vmem((8, width), F32),
            vmem((4, 2, 4, 4, 4) + tile, F32),
            vmem((2, 4, 4) + tile, F32),
            vmem((2,) + tile, F32),
            vmem((4, 4, 4, 4) + tile, F32),
            vmem((4, 4, 4, 4) + tile, F32),
            vmem((4, 4, 4) + tile, F32),
            vmem((4, 3, 4, 4) + tile, F32),
            vmem((2, 4, 4, 4) + tile, F32),
            vmem((15, 4) + tile, F32),
            vmem((4, 4) + tile, F32),
            vmem((4, 4) + tile, F32),
            vmem((3, 4) + tile, F32),
            vmem((4, 4) + tile, F32),
            vmem(tile, F32),
            vmem((3,) + tile, F32),
            vmem((4,) + tile, F32),
            vmem((2, 4) + tile, F32),
            vmem((48, 128), jnp.int16),
            dma((6,)), dma((6,)), dma((4,)), dma((4,)), dma((6,)), dma((6,)), dma((13,)),
            dma((COPIES,)), dma((COPIES,)),
        ],
        compiler_params=pltpu.CompilerParams(
            collective_id=0, has_side_effects=True, vmem_limit_bytes=58 * 1024 * 1024
        ),
        name="whole",
    )(
        init, brown, step.reshape(1, -1), length.reshape(1, -1), obs.T, observed, w_in,
        b_in, w_out, b_out.reshape(1, -1), dec, prior.reshape(1, -1), diff.reshape(1, -1),
    )


def finish_kernel(elbo_in, out, tiny, ginit_in, elbo, w_in, w_out, dec, b_in, b_out, scores, ginit, turn):
    me = lax.axis_index("mp")
    elbo[...] = elbo_in[...]
    ginit[...] = ginit_in[...]
    for n in range(32):
        block = out[n // 16, (n // 4) % 4, n % 4].astype(jnp.int32).astype(F32)
        rs = slice(n * 8, n * 8 + 8)
        part = [block[t * 8 : t * 8 + 8] * jnp.exp2(block[40 + t : 41 + t]) for t in range(5)]
        w_in[rs, :128] = part[0]
        w_in[rs, 128:] = part[1]
        turn[rs, :128] = part[2]
        turn[rs, 128:] = part[3]
        dec[rs, :] = part[4]
    w_out[...] = turn[...].T
    for r in range(2):
        b_in[:, r * 128 : (r + 1) * 128] = tiny[0, pl.ds(2 * me + r, 1), :]
        b_out[:, r * 128 : (r + 1) * 128] = tiny[1, r : r + 1, :]
    first = lax.broadcasted_iota(jnp.int32, (1, 128), 1) == 0
    both = jnp.where(first, tiny[1, 2:3, :], tiny[1, 3:4, :])
    scores[...] = both[:, :2]


def unpack(elbo, out, tiny, ginit):
    vmem = pltpu.VMEM
    return pl.pallas_call(
        finish_kernel,
        out_shape=tuple(
            jax.ShapeDtypeStruct(s, F32)
            for s in ((1, 128), (256, 256), (256, 256), (256, 128), (1, 256), (1, 256), (1, 2), (128, 256))
        ),
        in_specs=[pl.BlockSpec(memory_space=vmem)] * 4,
        out_specs=[pl.BlockSpec(memory_space=vmem)] * 8,
        scratch_shapes=[vmem((256, 256), F32)],
        name="unpack",
    )(elbo, out, tiny, ginit)


def on_device(
    init_state, brownian, step_size, lengths, obs_steps, observed,
    w_in, b_in, w_out, b_out, decoder, prior_rate, diffusion,
):
    total = init_state.shape[0] * lax.axis_size(BATCH_MP)
    elbo, parts, tiny, grad_init = whole(
        total, init_state, brownian, step_size, lengths, obs_steps, observed,
        w_in, b_in, w_out, b_out, decoder, prior_rate, diffusion,
    )
    elbo, own_in, own_out, grad_dec, own_b, grad_b_out, scores, grad_init = unpack(
        elbo, parts, tiny, grad_init
    )
    return (
        elbo.reshape(-1), scores.reshape(-1), own_in, own_b.reshape(-1), own_out, grad_b_out.reshape(-1),
        grad_dec, grad_init,
    )


def solution(mesh):
    torus = Mesh(
        mesh.devices.reshape(4, 4, 2, mesh.shape["mp"]), ("batch_0", "batch_1", "batch_2", "mp")
    )
    placed = (
        P(BATCH_MP, None), P(None, BATCH_MP, None), P(BATCH_MP), P(BATCH_MP), P(BATCH_MP, None),
        P(BATCH_MP, None, None), P(None, "mp"), P("mp"), P("mp", None), P(), P(), P(), P(),
    )
    return jax.shard_map(
        on_device,
        mesh=torus,
        in_specs=placed,
        out_specs=(
            P(BATCH_MP), P(), P(None, "mp"), P("mp"), P("mp", None), P(), P(), P(BATCH_MP, None),
        ),
        check_vma=False,
    )
```

```python
import functools
import itertools

import jax
import jax.numpy as jnp
from jax import lax
from jax.experimental import pallas as pl
from jax.experimental.pallas import tpu as pltpu
from jax.sharding import Mesh
from jax.sharding import PartitionSpec as P

BATCH_MP = ("batch_0", "batch_1", "batch_2", "mp")
F32, BF16 = jnp.float32, jnp.bfloat16
UNROLL = 8


def mm(a, b):
    return jnp.dot(a, b, preferred_element_type=F32)


def twice(a):
    return jnp.concatenate([a, a], axis=1)


AXES = {"x": "mp", "y": "batch_0", "z": "batch_1", "c": "batch_2"}
LOGICAL = pl.DeviceIdType.MESH
COPIES = 168


def pack(tiles):
    rows, marks = [], []
    for tile in tiles:
        top = jnp.max(jnp.max(jnp.abs(tile), axis=0, keepdims=True), axis=1, keepdims=True)
        power = jnp.ceil(jnp.log2(jnp.maximum(top, 1e-30) * (1.0 / 32000.0)))
        rows.append(jnp.floor(tile * jnp.exp2(-power) + 0.5))
        marks.append(jnp.broadcast_to(power, (1, 128)))
    marks.append(jnp.zeros((3, 128), F32))
    return jnp.concatenate(rows + marks, axis=0).astype(jnp.int32).astype(jnp.int16)


def far(axis, where):
    return {AXES[axis]: where}


def remote(src, dst, send, recv, to):
    copy = pltpu.make_async_remote_copy(
        src_ref=src, dst_ref=dst, send_sem=send, recv_sem=recv, device_id=to, device_id_type=LOGICAL
    )
    copy.start()
    return copy


def meet(peers):
    barrier = pltpu.get_barrier_semaphore()
    for peer in peers:
        pl.semaphore_signal(barrier, inc=1, device_id=peer, device_id_type=LOGICAL)
    pl.semaphore_wait(barrier, len(peers))


def whole_kernel(
    scale,
    init_in, brown_in, step_in, length_in, obs_in, observed_in, w_in, b_in, w_out, b_out_in, dec_in, prior_in, diff_in,
    elbo, out, tiny_out, ginit,
    wi, wo, bi, init, brown, step, length, obs, observed, b_out, dec, prior, diff,
    state, stepb, lenb, dr, obsb, obsf, acc, klacc, traj_t, acts, scaled, pre, back, upd_t,
    w_in_t, w_out_t, dec_t, cot, ob, sum_in, sum_out,
    big, small, tiny, got, cur, mid, r1, chain, r2, small_got, small_cur, s1, s2, tiny_got, tiny_cur, t1, t2, packed,
    wsend, wrecv, bsend, brecv, psend, precv, local, send, recv,
):
    steps, rows, width = brown.shape
    hidden = wi.shape[1]
    n_obs = obs.shape[0]
    loads = []

    def fetch(src, dst):
        copy = pltpu.make_async_copy(src, dst, local.at[len(loads)])
        copy.start()
        loads.append(copy)

    me = lax.axis_index("mp")
    depth, share = w_in.shape
    own_cols = pl.ds(pl.multiple_of(me * share, share), share)
    fetch(w_in, wi.at[:, own_cols])
    fetch(w_out, wo.at[own_cols, :])
    fetch(b_in, bi.at[own_cols])
    fetch(step_in, step)
    fetch(length_in, length)
    fetch(obs_in, obs)
    fetch(b_out_in, b_out)
    fetch(prior_in, prior)
    fetch(diff_in, diff)
    fetch(dec_in, dec)
    fetch(init_in, init)
    fetch(observed_in, observed)
    fetch(brown_in, brown)

    place = {a: lax.axis_index(AXES[a]) for a in "xyzc"}
    core = place["c"]
    mate = far("c", 1 - core)

    def other(axis, d):
        return lax.rem(place[axis] + d, 4)

    plane = [(da, db) for da in range(4) for db in range(4) if (da, db) != (0, 0)]
    plane.sort(key=lambda p: -sum(min(d, 4 - d) for d in p))

    def in_plane(axes, da, db):
        return {AXES[axes[0]]: other(axes[0], da), AXES[axes[1]]: other(axes[1], db)}

    peers = [far(a, other(a, d)) for a in "xyz" for d in (1, 2, 3)]
    peers += [in_plane(axes, *p) for axes in ("yz", "xz", "xy") for p in plane if 0 not in p]
    meet([mate] + peers)

    right, left, across = other("x", 1), other("x", 3), other("x", 2)
    half = depth // 2
    to_right, to_left = far("x", right), far("x", left)

    def at_in(block, part=0, parts=1):
        size = half // parts
        at_row = pl.ds(pl.multiple_of(core * half + part * size, size), size)
        return wi.at[at_row, pl.ds(pl.multiple_of(block * share, share), share)]

    def at_out(block, part=0, parts=1):
        size = half // parts
        return wo.at[pl.ds(pl.multiple_of(block * share + core * half + part * size, size), size), :]

    turns = itertools.count()

    def pass_on(ref, to):
        n = next(turns)
        return remote(ref, ref, wsend.at[n], wrecv.at[n], to)

    for copy in loads[:3]:
        copy.wait()
    in_r, out_l = [], []
    for p in range(2):
        in_r.append(pass_on(at_in(me, p, 2), to_right))
        out_l.append(pass_on(at_out(me, p, 2), to_left))
    out_r = pass_on(at_out(me), to_right)
    in_l = pass_on(at_in(me), to_left)
    own_bias = bi.at[own_cols]
    biases = [
        remote(own_bias, own_bias, bsend.at[d], brecv.at[d], far("x", other("x", d))) for d in (1, 2, 3)
    ]
    for copy in loads[3:-1]:
        copy.wait()

    stepb[...] = jnp.broadcast_to(step[...], (rows, rows)).T
    lenb[...] = jnp.broadcast_to(length[...], (rows, rows)).T
    dr[...] = diff[...] * twice(jnp.sqrt(stepb[...]))
    for j in range(n_obs):
        obsb[j] = jnp.broadcast_to(obs[j : j + 1, :], (rows, rows)).T
    dec_flip = dec[...].T
    dec_t[...] = jnp.concatenate([dec_flip, dec_flip], axis=0)
    klacc[...] = jnp.zeros_like(klacc)
    acc[...] = jnp.zeros_like(acc)
    sum_in[...] = jnp.zeros_like(sum_in)
    sum_out[...] = jnp.zeros_like(sum_out)
    tiny[...] = jnp.zeros_like(tiny)
    state[...] = init[...]
    inv = 1.0 / diff[...]
    obsf[...] = observed[...].astype(F32).reshape(rows * n_obs, dec.shape[1])

    sent = []

    def share_with_mate(ref):
        n = len(sent)
        sent.append(remote(ref, ref, psend.at[n], precv.at[n], mate))

    in_rr, out_ll = [], []
    for p in range(2):
        in_r[p].wait_recv()
        in_rr.append(pass_on(at_in(left, p, 2), to_right))
        share_with_mate(at_in(left, p, 2))
        out_l[p].wait_recv()
        out_ll.append(pass_on(at_out(right, p, 2), to_left))
        share_with_mate(at_out(right, p, 2))
    out_r.wait_recv()
    share_with_mate(at_out(left))
    in_l.wait_recv()
    share_with_mate(at_in(right))
    for p in range(2):
        in_rr[p].wait_recv()
        share_with_mate(at_in(across, p, 2))
        out_ll[p].wait_recv()
        share_with_mate(at_out(across, p, 2))
    for copy in biases + sent:
        copy.wait()
    for copy in in_r + out_l + [out_r, in_l] + in_rr + out_ll:
        copy.wait_send()

    w_in_t[...] = wi[...].T
    w_out_t[...] = wo[...].T
    bias = bi[...].astype(F32).reshape(1, hidden)
    loads[-1].wait()

    def see(k, rounded):
        seen = mm(rounded, dec[...])
        for j in range(n_obs):
            acc[j] = jnp.where(obsb[j] == k, seen, acc[j])

    def at(k):
        return pl.ds(pl.multiple_of(k * rows, rows), rows)

    def forward(k, carry):
        s = state[...]
        rounded = s.astype(BF16)
        drift = b_out[...]
        for n in range(0, hidden, width):
            cs = slice(n, n + width)
            activity = jnp.tanh(mm(rounded, wi[:, cs]) + bias[:, cs]).astype(BF16)
            acts[at(k), cs] = activity
            drift = drift + mm(activity, wo[cs, :])
        live = lenb[...] > k
        factor = jnp.where(live, stepb[...], 0.0)
        residual = (drift + prior[...] * s) * inv
        noise = dr[...] * brown[k].astype(F32)
        state[...] = s + twice(factor) * drift + jnp.where(twice(live), noise, 0.0)
        scaled[k] = residual
        traj_t[:, at(k)] = rounded.T
        see(k, rounded)
        return carry

    lax.fori_loop(0, steps, forward, 0, unroll=UNROLL)
    last = state[...].astype(BF16)
    traj_t[:, at(steps)] = last.T
    see(steps, last)

    total = jnp.zeros((rows, rows), F32)
    for j in range(n_obs):
        misfit = acc[j] - obsf[pl.ds(j, rows, stride=n_obs), :]
        total = total + misfit * misfit
        acc[j] = misfit.astype(BF16).astype(F32)
    loglik = -0.5 * total

    def gathered(k):
        m = jnp.zeros((rows, rows), F32)
        for j in range(n_obs):
            m = m + jnp.where(obsb[j] == k, acc[j], 0.0)
        high = m.astype(BF16)
        low = (m - high.astype(F32)).astype(BF16)
        return jnp.concatenate([high, low], axis=1)

    final = gathered(steps)
    back[at(steps), :] = final
    cot[...] = mm(final, dec_t[...])
    final = gathered(steps - 1)
    back[at(steps - 1), :] = final
    ob[...] = mm(final, dec_t[...])

    def backward(i, carry):
        k = steps - 1 - i
        c = cot[...]
        factor = twice(jnp.where(lenb[...] > k, stepb[...], 0.0))
        residual = scaled[k]
        square = residual * residual
        klacc[...] += (0.5 * factor[:, :rows]) * (square[:, :rows] + square[:, rows:])
        part = residual * inv
        update = factor * (c + part)
        rounded = update.astype(BF16)
        value = acts[at(k), :].astype(F32)
        pre_grad = mm(rounded, w_out_t[...]) * (1.0 - value * value)
        pre_round = pre_grad.astype(BF16)
        ahead = ob[...]
        before = jnp.maximum(k - 1, 0)
        seen = gathered(before)
        ob[...] = mm(seen, dec_t[...])
        cot[...] = (c + factor * prior[...] * part + ahead) + mm(pre_round, w_in_t[...])
        pre[at(k), :] = pre_round
        back[at(before), :] = seen
        upd_t[:, at(k)] = rounded.T
        sum_in[...] += jnp.sum(pre_grad.reshape(rows // 8, 8, hidden), axis=0)
        sum_out[...] += jnp.sum(update.reshape(rows // 8, 8, width), axis=0)
        return carry

    lax.fori_loop(0, steps, backward, 0, unroll=UNROLL)
    ginit[...] = cot[...]
    divisor = (width * lenb[...] + rows * n_obs).astype(F32)
    per_series = jnp.sum(loglik - klacc[...], axis=1, keepdims=True) / divisor
    elbo[...] = per_series.T[0:1, :]

    pending = []
    first = {}
    flying = {}
    used = itertools.count()

    def go(src, dst, to, *key):
        n = next(used)
        copy = remote(src, dst, send.at[n], recv.at[n], to)
        pending.append(copy)
        flying.setdefault(key, []).append(copy)

    def landed(*key):
        for copy in flying[key]:
            copy.wait_recv()

    def along(dims, axis, index):
        return tuple(index if a == axis else slice(None) for a in dims)

    def grads(d, base, left_ref, right_ref):
        n = other("x", d)
        cols = pl.ds(pl.multiple_of(n * width, width), width)
        grad = mm(left_ref[:, : steps * rows], right_ref[:, cols]) * scale
        for u in (base, base + 1):
            h = u - base
            big[u, :, n] = grad[:, h * rows : (h + 1) * rows].reshape(2, 4, 4, 8, rows)
        for u in (base, base + 1):
            go(big.at[u, 1 - core, n], got.at[u, n], mate, "half", u, d)

    def halves(d, base):
        n = other("x", d)
        for u in (base, base + 1):
            landed("half", u, d)
            cur[u, n] = big[u, core, n] + got[u, n]
        return n

    def sideways(d):
        n = halves(d, 2)
        for e in (2, 1, 3):
            y, z = other("y", e), other("z", e)
            go(cur.at[2, n, y], r1.at[2, e - 1, n], far("y", y), "one", 2)
            go(cur.at[3, n, :, z], r1.at[3, e - 1, n], far("z", z), "one", 3)

    def relay(u, block, to):
        landed("across", u)
        chain[u, 1] = cur[u, block] + chain[u, 0]
        go(chain.at[u, 1], chain.at[u, 2], to, "one", u)

    grads(2, 0, traj_t, pre)
    grads(2, 2, upd_t, acts)
    grads(1, 2, upd_t, acts)
    halves(2, 0)
    go(cur.at[0, across], chain.at[0, 0], to_right, "across", 0)
    go(cur.at[1, across], chain.at[1, 0], to_left, "across", 1)
    grads(3, 2, upd_t, acts)
    sideways(2)
    grads(0, 2, upd_t, acts)
    sideways(1)
    grads(1, 0, traj_t, pre)
    sideways(3)
    grads(3, 0, traj_t, pre)
    sideways(0)
    grads(0, 0, traj_t, pre)
    halves(1, 0)
    go(cur.at[1, right], chain.at[1, 3], to_right, "one", 1)

    grad_dec = mm(traj_t[...], back[...]) * scale
    small[...] = (grad_dec[:, :rows] + grad_dec[:, rows:]).reshape(2, 4, 4, 8, rows)
    row_in = jnp.sum(sum_in[...], axis=0, keepdims=True) * scale
    row_out = jnp.sum(sum_out[...], axis=0, keepdims=True) * scale
    for r in range(hidden // rows):
        tiny[0, r : r + 1, :] = row_in[:, r * rows : (r + 1) * rows]
    for r in range(width // rows):
        tiny[1, r : r + 1, :] = row_out[:, r * rows : (r + 1) * rows]
    for r, part in ((2, loglik), (3, klacc[...])):
        total = jnp.sum(jnp.sum(part, axis=0, keepdims=True), axis=1, keepdims=True) * scale
        tiny[1, r : r + 1, :] = jnp.broadcast_to(total, (1, rows))
    go(small.at[1 - core], small_got, mate, "half", "small")
    go(tiny.at[1 - core], tiny_got, mate, "half", "tiny")

    halves(3, 0)
    go(cur.at[0, left], chain.at[0, 3], to_left, "one", 0)
    relay(0, right, to_right)
    relay(1, left, to_left)
    halves(0, 0)
    landed("half", "small")
    small_cur[...] = small[core] + small_got[...]
    landed("half", "tiny")
    tiny_cur[0] = tiny[core] + tiny_got[...]
    for d in (2, 1, 3):
        to = far("y", other("y", d))
        go(small_cur.at[other("y", d)], s1.at[d - 1], to, "one", "small")
        go(tiny_cur.at[0], t1.at[place["y"]], to, "one", "tiny")

    for flow, members in (("x", (0, 1)), ("y", (2,)), ("z", (3,))):
        for u in members:
            landed("one", u)
            own = cur[(u,) + along("xyz", flow, place[flow])]
            if flow == "x":
                mid[u] = own + chain[u, 2] + chain[u, 3]
            else:
                mid[u] = own + r1[u, 0] + r1[u, 1] + r1[u, 2]
        axes = "xyz".replace(flow, "")
        us = pl.ds(members[0], len(members))
        for n, (da, db) in enumerate(plane):
            src = mid.at[us, other(axes[0], da), other(axes[1], db)]
            go(src, r2.at[n, us], in_plane(axes, da, db), "two", flow)

    landed("one", "tiny")
    t1[place["y"]] = tiny_cur[0]
    tiny_cur[1] = t1[0] + t1[1] + t1[2] + t1[3]
    landed("one", "small")
    small_got[0] = small_cur[place["y"]] + s1[0] + s1[1] + s1[2]
    for dx, dz in plane:
        to = in_plane("xz", dx, dz)
        go(small_got.at[0, other("z", dz)], s2.at[me, place["z"]], to, "two", "small")
    for d in (2, 1, 3):
        go(tiny_cur.at[1], t2.at[0, place["z"]], far("z", other("z", d)), "two", "tiny")
    def summed(parts):
        total = parts[0]
        for part in parts[1:]:
            total = total + part
        return total

    tiles = {}
    for flow, members in (("x", (0, 1)), ("y", (2,)), ("z", (3,))):
        landed("two", flow)
        axes = "xyz".replace(flow, "")
        for u in members:
            own = mid[u, place[axes[0]], place[axes[1]]]
            tiles[u] = summed([own] + [r2[n, u] for n in range(15)])
    landed("two", "small")
    s2[me, place["z"]] = small_got[0, place["z"]]
    landed("two", "tiny")
    t2[0, place["z"]] = tiny_cur[1]
    tiny_cur[2] = summed([t2[0, z] for z in range(4)])
    tiles[4] = summed([s2[x, z] for x in range(4) for z in range(4)])
    packed[...] = pack([tiles[t] for t in range(5)])

    home = out.at[core, place["y"], place["z"]]
    for n, (dy, dz) in enumerate(plane):
        go(packed, home, in_plane("yz", dy, dz), "all", n)
    for d in (2, 1, 3):
        go(tiny_cur.at[2], t2.at[1, me], far("x", other("x", d)), "all", "tiny")
    go(packed, home, mate, "last", "own")
    out[core, place["y"], place["z"]] = packed[...]
    for n, (dy, dz) in reversed(list(enumerate(plane))):
        landed("all", n)
        came = out.at[core, lax.rem(place["y"] + 4 - dy, 4), lax.rem(place["z"] + 4 - dz, 4)]
        go(came, came, mate, "last", n)
    landed("all", "tiny")
    t2[1, me] = tiny_cur[2]
    tiny_out[core] = summed([t2[1, x] for x in range(4)])
    go(tiny_out.at[core], tiny_out.at[core], mate, "last", "tiny")
    landed("last", "tiny")
    landed("last", "own")
    for n in range(len(plane)):
        landed("last", n)
    for copy in pending:
        copy.wait_send()


def whole(total, init, brown, step, length, obs, observed, w_in, b_in, w_out, b_out, dec, prior, diff):
    steps, rows, width = brown.shape
    hidden, n_obs = 4 * w_in.shape[1], obs.shape[1]
    vmem, dma = pltpu.VMEM, pltpu.SemaphoreType.DMA
    near, rest = pl.BlockSpec(memory_space=vmem), pl.BlockSpec(memory_space=pl.ANY)
    tile = (8, 128)
    return pl.pallas_call(
        functools.partial(whole_kernel, 1.0 / total),
        out_shape=(
            jax.ShapeDtypeStruct((1, rows), F32),
            jax.ShapeDtypeStruct((2, 4, 4, 48, 128), jnp.int16),
            jax.ShapeDtypeStruct((2,) + tile, F32),
            jax.ShapeDtypeStruct((rows, width), F32),
        ),
        in_specs=[rest] * 13,
        out_specs=[near] * 4,
        scratch_shapes=[
            vmem((width, hidden), BF16),
            vmem((hidden, width), BF16),
            vmem((hidden,), BF16),
            vmem(init.shape, F32),
            vmem(brown.shape, BF16),
            vmem((1, rows), F32),
            vmem((1, rows), jnp.int32),
            vmem((n_obs, rows), jnp.int32),
            vmem(observed.shape, BF16),
            vmem((1, width), F32),
            vmem(dec.shape, BF16),
            vmem((1, width), F32),
            vmem((1, width), F32),
            vmem((rows, width), F32),
            vmem((rows, rows), F32),
            vmem((rows, rows), jnp.int32),
            vmem((rows, width), F32),
            vmem((n_obs, rows, rows), jnp.int32),
            vmem((rows * n_obs, rows), F32),
            vmem((n_obs, rows, rows), F32),
            vmem((rows, rows), F32),
            vmem((width, (steps + 1) * rows), BF16),
            vmem((steps * rows, hidden), BF16),
            vmem((steps, rows, width), F32),
            vmem((steps * rows, hidden), BF16),
            vmem(((steps + 1) * rows, width), BF16),
            vmem((width, steps * rows), BF16),
            vmem((hidden, width), BF16),
            vmem((width, hidden), BF16),
            vmem((width, width), BF16),
            vmem((rows, width), F32),
            vmem((rows, width), F32),
            vmem((8, hidden), F32),
            vmem((8, width), F32),
            vmem((4, 2, 4, 4, 4) + tile, F32),
            vmem((2, 4, 4) + tile, F32),
            vmem((2,) + tile, F32),
            vmem((4, 4, 4, 4) + tile, F32),
            vmem((4, 4, 4, 4) + tile, F32),
            vmem((4, 4, 4) + tile, F32),
            vmem((4, 3, 4, 4) + tile, F32),
            vmem((2, 4, 4, 4) + tile, F32),
            vmem((15, 4) + tile, F32),
            vmem((4, 4) + tile, F32),
            vmem((4, 4) + tile, F32),
            vmem((3, 4) + tile, F32),
            vmem((4, 4) + tile, F32),
            vmem(tile, F32),
            vmem((3,) + tile, F32),
            vmem((4,) + tile, F32),
            vmem((2, 4) + tile, F32),
            vmem((48, 128), jnp.int16),
            dma((10,)), dma((10,)), dma((4,)), dma((4,)), dma((10,)), dma((10,)), dma((13,)),
            dma((COPIES,)), dma((COPIES,)),
        ],
        compiler_params=pltpu.CompilerParams(
            collective_id=0, has_side_effects=True, vmem_limit_bytes=58 * 1024 * 1024
        ),
        name="whole",
    )(
        init, brown, step.reshape(1, -1), length.reshape(1, -1), obs.T, observed, w_in,
        b_in, w_out, b_out.reshape(1, -1), dec, prior.reshape(1, -1), diff.reshape(1, -1),
    )


def finish_kernel(elbo_in, out, tiny, ginit_in, elbo, w_in, w_out, dec, b_in, b_out, scores, ginit, turn):
    me = lax.axis_index("mp")
    elbo[...] = elbo_in[...]
    ginit[...] = ginit_in[...]
    for n in range(32):
        block = out[n // 16, (n // 4) % 4, n % 4].astype(jnp.int32).astype(F32)
        rs = slice(n * 8, n * 8 + 8)
        part = [block[t * 8 : t * 8 + 8] * jnp.exp2(block[40 + t : 41 + t]) for t in range(5)]
        w_in[rs, :128] = part[0]
        w_in[rs, 128:] = part[1]
        turn[rs, :128] = part[2]
        turn[rs, 128:] = part[3]
        dec[rs, :] = part[4]
    w_out[...] = turn[...].T
    for r in range(2):
        b_in[:, r * 128 : (r + 1) * 128] = tiny[0, pl.ds(2 * me + r, 1), :]
        b_out[:, r * 128 : (r + 1) * 128] = tiny[1, r : r + 1, :]
    first = lax.broadcasted_iota(jnp.int32, (1, 128), 1) == 0
    both = jnp.where(first, tiny[1, 2:3, :], tiny[1, 3:4, :])
    scores[...] = both[:, :2]


def unpack(elbo, out, tiny, ginit):
    vmem = pltpu.VMEM
    return pl.pallas_call(
        finish_kernel,
        out_shape=tuple(
            jax.ShapeDtypeStruct(s, F32)
            for s in ((1, 128), (256, 256), (256, 256), (256, 128), (1, 256), (1, 256), (1, 2), (128, 256))
        ),
        in_specs=[pl.BlockSpec(memory_space=vmem)] * 4,
        out_specs=[pl.BlockSpec(memory_space=vmem)] * 8,
        scratch_shapes=[vmem((256, 256), F32)],
        name="unpack",
    )(elbo, out, tiny, ginit)


def on_device(
    init_state, brownian, step_size, lengths, obs_steps, observed,
    w_in, b_in, w_out, b_out, decoder, prior_rate, diffusion,
):
    total = init_state.shape[0] * lax.axis_size(BATCH_MP)
    elbo, parts, tiny, grad_init = whole(
        total, init_state, brownian, step_size, lengths, obs_steps, observed,
        w_in, b_in, w_out, b_out, decoder, prior_rate, diffusion,
    )
    elbo, own_in, own_out, grad_dec, own_b, grad_b_out, scores, grad_init = unpack(
        elbo, parts, tiny, grad_init
    )
    return (
        elbo.reshape(-1), scores.reshape(-1), own_in, own_b.reshape(-1), own_out, grad_b_out.reshape(-1),
        grad_dec, grad_init,
    )


def solution(mesh):
    torus = Mesh(
        mesh.devices.reshape(4, 4, 2, mesh.shape["mp"]), ("batch_0", "batch_1", "batch_2", "mp")
    )
    placed = (
        P(BATCH_MP, None), P(None, BATCH_MP, None), P(BATCH_MP), P(BATCH_MP), P(BATCH_MP, None),
        P(BATCH_MP, None, None), P(None, "mp"), P("mp"), P("mp", None), P(), P(), P(), P(),
    )
    return jax.shard_map(
        on_device,
        mesh=torus,
        in_specs=placed,
        out_specs=(
            P(BATCH_MP), P(), P(None, "mp"), P("mp"), P("mp", None), P(), P(), P(BATCH_MP, None),
        ),
        check_vma=False,
    )
```

```python
import functools
import itertools

import jax
import jax.numpy as jnp
from jax import lax
from jax.experimental import pallas as pl
from jax.experimental.pallas import tpu as pltpu
from jax.sharding import Mesh
from jax.sharding import PartitionSpec as P

BATCH_MP = ("batch_0", "batch_1", "batch_2", "mp")
F32, BF16 = jnp.float32, jnp.bfloat16
UNROLL = 8


def mm(a, b):
    return jnp.dot(a, b, preferred_element_type=F32)


def twice(a):
    return jnp.concatenate([a, a], axis=1)


AXES = {"x": "mp", "y": "batch_0", "z": "batch_1", "c": "batch_2"}
LOGICAL = pl.DeviceIdType.MESH
COPIES = 168


def pack(tiles):
    rows, marks = [], []
    for tile in tiles:
        top = jnp.max(jnp.max(jnp.abs(tile), axis=0, keepdims=True), axis=1, keepdims=True)
        power = jnp.ceil(jnp.log2(jnp.maximum(top, 1e-30) * (1.0 / 32000.0)))
        rows.append(jnp.floor(tile * jnp.exp2(-power) + 0.5))
        marks.append(jnp.broadcast_to(power, (1, 128)))
    marks.append(jnp.zeros((3, 128), F32))
    return jnp.concatenate(rows + marks, axis=0).astype(jnp.int32).astype(jnp.int16)


def far(axis, where):
    return {AXES[axis]: where}


def remote(src, dst, send, recv, to):
    copy = pltpu.make_async_remote_copy(
        src_ref=src, dst_ref=dst, send_sem=send, recv_sem=recv, device_id=to, device_id_type=LOGICAL
    )
    copy.start()
    return copy


def meet(peers):
    barrier = pltpu.get_barrier_semaphore()
    for peer in peers:
        pl.semaphore_signal(barrier, inc=1, device_id=peer, device_id_type=LOGICAL)
    pl.semaphore_wait(barrier, len(peers))


def whole_kernel(
    scale,
    init_in, brown_in, step_in, length_in, obs_in, observed_in, w_in, b_in, w_out, b_out_in, dec_in, prior_in, diff_in,
    elbo, out, tiny_out, ginit,
    wi, wo, bi, init, brown, step, length, obs, observed, b_out, dec, prior, diff,
    state, stepb, lenb, dr, obsb, obsf, acc, klacc, traj_t, acts, scaled, pre, back, upd_t,
    w_in_t, w_out_t, dec_t, cot, ob, sum_in, sum_out,
    big, small, tiny, got, cur, mid, r1, chain, r2, small_got, small_cur, s1, s2, tiny_got, tiny_cur, t1, t2, packed,
    wsend, wrecv, bsend, brecv, psend, precv, local, send, recv,
):
    steps, rows, width = brown.shape
    hidden = wi.shape[1]
    n_obs = obs.shape[0]
    loads = []

    def fetch(src, dst):
        copy = pltpu.make_async_copy(src, dst, local.at[len(loads)])
        copy.start()
        loads.append(copy)

    me = lax.axis_index("mp")
    depth, share = w_in.shape
    own_cols = pl.ds(pl.multiple_of(me * share, share), share)
    fetch(w_in, wi.at[:, own_cols])
    fetch(w_out, wo.at[own_cols, :])
    fetch(b_in, bi.at[own_cols])
    fetch(step_in, step)
    fetch(length_in, length)
    fetch(obs_in, obs)
    fetch(b_out_in, b_out)
    fetch(prior_in, prior)
    fetch(diff_in, diff)
    fetch(dec_in, dec)
    fetch(init_in, init)
    fetch(observed_in, observed)
    fetch(brown_in, brown)

    place = {a: lax.axis_index(AXES[a]) for a in "xyzc"}
    core = place["c"]
    mate = far("c", 1 - core)

    def other(axis, d):
        return lax.rem(place[axis] + d, 4)

    plane = [(da, db) for da in range(4) for db in range(4) if (da, db) != (0, 0)]
    plane.sort(key=lambda p: -sum(min(d, 4 - d) for d in p))

    def in_plane(axes, da, db):
        return {AXES[axes[0]]: other(axes[0], da), AXES[axes[1]]: other(axes[1], db)}

    peers = [far(a, other(a, d)) for a in "xyz" for d in (1, 2, 3)]
    peers += [in_plane(axes, *p) for axes in ("yz", "xz", "xy") for p in plane if 0 not in p]
    meet([mate] + peers)

    right, left, across = other("x", 1), other("x", 3), other("x", 2)
    half = depth // 2
    to_right, to_left = far("x", right), far("x", left)

    def at_in(block, part=0, parts=1):
        size = half // parts
        at_row = pl.ds(pl.multiple_of(core * half + part * size, size), size)
        return wi.at[at_row, pl.ds(pl.multiple_of(block * share, share), share)]

    def at_out(block, part=0, parts=1):
        size = half // parts
        return wo.at[pl.ds(pl.multiple_of(block * share + core * half + part * size, size), size), :]

    turns = itertools.count()

    def pass_on(ref, to):
        n = next(turns)
        return remote(ref, ref, wsend.at[n], wrecv.at[n], to)

    for copy in loads[:3]:
        copy.wait()
    in_r, out_l = [], []
    for p in range(2):
        in_r.append(pass_on(at_in(me, p, 2), to_right))
        out_l.append(pass_on(at_out(me, p, 2), to_left))
    out_r = pass_on(at_out(me), to_right)
    in_l = pass_on(at_in(me), to_left)
    own_bias = bi.at[own_cols]
    biases = [
        remote(own_bias, own_bias, bsend.at[d], brecv.at[d], far("x", other("x", d))) for d in (1, 2, 3)
    ]
    for copy in loads[3:-1]:
        copy.wait()

    stepb[...] = jnp.broadcast_to(step[...], (rows, rows)).T
    lenb[...] = jnp.broadcast_to(length[...], (rows, rows)).T
    dr[...] = diff[...] * twice(jnp.sqrt(stepb[...]))
    for j in range(n_obs):
        obsb[j] = jnp.broadcast_to(obs[j : j + 1, :], (rows, rows)).T
    dec_flip = dec[...].T
    dec_t[...] = jnp.concatenate([dec_flip, dec_flip], axis=0)
    klacc[...] = jnp.zeros_like(klacc)
    acc[...] = jnp.zeros_like(acc)
    sum_in[...] = jnp.zeros_like(sum_in)
    sum_out[...] = jnp.zeros_like(sum_out)
    tiny[...] = jnp.zeros_like(tiny)
    state[...] = init[...]
    inv = 1.0 / diff[...]
    obsf[...] = observed[...].astype(F32).reshape(rows * n_obs, dec.shape[1])

    sent = []

    def share_with_mate(ref):
        n = len(sent)
        sent.append(remote(ref, ref, psend.at[n], precv.at[n], mate))

    in_rr, out_ll = [], []
    for p in range(2):
        in_r[p].wait_recv()
        in_rr.append(pass_on(at_in(left, p, 2), to_right))
        share_with_mate(at_in(left, p, 2))
        out_l[p].wait_recv()
        out_ll.append(pass_on(at_out(right, p, 2), to_left))
        share_with_mate(at_out(right, p, 2))
    out_r.wait_recv()
    share_with_mate(at_out(left))
    in_l.wait_recv()
    share_with_mate(at_in(right))
    for p in range(2):
        in_rr[p].wait_recv()
        share_with_mate(at_in(across, p, 2))
        out_ll[p].wait_recv()
        share_with_mate(at_out(across, p, 2))
    for copy in biases + sent:
        copy.wait()
    for copy in in_r + out_l + [out_r, in_l] + in_rr + out_ll:
        copy.wait_send()

    w_in_t[...] = wi[...].T
    w_out_t[...] = wo[...].T
    bias = bi[...].astype(F32).reshape(1, hidden)
    loads[-1].wait()

    def see(k, rounded):
        seen = mm(rounded, dec[...])
        for j in range(n_obs):
            acc[j] = jnp.where(obsb[j] == k, seen, acc[j])

    def at(k):
        return pl.ds(pl.multiple_of(k * rows, rows), rows)

    def forward(k, carry):
        s = state[...]
        rounded = s.astype(BF16)
        drift = b_out[...]
        for n in range(0, hidden, width):
            cs = slice(n, n + width)
            activity = jnp.tanh(mm(rounded, wi[:, cs]) + bias[:, cs]).astype(BF16)
            acts[at(k), cs] = activity
            drift = drift + mm(activity, wo[cs, :])
        live = lenb[...] > k
        factor = jnp.where(live, stepb[...], 0.0)
        residual = (drift + prior[...] * s) * inv
        noise = dr[...] * brown[k].astype(F32)
        state[...] = s + twice(factor) * drift + jnp.where(twice(live), noise, 0.0)
        scaled[k] = residual
        traj_t[:, at(k)] = rounded.T
        see(k, rounded)
        return carry

    lax.fori_loop(0, steps, forward, 0, unroll=UNROLL)
    last = state[...].astype(BF16)
    traj_t[:, at(steps)] = last.T
    see(steps, last)

    total = jnp.zeros((rows, rows), F32)
    for j in range(n_obs):
        misfit = acc[j] - obsf[pl.ds(j, rows, stride=n_obs), :]
        total = total + misfit * misfit
        acc[j] = misfit.astype(BF16).astype(F32)
    loglik = -0.5 * total

    def gathered(k):
        m = jnp.zeros((rows, rows), F32)
        for j in range(n_obs):
            m = m + jnp.where(obsb[j] == k, acc[j], 0.0)
        high = m.astype(BF16)
        low = (m - high.astype(F32)).astype(BF16)
        return jnp.concatenate([high, low], axis=1)

    final = gathered(steps)
    back[at(steps), :] = final
    cot[...] = mm(final, dec_t[...])
    final = gathered(steps - 1)
    back[at(steps - 1), :] = final
    ob[...] = mm(final, dec_t[...])

    def backward(i, carry):
        k = steps - 1 - i
        c = cot[...]
        factor = twice(jnp.where(lenb[...] > k, stepb[...], 0.0))
        residual = scaled[k]
        square = residual * residual
        klacc[...] += (0.5 * factor[:, :rows]) * (square[:, :rows] + square[:, rows:])
        part = residual * inv
        update = factor * (c + part)
        rounded = update.astype(BF16)
        value = acts[at(k), :].astype(F32)
        pre_grad = mm(rounded, w_out_t[...]) * (1.0 - value * value)
        pre_round = pre_grad.astype(BF16)
        ahead = ob[...]
        before = jnp.maximum(k - 1, 0)
        seen = gathered(before)
        ob[...] = mm(seen, dec_t[...])
        cot[...] = (c + factor * prior[...] * part + ahead) + mm(pre_round, w_in_t[...])
        pre[at(k), :] = pre_round
        back[at(before), :] = seen
        upd_t[:, at(k)] = rounded.T
        sum_in[...] += jnp.sum(pre_grad.reshape(rows // 8, 8, hidden), axis=0)
        sum_out[...] += jnp.sum(update.reshape(rows // 8, 8, width), axis=0)
        return carry

    lax.fori_loop(0, steps, backward, 0, unroll=UNROLL)
    ginit[...] = cot[...]
    divisor = (width * lenb[...] + rows * n_obs).astype(F32)
    per_series = jnp.sum(loglik - klacc[...], axis=1, keepdims=True) / divisor
    elbo[...] = per_series.T[0:1, :]

    pending = []
    first = {}
    flying = {}
    used = itertools.count()

    def go(src, dst, to, *key):
        n = next(used)
        copy = remote(src, dst, send.at[n], recv.at[n], to)
        pending.append(copy)
        flying.setdefault(key, []).append(copy)

    def landed(*key):
        for copy in flying[key]:
            copy.wait_recv()

    def along(dims, axis, index):
        return tuple(index if a == axis else slice(None) for a in dims)

    ready = []

    def flush():
        for u, d in ready:
            n = other("x", d)
            go(big.at[u, 1 - core, n], got.at[u, n], mate, "half", u, d)
        ready.clear()

    def grads(d, base, left_ref, right_ref, between=()):
        n = other("x", d)
        cols = pl.ds(pl.multiple_of(n * width, width), width)
        grad = mm(left_ref[:, : steps * rows], right_ref[:, cols]) * scale
        flush()
        for task in between:
            task()
        for u in (base, base + 1):
            h = u - base
            big[u, :, n] = grad[:, h * rows : (h + 1) * rows].reshape(2, 4, 4, 8, rows)
            ready.append((u, d))

    def halves(d, base):
        n = other("x", d)
        for u in (base, base + 1):
            landed("half", u, d)
            cur[u, n] = big[u, core, n] + got[u, n]
        return n

    def sideways(d):
        n = halves(d, 2)
        for e in (2, 1, 3):
            y, z = other("y", e), other("z", e)
            go(cur.at[2, n, y], r1.at[2, e - 1, n], far("y", y), "one", 2)
            go(cur.at[3, n, :, z], r1.at[3, e - 1, n], far("z", z), "one", 3)

    def relay(u, block, to):
        landed("across", u)
        chain[u, 1] = cur[u, block] + chain[u, 0]
        go(chain.at[u, 1], chain.at[u, 2], to, "one", u)

    def send_across():
        halves(2, 0)
        go(cur.at[0, across], chain.at[0, 0], to_right, "across", 0)
        go(cur.at[1, across], chain.at[1, 0], to_left, "across", 1)

    grads(2, 0, traj_t, pre)
    grads(2, 2, upd_t, acts)
    grads(1, 2, upd_t, acts)
    grads(3, 2, upd_t, acts, [send_across])
    grads(0, 2, upd_t, acts, [lambda: sideways(2)])
    grads(1, 0, traj_t, pre, [lambda: sideways(1)])
    grads(3, 0, traj_t, pre, [lambda: sideways(3)])
    grads(0, 0, traj_t, pre, [lambda: sideways(0)])
    grad_dec = mm(traj_t[...], back[...]) * scale
    flush()
    halves(1, 0)
    go(cur.at[1, right], chain.at[1, 3], to_right, "one", 1)

    small[...] = (grad_dec[:, :rows] + grad_dec[:, rows:]).reshape(2, 4, 4, 8, rows)
    row_in = jnp.sum(sum_in[...], axis=0, keepdims=True) * scale
    row_out = jnp.sum(sum_out[...], axis=0, keepdims=True) * scale
    for r in range(hidden // rows):
        tiny[0, r : r + 1, :] = row_in[:, r * rows : (r + 1) * rows]
    for r in range(width // rows):
        tiny[1, r : r + 1, :] = row_out[:, r * rows : (r + 1) * rows]
    for r, part in ((2, loglik), (3, klacc[...])):
        total = jnp.sum(jnp.sum(part, axis=0, keepdims=True), axis=1, keepdims=True) * scale
        tiny[1, r : r + 1, :] = jnp.broadcast_to(total, (1, rows))
    go(small.at[1 - core], small_got, mate, "half", "small")
    go(tiny.at[1 - core], tiny_got, mate, "half", "tiny")

    halves(3, 0)
    go(cur.at[0, left], chain.at[0, 3], to_left, "one", 0)
    relay(0, right, to_right)
    relay(1, left, to_left)
    halves(0, 0)
    landed("half", "small")
    small_cur[...] = small[core] + small_got[...]
    landed("half", "tiny")
    tiny_cur[0] = tiny[core] + tiny_got[...]
    for d in (2, 1, 3):
        to = far("y", other("y", d))
        go(small_cur.at[other("y", d)], s1.at[d - 1], to, "one", "small")
        go(tiny_cur.at[0], t1.at[place["y"]], to, "one", "tiny")

    for flow, members in (("x", (0, 1)), ("y", (2,)), ("z", (3,))):
        for u in members:
            landed("one", u)
            own = cur[(u,) + along("xyz", flow, place[flow])]
            if flow == "x":
                mid[u] = own + chain[u, 2] + chain[u, 3]
            else:
                mid[u] = own + r1[u, 0] + r1[u, 1] + r1[u, 2]
        axes = "xyz".replace(flow, "")
        us = pl.ds(members[0], len(members))
        for n, (da, db) in enumerate(plane):
            src = mid.at[us, other(axes[0], da), other(axes[1], db)]
            go(src, r2.at[n, us], in_plane(axes, da, db), "two", flow)

    landed("one", "tiny")
    t1[place["y"]] = tiny_cur[0]
    tiny_cur[1] = t1[0] + t1[1] + t1[2] + t1[3]
    landed("one", "small")
    small_got[0] = small_cur[place["y"]] + s1[0] + s1[1] + s1[2]
    for dx, dz in plane:
        to = in_plane("xz", dx, dz)
        go(small_got.at[0, other("z", dz)], s2.at[me, place["z"]], to, "two", "small")
    for d in (2, 1, 3):
        go(tiny_cur.at[1], t2.at[0, place["z"]], far("z", other("z", d)), "two", "tiny")
    def summed(parts):
        total = parts[0]
        for part in parts[1:]:
            total = total + part
        return total

    tiles = {}
    for flow, members in (("x", (0, 1)), ("y", (2,)), ("z", (3,))):
        landed("two", flow)
        axes = "xyz".replace(flow, "")
        for u in members:
            own = mid[u, place[axes[0]], place[axes[1]]]
            tiles[u] = summed([own] + [r2[n, u] for n in range(15)])
    landed("two", "small")
    s2[me, place["z"]] = small_got[0, place["z"]]
    landed("two", "tiny")
    t2[0, place["z"]] = tiny_cur[1]
    tiny_cur[2] = summed([t2[0, z] for z in range(4)])
    tiles[4] = summed([s2[x, z] for x in range(4) for z in range(4)])
    packed[...] = pack([tiles[t] for t in range(5)])

    home = out.at[core, place["y"], place["z"]]
    for n, (dy, dz) in enumerate(plane):
        go(packed, home, in_plane("yz", dy, dz), "all", n)
    for d in (2, 1, 3):
        go(tiny_cur.at[2], t2.at[1, me], far("x", other("x", d)), "all", "tiny")
    go(packed, home, mate, "last", "own")
    out[core, place["y"], place["z"]] = packed[...]
    for n, (dy, dz) in reversed(list(enumerate(plane))):
        landed("all", n)
        came = out.at[core, lax.rem(place["y"] + 4 - dy, 4), lax.rem(place["z"] + 4 - dz, 4)]
        go(came, came, mate, "last", n)
    landed("all", "tiny")
    t2[1, me] = tiny_cur[2]
    tiny_out[core] = summed([t2[1, x] for x in range(4)])
    go(tiny_out.at[core], tiny_out.at[core], mate, "last", "tiny")
    landed("last", "tiny")
    landed("last", "own")
    for n in range(len(plane)):
        landed("last", n)
    for copy in pending:
        copy.wait_send()


def whole(total, init, brown, step, length, obs, observed, w_in, b_in, w_out, b_out, dec, prior, diff):
    steps, rows, width = brown.shape
    hidden, n_obs = 4 * w_in.shape[1], obs.shape[1]
    vmem, dma = pltpu.VMEM, pltpu.SemaphoreType.DMA
    near, rest = pl.BlockSpec(memory_space=vmem), pl.BlockSpec(memory_space=pl.ANY)
    tile = (8, 128)
    return pl.pallas_call(
        functools.partial(whole_kernel, 1.0 / total),
        out_shape=(
            jax.ShapeDtypeStruct((1, rows), F32),
            jax.ShapeDtypeStruct((2, 4, 4, 48, 128), jnp.int16),
            jax.ShapeDtypeStruct((2,) + tile, F32),
            jax.ShapeDtypeStruct((rows, width), F32),
        ),
        in_specs=[rest] * 13,
        out_specs=[near] * 4,
        scratch_shapes=[
            vmem((width, hidden), BF16),
            vmem((hidden, width), BF16),
            vmem((hidden,), BF16),
            vmem(init.shape, F32),
            vmem(brown.shape, BF16),
            vmem((1, rows), F32),
            vmem((1, rows), jnp.int32),
            vmem((n_obs, rows), jnp.int32),
            vmem(observed.shape, BF16),
            vmem((1, width), F32),
            vmem(dec.shape, BF16),
            vmem((1, width), F32),
            vmem((1, width), F32),
            vmem((rows, width), F32),
            vmem((rows, rows), F32),
            vmem((rows, rows), jnp.int32),
            vmem((rows, width), F32),
            vmem((n_obs, rows, rows), jnp.int32),
            vmem((rows * n_obs, rows), F32),
            vmem((n_obs, rows, rows), F32),
            vmem((rows, rows), F32),
            vmem((width, (steps + 1) * rows), BF16),
            vmem((steps * rows, hidden), BF16),
            vmem((steps, rows, width), F32),
            vmem((steps * rows, hidden), BF16),
            vmem(((steps + 1) * rows, width), BF16),
            vmem((width, steps * rows), BF16),
            vmem((hidden, width), BF16),
            vmem((width, hidden), BF16),
            vmem((width, width), BF16),
            vmem((rows, width), F32),
            vmem((rows, width), F32),
            vmem((8, hidden), F32),
            vmem((8, width), F32),
            vmem((4, 2, 4, 4, 4) + tile, F32),
            vmem((2, 4, 4) + tile, F32),
            vmem((2,) + tile, F32),
            vmem((4, 4, 4, 4) + tile, F32),
            vmem((4, 4, 4, 4) + tile, F32),
            vmem((4, 4, 4) + tile, F32),
            vmem((4, 3, 4, 4) + tile, F32),
            vmem((2, 4, 4, 4) + tile, F32),
            vmem((15, 4) + tile, F32),
            vmem((4, 4) + tile, F32),
            vmem((4, 4) + tile, F32),
            vmem((3, 4) + tile, F32),
            vmem((4, 4) + tile, F32),
            vmem(tile, F32),
            vmem((3,) + tile, F32),
            vmem((4,) + tile, F32),
            vmem((2, 4) + tile, F32),
            vmem((48, 128), jnp.int16),
            dma((10,)), dma((10,)), dma((4,)), dma((4,)), dma((10,)), dma((10,)), dma((13,)),
            dma((COPIES,)), dma((COPIES,)),
        ],
        compiler_params=pltpu.CompilerParams(
            collective_id=0, has_side_effects=True, vmem_limit_bytes=58 * 1024 * 1024
        ),
        name="whole",
    )(
        init, brown, step.reshape(1, -1), length.reshape(1, -1), obs.T, observed, w_in,
        b_in, w_out, b_out.reshape(1, -1), dec, prior.reshape(1, -1), diff.reshape(1, -1),
    )


def finish_kernel(elbo_in, out, tiny, ginit_in, elbo, w_in, w_out, dec, b_in, b_out, scores, ginit, turn):
    me = lax.axis_index("mp")
    elbo[...] = elbo_in[...]
    ginit[...] = ginit_in[...]
    for n in range(32):
        block = out[n // 16, (n // 4) % 4, n % 4].astype(jnp.int32).astype(F32)
        rs = slice(n * 8, n * 8 + 8)
        part = [block[t * 8 : t * 8 + 8] * jnp.exp2(block[40 + t : 41 + t]) for t in range(5)]
        w_in[rs, :128] = part[0]
        w_in[rs, 128:] = part[1]
        turn[rs, :128] = part[2]
        turn[rs, 128:] = part[3]
        dec[rs, :] = part[4]
    w_out[...] = turn[...].T
    for r in range(2):
        b_in[:, r * 128 : (r + 1) * 128] = tiny[0, pl.ds(2 * me + r, 1), :]
        b_out[:, r * 128 : (r + 1) * 128] = tiny[1, r : r + 1, :]
    first = lax.broadcasted_iota(jnp.int32, (1, 128), 1) == 0
    both = jnp.where(first, tiny[1, 2:3, :], tiny[1, 3:4, :])
    scores[...] = both[:, :2]


def unpack(elbo, out, tiny, ginit):
    vmem = pltpu.VMEM
    return pl.pallas_call(
        finish_kernel,
        out_shape=tuple(
            jax.ShapeDtypeStruct(s, F32)
            for s in ((1, 128), (256, 256), (256, 256), (256, 128), (1, 256), (1, 256), (1, 2), (128, 256))
        ),
        in_specs=[pl.BlockSpec(memory_space=vmem)] * 4,
        out_specs=[pl.BlockSpec(memory_space=vmem)] * 8,
        scratch_shapes=[vmem((256, 256), F32)],
        name="unpack",
    )(elbo, out, tiny, ginit)


def on_device(
    init_state, brownian, step_size, lengths, obs_steps, observed,
    w_in, b_in, w_out, b_out, decoder, prior_rate, diffusion,
):
    total = init_state.shape[0] * lax.axis_size(BATCH_MP)
    elbo, parts, tiny, grad_init = whole(
        total, init_state, brownian, step_size, lengths, obs_steps, observed,
        w_in, b_in, w_out, b_out, decoder, prior_rate, diffusion,
    )
    elbo, own_in, own_out, grad_dec, own_b, grad_b_out, scores, grad_init = unpack(
        elbo, parts, tiny, grad_init
    )
    return (
        elbo.reshape(-1), scores.reshape(-1), own_in, own_b.reshape(-1), own_out, grad_b_out.reshape(-1),
        grad_dec, grad_init,
    )


def solution(mesh):
    torus = Mesh(
        mesh.devices.reshape(4, 4, 2, mesh.shape["mp"]), ("batch_0", "batch_1", "batch_2", "mp")
    )
    placed = (
        P(BATCH_MP, None), P(None, BATCH_MP, None), P(BATCH_MP), P(BATCH_MP), P(BATCH_MP, None),
        P(BATCH_MP, None, None), P(None, "mp"), P("mp"), P("mp", None), P(), P(), P(), P(),
    )
    return jax.shard_map(
        on_device,
        mesh=torus,
        in_specs=placed,
        out_specs=(
            P(BATCH_MP), P(), P(None, "mp"), P("mp"), P("mp", None), P(), P(), P(BATCH_MP, None),
        ),
        check_vma=False,
    )
```

```python
import functools
import itertools

import jax
import jax.numpy as jnp
from jax import lax
from jax.experimental import pallas as pl
from jax.experimental.pallas import tpu as pltpu
from jax.sharding import Mesh
from jax.sharding import PartitionSpec as P

BATCH_MP = ("batch_0", "batch_1", "batch_2", "mp")
F32, BF16 = jnp.float32, jnp.bfloat16
UNROLL = 16


def mm(a, b):
    return jnp.dot(a, b, preferred_element_type=F32)


def twice(a):
    return jnp.concatenate([a, a], axis=1)


AXES = {"x": "mp", "y": "batch_0", "z": "batch_1", "c": "batch_2"}
LOGICAL = pl.DeviceIdType.MESH
COPIES = 168


def pack(tiles):
    rows, marks = [], []
    for tile in tiles:
        top = jnp.max(jnp.max(jnp.abs(tile), axis=0, keepdims=True), axis=1, keepdims=True)
        power = jnp.ceil(jnp.log2(jnp.maximum(top, 1e-30) * (1.0 / 32000.0)))
        rows.append(jnp.floor(tile * jnp.exp2(-power) + 0.5))
        marks.append(jnp.broadcast_to(power, (1, 128)))
    marks.append(jnp.zeros((3, 128), F32))
    return jnp.concatenate(rows + marks, axis=0).astype(jnp.int32).astype(jnp.int16)


def far(axis, where):
    return {AXES[axis]: where}


def remote(src, dst, send, recv, to):
    copy = pltpu.make_async_remote_copy(
        src_ref=src, dst_ref=dst, send_sem=send, recv_sem=recv, device_id=to, device_id_type=LOGICAL
    )
    copy.start()
    return copy


def meet(peers):
    barrier = pltpu.get_barrier_semaphore()
    for peer in peers:
        pl.semaphore_signal(barrier, inc=1, device_id=peer, device_id_type=LOGICAL)
    pl.semaphore_wait(barrier, len(peers))


def whole_kernel(
    scale,
    init_in, brown_in, step_in, length_in, obs_in, observed_in, w_in, b_in, w_out, b_out_in, dec_in, prior_in, diff_in,
    elbo, out, tiny_out, ginit,
    wi, wo, bi, init, brown, step, length, obs, observed, b_out, dec, prior, diff,
    state, stepb, lenb, dr, obsb, obsf, acc, klacc, traj_t, acts, scaled, pre, back, upd_t,
    w_in_t, w_out_t, dec_t, cot, ob, sum_in, sum_out,
    big, small, tiny, got, cur, mid, r1, chain, r2, small_got, small_cur, s1, s2, tiny_got, tiny_cur, t1, t2, packed,
    wsend, wrecv, bsend, brecv, psend, precv, local, send, recv,
):
    steps, rows, width = brown.shape
    hidden = wi.shape[1]
    n_obs = obs.shape[0]
    loads = []

    def fetch(src, dst):
        copy = pltpu.make_async_copy(src, dst, local.at[len(loads)])
        copy.start()
        loads.append(copy)

    me = lax.axis_index("mp")
    depth, share = w_in.shape
    own_cols = pl.ds(pl.multiple_of(me * share, share), share)
    fetch(w_in, wi.at[:, own_cols])
    fetch(w_out, wo.at[own_cols, :])
    fetch(b_in, bi.at[own_cols])
    fetch(step_in, step)
    fetch(length_in, length)
    fetch(obs_in, obs)
    fetch(b_out_in, b_out)
    fetch(prior_in, prior)
    fetch(diff_in, diff)
    fetch(dec_in, dec)
    fetch(init_in, init)
    fetch(observed_in, observed)
    fetch(brown_in, brown)

    place = {a: lax.axis_index(AXES[a]) for a in "xyzc"}
    core = place["c"]
    mate = far("c", 1 - core)

    def other(axis, d):
        return lax.rem(place[axis] + d, 4)

    plane = [(da, db) for da in range(4) for db in range(4) if (da, db) != (0, 0)]
    plane.sort(key=lambda p: -sum(min(d, 4 - d) for d in p))

    def in_plane(axes, da, db):
        return {AXES[axes[0]]: other(axes[0], da), AXES[axes[1]]: other(axes[1], db)}

    peers = [far(a, other(a, d)) for a in "xyz" for d in (1, 2, 3)]
    peers += [in_plane(axes, *p) for axes in ("yz", "xz", "xy") for p in plane if 0 not in p]
    meet([mate] + peers)

    right, left, across = other("x", 1), other("x", 3), other("x", 2)
    half = depth // 2
    to_right, to_left = far("x", right), far("x", left)

    def at_in(block, part=0, parts=1):
        size = half // parts
        at_row = pl.ds(pl.multiple_of(core * half + part * size, size), size)
        return wi.at[at_row, pl.ds(pl.multiple_of(block * share, share), share)]

    def at_out(block, part=0, parts=1):
        size = half // parts
        return wo.at[pl.ds(pl.multiple_of(block * share + core * half + part * size, size), size), :]

    turns = itertools.count()

    def pass_on(ref, to):
        n = next(turns)
        return remote(ref, ref, wsend.at[n], wrecv.at[n], to)

    for copy in loads[:3]:
        copy.wait()
    in_r, out_l = [], []
    for p in range(2):
        in_r.append(pass_on(at_in(me, p, 2), to_right))
        out_l.append(pass_on(at_out(me, p, 2), to_left))
    out_r = pass_on(at_out(me), to_right)
    in_l = pass_on(at_in(me), to_left)
    own_bias = bi.at[own_cols]
    biases = [
        remote(own_bias, own_bias, bsend.at[d], brecv.at[d], far("x", other("x", d))) for d in (1, 2, 3)
    ]
    for copy in loads[3:-1]:
        copy.wait()

    stepb[...] = jnp.broadcast_to(step[...], (rows, rows)).T
    lenb[...] = jnp.broadcast_to(length[...], (rows, rows)).T
    dr[...] = diff[...] * twice(jnp.sqrt(stepb[...]))
    for j in range(n_obs):
        obsb[j] = jnp.broadcast_to(obs[j : j + 1, :], (rows, rows)).T
    dec_flip = dec[...].T
    dec_t[...] = jnp.concatenate([dec_flip, dec_flip], axis=0)
    klacc[...] = jnp.zeros_like(klacc)
    acc[...] = jnp.zeros_like(acc)
    sum_in[...] = jnp.zeros_like(sum_in)
    sum_out[...] = jnp.zeros_like(sum_out)
    tiny[...] = jnp.zeros_like(tiny)
    state[...] = init[...]
    inv = 1.0 / diff[...]
    obsf[...] = observed[...].astype(F32).reshape(rows * n_obs, dec.shape[1])

    sent = []

    def share_with_mate(ref):
        n = len(sent)
        sent.append(remote(ref, ref, psend.at[n], precv.at[n], mate))

    in_rr, out_ll = [], []
    for p in range(2):
        in_r[p].wait_recv()
        in_rr.append(pass_on(at_in(left, p, 2), to_right))
        share_with_mate(at_in(left, p, 2))
        out_l[p].wait_recv()
        out_ll.append(pass_on(at_out(right, p, 2), to_left))
        share_with_mate(at_out(right, p, 2))
    out_r.wait_recv()
    share_with_mate(at_out(left))
    in_l.wait_recv()
    share_with_mate(at_in(right))
    for p in range(2):
        in_rr[p].wait_recv()
        share_with_mate(at_in(across, p, 2))
        out_ll[p].wait_recv()
        share_with_mate(at_out(across, p, 2))
    for copy in biases + sent:
        copy.wait()
    for copy in in_r + out_l + [out_r, in_l] + in_rr + out_ll:
        copy.wait_send()

    w_in_t[...] = wi[...].T
    w_out_t[...] = wo[...].T
    bias = bi[...].astype(F32).reshape(1, hidden)
    loads[-1].wait()

    def see(k, rounded):
        seen = mm(rounded, dec[...])
        for j in range(n_obs):
            acc[j] = jnp.where(obsb[j] == k, seen, acc[j])

    def at(k):
        return pl.ds(pl.multiple_of(k * rows, rows), rows)

    def forward(k, carry):
        s = carry
        rounded = s.astype(BF16)
        drift = b_out[...]
        for n in range(0, hidden, width):
            cs = slice(n, n + width)
            activity = jnp.tanh(mm(rounded, wi[:, cs]) + bias[:, cs]).astype(BF16)
            acts[at(k), cs] = activity
            drift = drift + mm(activity, wo[cs, :])
        live = lenb[...] > k
        factor = jnp.where(live, stepb[...], 0.0)
        residual = (drift + prior[...] * s) * inv
        noise = dr[...] * brown[k].astype(F32)
        following = s + twice(factor) * drift + jnp.where(twice(live), noise, 0.0)
        scaled[k] = residual
        traj_t[:, at(k)] = rounded.T
        see(k, rounded)
        return following

    state[...] = lax.fori_loop(0, steps, forward, state[...], unroll=UNROLL)
    last = state[...].astype(BF16)
    traj_t[:, at(steps)] = last.T
    see(steps, last)

    total = jnp.zeros((rows, rows), F32)
    for j in range(n_obs):
        misfit = acc[j] - obsf[pl.ds(j, rows, stride=n_obs), :]
        total = total + misfit * misfit
        acc[j] = misfit.astype(BF16).astype(F32)
    loglik = -0.5 * total

    def gathered(k):
        m = jnp.zeros((rows, rows), F32)
        for j in range(n_obs):
            m = m + jnp.where(obsb[j] == k, acc[j], 0.0)
        high = m.astype(BF16)
        low = (m - high.astype(F32)).astype(BF16)
        return jnp.concatenate([high, low], axis=1)

    final = gathered(steps)
    back[at(steps), :] = final
    cot[...] = mm(final, dec_t[...])
    final = gathered(steps - 1)
    back[at(steps - 1), :] = final
    ob[...] = mm(final, dec_t[...])

    def backward(i, carry):
        k = steps - 1 - i
        c = cot[...]
        factor = twice(jnp.where(lenb[...] > k, stepb[...], 0.0))
        residual = scaled[k]
        square = residual * residual
        klacc[...] += (0.5 * factor[:, :rows]) * (square[:, :rows] + square[:, rows:])
        part = residual * inv
        update = factor * (c + part)
        rounded = update.astype(BF16)
        value = acts[at(k), :].astype(F32)
        pre_grad = mm(rounded, w_out_t[...]) * (1.0 - value * value)
        pre_round = pre_grad.astype(BF16)
        ahead = ob[...]
        before = jnp.maximum(k - 1, 0)
        seen = gathered(before)
        ob[...] = mm(seen, dec_t[...])
        cot[...] = (c + factor * prior[...] * part + ahead) + mm(pre_round, w_in_t[...])
        pre[at(k), :] = pre_round
        back[at(before), :] = seen
        upd_t[:, at(k)] = rounded.T
        sum_in[...] += jnp.sum(pre_grad.reshape(rows // 8, 8, hidden), axis=0)
        sum_out[...] += jnp.sum(update.reshape(rows // 8, 8, width), axis=0)
        return carry

    lax.fori_loop(0, steps, backward, 0, unroll=UNROLL)
    ginit[...] = cot[...]
    divisor = (width * lenb[...] + rows * n_obs).astype(F32)
    per_series = jnp.sum(loglik - klacc[...], axis=1, keepdims=True) / divisor
    elbo[...] = per_series.T[0:1, :]

    pending = []
    first = {}
    flying = {}
    used = itertools.count()

    def go(src, dst, to, *key):
        n = next(used)
        copy = remote(src, dst, send.at[n], recv.at[n], to)
        pending.append(copy)
        flying.setdefault(key, []).append(copy)

    def landed(*key):
        for copy in flying[key]:
            copy.wait_recv()

    def along(dims, axis, index):
        return tuple(index if a == axis else slice(None) for a in dims)

    ready = []

    def flush():
        for u, d in ready:
            n = other("x", d)
            go(big.at[u, 1 - core, n], got.at[u, n], mate, "half", u, d)
        ready.clear()

    def grads(d, base, left_ref, right_ref, between=()):
        n = other("x", d)
        cols = pl.ds(pl.multiple_of(n * width, width), width)
        grad = mm(left_ref[:, : steps * rows], right_ref[:, cols]) * scale
        flush()
        for task in between:
            task()
        for u in (base, base + 1):
            h = u - base
            big[u, :, n] = grad[:, h * rows : (h + 1) * rows].reshape(2, 4, 4, 8, rows)
            ready.append((u, d))

    def halves(d, base):
        n = other("x", d)
        for u in (base, base + 1):
            landed("half", u, d)
            cur[u, n] = big[u, core, n] + got[u, n]
        return n

    def sideways(d):
        n = halves(d, 2)
        for e in (2, 1, 3):
            y, z = other("y", e), other("z", e)
            go(cur.at[2, n, y], r1.at[2, e - 1, n], far("y", y), "one", 2)
            go(cur.at[3, n, :, z], r1.at[3, e - 1, n], far("z", z), "one", 3)

    def relay(u, block, to):
        landed("across", u)
        chain[u, 1] = cur[u, block] + chain[u, 0]
        go(chain.at[u, 1], chain.at[u, 2], to, "one", u)

    def send_across():
        halves(2, 0)
        go(cur.at[0, across], chain.at[0, 0], to_right, "across", 0)
        go(cur.at[1, across], chain.at[1, 0], to_left, "across", 1)

    grads(2, 0, traj_t, pre)
    grads(2, 2, upd_t, acts)
    grads(1, 2, upd_t, acts)
    grads(3, 2, upd_t, acts, [send_across])
    grads(0, 2, upd_t, acts, [lambda: sideways(2)])
    grads(1, 0, traj_t, pre, [lambda: sideways(1)])
    grads(3, 0, traj_t, pre, [lambda: sideways(3)])
    grads(0, 0, traj_t, pre, [lambda: sideways(0)])
    grad_dec = mm(traj_t[...], back[...]) * scale
    flush()
    halves(1, 0)
    go(cur.at[1, right], chain.at[1, 3], to_right, "one", 1)

    small[...] = (grad_dec[:, :rows] + grad_dec[:, rows:]).reshape(2, 4, 4, 8, rows)
    row_in = jnp.sum(sum_in[...], axis=0, keepdims=True) * scale
    row_out = jnp.sum(sum_out[...], axis=0, keepdims=True) * scale
    for r in range(hidden // rows):
        tiny[0, r : r + 1, :] = row_in[:, r * rows : (r + 1) * rows]
    for r in range(width // rows):
        tiny[1, r : r + 1, :] = row_out[:, r * rows : (r + 1) * rows]
    for r, part in ((2, loglik), (3, klacc[...])):
        total = jnp.sum(jnp.sum(part, axis=0, keepdims=True), axis=1, keepdims=True) * scale
        tiny[1, r : r + 1, :] = jnp.broadcast_to(total, (1, rows))
    go(small.at[1 - core], small_got, mate, "half", "small")
    go(tiny.at[1 - core], tiny_got, mate, "half", "tiny")

    halves(3, 0)
    go(cur.at[0, left], chain.at[0, 3], to_left, "one", 0)
    relay(0, right, to_right)
    relay(1, left, to_left)
    halves(0, 0)
    landed("half", "small")
    small_cur[...] = small[core] + small_got[...]
    landed("half", "tiny")
    tiny_cur[0] = tiny[core] + tiny_got[...]
    for d in (2, 1, 3):
        to = far("y", other("y", d))
        go(small_cur.at[other("y", d)], s1.at[d - 1], to, "one", "small")
        go(tiny_cur.at[0], t1.at[place["y"]], to, "one", "tiny")

    for flow, members in (("x", (0, 1)), ("y", (2,)), ("z", (3,))):
        for u in members:
            landed("one", u)
            own = cur[(u,) + along("xyz", flow, place[flow])]
            if flow == "x":
                mid[u] = own + chain[u, 2] + chain[u, 3]
            else:
                mid[u] = own + r1[u, 0] + r1[u, 1] + r1[u, 2]
        axes = "xyz".replace(flow, "")
        us = pl.ds(members[0], len(members))
        for n, (da, db) in enumerate(plane):
            src = mid.at[us, other(axes[0], da), other(axes[1], db)]
            go(src, r2.at[n, us], in_plane(axes, da, db), "two", flow)

    landed("one", "tiny")
    t1[place["y"]] = tiny_cur[0]
    tiny_cur[1] = t1[0] + t1[1] + t1[2] + t1[3]
    landed("one", "small")
    small_got[0] = small_cur[place["y"]] + s1[0] + s1[1] + s1[2]
    for dx, dz in plane:
        to = in_plane("xz", dx, dz)
        go(small_got.at[0, other("z", dz)], s2.at[me, place["z"]], to, "two", "small")
    for d in (2, 1, 3):
        go(tiny_cur.at[1], t2.at[0, place["z"]], far("z", other("z", d)), "two", "tiny")
    def summed(parts):
        total = parts[0]
        for part in parts[1:]:
            total = total + part
        return total

    tiles = {}
    for flow, members in (("x", (0, 1)), ("y", (2,)), ("z", (3,))):
        landed("two", flow)
        axes = "xyz".replace(flow, "")
        for u in members:
            own = mid[u, place[axes[0]], place[axes[1]]]
            tiles[u] = summed([own] + [r2[n, u] for n in range(15)])
    landed("two", "small")
    s2[me, place["z"]] = small_got[0, place["z"]]
    landed("two", "tiny")
    t2[0, place["z"]] = tiny_cur[1]
    tiny_cur[2] = summed([t2[0, z] for z in range(4)])
    tiles[4] = summed([s2[x, z] for x in range(4) for z in range(4)])
    packed[...] = pack([tiles[t] for t in range(5)])

    home = out.at[core, place["y"], place["z"]]
    for n, (dy, dz) in enumerate(plane):
        go(packed, home, in_plane("yz", dy, dz), "all", n)
    for d in (2, 1, 3):
        go(tiny_cur.at[2], t2.at[1, me], far("x", other("x", d)), "all", "tiny")
    go(packed, home, mate, "last", "own")
    out[core, place["y"], place["z"]] = packed[...]
    for n, (dy, dz) in reversed(list(enumerate(plane))):
        landed("all", n)
        came = out.at[core, lax.rem(place["y"] + 4 - dy, 4), lax.rem(place["z"] + 4 - dz, 4)]
        go(came, came, mate, "last", n)
    landed("all", "tiny")
    t2[1, me] = tiny_cur[2]
    tiny_out[core] = summed([t2[1, x] for x in range(4)])
    go(tiny_out.at[core], tiny_out.at[core], mate, "last", "tiny")
    landed("last", "tiny")
    landed("last", "own")
    for n in range(len(plane)):
        landed("last", n)
    for copy in pending:
        copy.wait_send()


def whole(total, init, brown, step, length, obs, observed, w_in, b_in, w_out, b_out, dec, prior, diff):
    steps, rows, width = brown.shape
    hidden, n_obs = 4 * w_in.shape[1], obs.shape[1]
    vmem, dma = pltpu.VMEM, pltpu.SemaphoreType.DMA
    near, rest = pl.BlockSpec(memory_space=vmem), pl.BlockSpec(memory_space=pl.ANY)
    tile = (8, 128)
    return pl.pallas_call(
        functools.partial(whole_kernel, 1.0 / total),
        out_shape=(
            jax.ShapeDtypeStruct((1, rows), F32),
            jax.ShapeDtypeStruct((2, 4, 4, 48, 128), jnp.int16),
            jax.ShapeDtypeStruct((2,) + tile, F32),
            jax.ShapeDtypeStruct((rows, width), F32),
        ),
        in_specs=[rest] * 13,
        out_specs=[near] * 4,
        scratch_shapes=[
            vmem((width, hidden), BF16),
            vmem((hidden, width), BF16),
            vmem((hidden,), BF16),
            vmem(init.shape, F32),
            vmem(brown.shape, BF16),
            vmem((1, rows), F32),
            vmem((1, rows), jnp.int32),
            vmem((n_obs, rows), jnp.int32),
            vmem(observed.shape, BF16),
            vmem((1, width), F32),
            vmem(dec.shape, BF16),
            vmem((1, width), F32),
            vmem((1, width), F32),
            vmem((rows, width), F32),
            vmem((rows, rows), F32),
            vmem((rows, rows), jnp.int32),
            vmem((rows, width), F32),
            vmem((n_obs, rows, rows), jnp.int32),
            vmem((rows * n_obs, rows), F32),
            vmem((n_obs, rows, rows), F32),
            vmem((rows, rows), F32),
            vmem((width, (steps + 1) * rows), BF16),
            vmem((steps * rows, hidden), BF16),
            vmem((steps, rows, width), F32),
            vmem((steps * rows, hidden), BF16),
            vmem(((steps + 1) * rows, width), BF16),
            vmem((width, steps * rows), BF16),
            vmem((hidden, width), BF16),
            vmem((width, hidden), BF16),
            vmem((width, width), BF16),
            vmem((rows, width), F32),
            vmem((rows, width), F32),
            vmem((8, hidden), F32),
            vmem((8, width), F32),
            vmem((4, 2, 4, 4, 4) + tile, F32),
            vmem((2, 4, 4) + tile, F32),
            vmem((2,) + tile, F32),
            vmem((4, 4, 4, 4) + tile, F32),
            vmem((4, 4, 4, 4) + tile, F32),
            vmem((4, 4, 4) + tile, F32),
            vmem((4, 3, 4, 4) + tile, F32),
            vmem((2, 4, 4, 4) + tile, F32),
            vmem((15, 4) + tile, F32),
            vmem((4, 4) + tile, F32),
            vmem((4, 4) + tile, F32),
            vmem((3, 4) + tile, F32),
            vmem((4, 4) + tile, F32),
            vmem(tile, F32),
            vmem((3,) + tile, F32),
            vmem((4,) + tile, F32),
            vmem((2, 4) + tile, F32),
            vmem((48, 128), jnp.int16),
            dma((10,)), dma((10,)), dma((4,)), dma((4,)), dma((10,)), dma((10,)), dma((13,)),
            dma((COPIES,)), dma((COPIES,)),
        ],
        compiler_params=pltpu.CompilerParams(
            collective_id=0, has_side_effects=True, vmem_limit_bytes=58 * 1024 * 1024
        ),
        name="whole",
    )(
        init, brown, step.reshape(1, -1), length.reshape(1, -1), obs.T, observed, w_in,
        b_in, w_out, b_out.reshape(1, -1), dec, prior.reshape(1, -1), diff.reshape(1, -1),
    )


def finish_kernel(elbo_in, out, tiny, ginit_in, elbo, w_in, w_out, dec, b_in, b_out, scores, ginit, turn):
    me = lax.axis_index("mp")
    elbo[...] = elbo_in[...]
    ginit[...] = ginit_in[...]
    for n in range(32):
        block = out[n // 16, (n // 4) % 4, n % 4].astype(jnp.int32).astype(F32)
        rs = slice(n * 8, n * 8 + 8)
        part = [block[t * 8 : t * 8 + 8] * jnp.exp2(block[40 + t : 41 + t]) for t in range(5)]
        w_in[rs, :128] = part[0]
        w_in[rs, 128:] = part[1]
        turn[rs, :128] = part[2]
        turn[rs, 128:] = part[3]
        dec[rs, :] = part[4]
    w_out[...] = turn[...].T
    for r in range(2):
        b_in[:, r * 128 : (r + 1) * 128] = tiny[0, pl.ds(2 * me + r, 1), :]
        b_out[:, r * 128 : (r + 1) * 128] = tiny[1, r : r + 1, :]
    first = lax.broadcasted_iota(jnp.int32, (1, 128), 1) == 0
    both = jnp.where(first, tiny[1, 2:3, :], tiny[1, 3:4, :])
    scores[...] = both[:, :2]


def unpack(elbo, out, tiny, ginit):
    vmem = pltpu.VMEM
    return pl.pallas_call(
        finish_kernel,
        out_shape=tuple(
            jax.ShapeDtypeStruct(s, F32)
            for s in ((1, 128), (256, 256), (256, 256), (256, 128), (1, 256), (1, 256), (1, 2), (128, 256))
        ),
        in_specs=[pl.BlockSpec(memory_space=vmem)] * 4,
        out_specs=[pl.BlockSpec(memory_space=vmem)] * 8,
        scratch_shapes=[vmem((256, 256), F32)],
        name="unpack",
    )(elbo, out, tiny, ginit)


def on_device(
    init_state, brownian, step_size, lengths, obs_steps, observed,
    w_in, b_in, w_out, b_out, decoder, prior_rate, diffusion,
):
    total = init_state.shape[0] * lax.axis_size(BATCH_MP)
    elbo, parts, tiny, grad_init = whole(
        total, init_state, brownian, step_size, lengths, obs_steps, observed,
        w_in, b_in, w_out, b_out, decoder, prior_rate, diffusion,
    )
    elbo, own_in, own_out, grad_dec, own_b, grad_b_out, scores, grad_init = unpack(
        elbo, parts, tiny, grad_init
    )
    return (
        elbo.reshape(-1), scores.reshape(-1), own_in, own_b.reshape(-1), own_out, grad_b_out.reshape(-1),
        grad_dec, grad_init,
    )


def solution(mesh):
    torus = Mesh(
        mesh.devices.reshape(4, 4, 2, mesh.shape["mp"]), ("batch_0", "batch_1", "batch_2", "mp")
    )
    placed = (
        P(BATCH_MP, None), P(None, BATCH_MP, None), P(BATCH_MP), P(BATCH_MP), P(BATCH_MP, None),
        P(BATCH_MP, None, None), P(None, "mp"), P("mp"), P("mp", None), P(), P(), P(), P(),
    )
    return jax.shard_map(
        on_device,
        mesh=torus,
        in_specs=placed,
        out_specs=(
            P(BATCH_MP), P(), P(None, "mp"), P("mp"), P("mp", None), P(), P(), P(BATCH_MP, None),
        ),
        check_vma=False,
    )
```
